256 devices in a mesh: lat: 2 (over x_hi), lon: 2 (over x_lo), lev: 64 (over z, y, core).
Axes of the slice: x: 4 (x_hi: 2, x_lo: 2; x = x_hi * 2 + x_lo), y: 4, z: 8, core: 2. Of those that a mesh axis runs over, the one named last changes fastest.
Arguments:
- along_axis_flow: bfloat16 [640, 4, 32, 1440], P(('lat', 'lev'), None, None, 'lon'), may hold values from -6 to 6
- poleward_flow: bfloat16 [640, 4, 32, 1440], P(('lat', 'lev'), None, None, 'lon'), may hold values from -6 to 6
- warmth_departure: bfloat16 [640, 4, 32, 1440], P(('lat', 'lev'), None, None, 'lon'), may hold values from -6 to 6
- validity_indicator: int32 [640, 32, 1440], P(('lat', 'lev'), None, 'lon'), may hold values from 0 to 1
- layer_depth_span: float32 [32], replicated, may hold values from 0.3 to 3
- desired_circulation_norm: float32 [640, 4, 32], P(('lat', 'lev')), may hold values from -4 to 4
Outputs:
- psi_norm: float32 [640, 4, 32], P(('lat', 'lev'))
- heat_cospec: float32 [720, 640, 128], P('lon', ('lat', 'lev'))
- momentum_cospec: float32 [720, 640, 128], P('lon', ('lat', 'lev'))
- budget_penalty: float32 [], replicated
The draws below stay inside these ranges and needn't reach their ends.
All inputs are finite; a program needn't handle non-finite values. Where the reference program divides by a largest or mean magnitude, that divisor is 1e-20 or more.
Results may differ from the reference program's by a relative error of at most 0.0033.
Values may be sent and summed in bfloat16 or wider, within the bound.
No kernel may reach another device: no remote copies, remote signals or barrier semaphores. Data moves between devices by JAX's collectives and lax.ppermute only.
A program may use at most 64 MiB of HBM per device.

```python
import math
import jax
import jax.numpy as jnp
from jax import lax

ENSEMBLE_MEMBERS = 4
ISOBARIC_SHEETS = 32
GRID_MERIDIANS = 1440
HARMONIC_ORDERS = 720
POLAR_ANGLES = 640


def draw_validity_indicator(key, part):
    first_key, second_key = jax.random.split(jax.random.fold_in(key, 11))
    row_rate = jax.random.randint(first_key, (POLAR_ANGLES, ISOBARIC_SHEETS, 1), 0, 9)
    cell_draw = jax.random.randint(second_key, (POLAR_ANGLES, ISOBARIC_SHEETS, GRID_MERIDIANS), 0, 8)
    return (cell_draw < row_rate).astype(jnp.int32)


def shard_levels(own_key, extent, cuts, least, largest):
    def one(position, shards_of):
        heights = jax.random.uniform(jax.random.fold_in(jax.random.fold_in(own_key, 6), position), (shards_of,), jnp.float32, least / len(cuts), largest / len(cuts))
        return jnp.repeat(jnp.exp(heights), extent[position] // shards_of).reshape((-1,) + (1,) * (len(extent) - position - 1))

    loudness = one(*cuts[0])
    for cut in cuts[1:]:
        loudness = loudness * one(*cut)
    return loudness


def centred(stream_key, extent, spread, reach, shards=(), held_as=jnp.bfloat16):
    result = jax.random.normal(stream_key, extent, jnp.float32) * spread
    if len(shards) > 0:
        result = shard_levels(stream_key, extent, shards, -0.22, 0.18) * result
    return jnp.clip(result, min=-reach, max=reach).astype(held_as)


def setup_inputs(seed: int = 0) -> dict:
    seeds = jax.random.split(jax.random.key(seed), 7)
    along_axis_flow = centred(seeds[0], (POLAR_ANGLES, ENSEMBLE_MEMBERS, ISOBARIC_SHEETS, GRID_MERIDIANS), 1.0, 6.0, ((0, 128), (3, 2)))
    poleward_flow = centred(seeds[1], (POLAR_ANGLES, ENSEMBLE_MEMBERS, ISOBARIC_SHEETS, GRID_MERIDIANS), 1.0, 6.0, ((0, 128), (3, 2)))
    warmth_departure = centred(seeds[2], (POLAR_ANGLES, ENSEMBLE_MEMBERS, ISOBARIC_SHEETS, GRID_MERIDIANS), 1.0, 6.0, ((0, 128), (3, 2)))
    validity_indicator = draw_validity_indicator(jax.random.fold_in(seeds[6], 71), 0)
    layer_depth_span = jnp.clip(jnp.exp(jax.random.uniform(seeds[4], (ISOBARIC_SHEETS,), jnp.float32, math.log(0.3), math.log(3.0))), 0.3, 3.0)
    desired_circulation_norm = centred(seeds[5], (POLAR_ANGLES, ENSEMBLE_MEMBERS, ISOBARIC_SHEETS), 0.5, 4.0, ((0, 128),), jnp.float32)
    return {"along_axis_flow": along_axis_flow, "poleward_flow": poleward_flow, "warmth_departure": warmth_departure, "validity_indicator": validity_indicator, "layer_depth_span": layer_depth_span, "desired_circulation_norm": desired_circulation_norm}


epsilon = 1e-6


def build_waves(wave_rows, lon_index):
    wavenumber = wave_rows // 2 + 1
    component = wave_rows % 2
    turns = (wavenumber[:, None] * lon_index[None, :]) % GRID_MERIDIANS
    angle = turns.astype(jnp.float32) * (2.0 * math.pi / GRID_MERIDIANS)
    return jnp.where(component[:, None] == 0, jnp.cos(angle), jnp.sin(angle)).astype(jnp.bfloat16)


def reference(along_axis_flow, poleward_flow, warmth_departure, validity_indicator, layer_depth_span, desired_circulation_norm):
    retained_indicator = validity_indicator.astype(jnp.bfloat16)
    waves_table = build_waves(jnp.arange(2 * HARMONIC_ORDERS, dtype=jnp.int32), jnp.arange(GRID_MERIDIANS, dtype=jnp.int32))
    norm_factor = 2.0 / (GRID_MERIDIANS * GRID_MERIDIANS)

    def one_circle_slice(items):
        u_row, v_row, t_row, keep_row = items
        input_tensors = jnp.stack([u_row * keep_row[None], v_row * keep_row[None], t_row * keep_row[None]])
        input_tensors = input_tensors.reshape(3, ENSEMBLE_MEMBERS * ISOBARIC_SHEETS, GRID_MERIDIANS)
        fourier_weights = lax.dot_general(waves_table, input_tensors, (((1,), (2,)), ((), ())), preferred_element_type=jnp.float32)
        fourier_weights = fourier_weights.reshape(HARMONIC_ORDERS, 2, 3, ENSEMBLE_MEMBERS * ISOBARIC_SHEETS)
        heat_part = norm_factor * (fourier_weights[:, 0, 1] * fourier_weights[:, 0, 2] + fourier_weights[:, 1, 1] * fourier_weights[:, 1, 2])
        moment_part = norm_factor * (fourier_weights[:, 0, 0] * fourier_weights[:, 0, 1] + fourier_weights[:, 1, 0] * fourier_weights[:, 1, 1])
        return heat_part, moment_part

    thermal_transport_sum, eastward_stress_sum = lax.map(one_circle_slice, (along_axis_flow, poleward_flow, warmth_departure, retained_indicator))
    heat_cospec = jnp.transpose(thermal_transport_sum, (1, 0, 2))
    momentum_cospec = jnp.transpose(eastward_stress_sum, (1, 0, 2))

    screened_northward_speed = poleward_flow * retained_indicator[:, None]
    zonal_v = jnp.sum(screened_northward_speed, axis=3, dtype=jnp.float32)
    kept_count = jnp.sum(validity_indicator, axis=2).astype(jnp.float32)
    mean_v = zonal_v / jnp.maximum(kept_count, 1.0)[:, None, :]
    rows_lat = jnp.arange(POLAR_ANGLES, dtype=jnp.int32).astype(jnp.float32)
    latitude = ((rows_lat + 0.5) / POLAR_ANGLES - 0.5) * math.pi
    cosine = jnp.cos(latitude)
    weighted = mean_v * cosine[:, None, None] * layer_depth_span[None, None, :]
    stream = jnp.cumsum(jnp.cumsum(weighted, axis=2), axis=0)
    peak_value = jnp.max(jnp.abs(stream))
    psi_norm = stream / (peak_value + epsilon)
    residual_accumulator = jnp.sum(cosine[:, None, None] * (psi_norm - desired_circulation_norm) ** 2)
    budget_penalty = residual_accumulator / (ENSEMBLE_MEMBERS * ISOBARIC_SHEETS * POLAR_ANGLES)
    return psi_norm, heat_cospec, momentum_cospec, budget_penalty
```

```python
import math

import jax
import jax.numpy as jnp
import numpy as np
from jax import lax
from jax.experimental import pallas as pl
from jax.experimental.pallas import tpu as pltpu
from jax.sharding import Mesh
from jax.sharding import PartitionSpec as P

MERIDIANS = 1440
ORDERS = 720
LAT_LEV = ("lat", "lev_0", "lev_1", "lev_2")
EPSILON = 1e-06
GROUPS = ((0,), (1, 2), (3, 4))
F32 = jnp.float32
BF16 = jnp.bfloat16
VMEM_LIMIT = 40 * 1024 * 1024


def half_table(lon):
    order = np.arange(1, ORDERS + 1, dtype=np.int64)
    turns = (order[:, None] * np.arange(lon, dtype=np.int64)[None, :]) % MERIDIANS
    angle = turns.astype(np.float32) * np.float32(2.0 * math.pi / MERIDIANS)
    both = np.stack([np.cos(angle), np.sin(angle)]).reshape(2, 2, ORDERS // 2, lon)
    return np.ascontiguousarray(both.transpose(1, 0, 2, 3)).reshape(2, ORDERS, lon)


def params(**kw):
    return pltpu.CompilerParams(vmem_limit_bytes=VMEM_LIMIT, **kw)


def masked(field_ref, keep):
    return (field_ref[0] * keep[None]).reshape(-1, keep.shape[-1])


def pack_kernel(half_ref, u_ref, v_ref, t_ref, m_ref, o_ref):
    keep = m_ref[0].astype(F32).astype(BF16)
    o_ref[0] = jnp.concatenate([masked(t_ref, keep), masked(u_ref, keep), masked(v_ref, keep)])


def pack(half, u, v, t, mask, rows):
    _, samples, levels, lon = u.shape
    part = samples // 2
    first = rows[0]
    field = pl.BlockSpec((1, part, levels, lon), lambda i, s: (i + first, s[0], 0, 0))
    return pl.pallas_call(
        pack_kernel,
        out_shape=jax.ShapeDtypeStruct((len(rows), 3 * part * levels, lon), BF16),
        grid_spec=pltpu.PrefetchScalarGridSpec(
            num_scalar_prefetch=1,
            grid=(len(rows),),
            in_specs=[
                field,
                field,
                field,
                pl.BlockSpec((1, levels, lon), lambda i, s: (i + first, 0, 0)),
            ],
            out_specs=pl.BlockSpec((1, 3 * part * levels, lon), lambda i, s: (i, 0, 0)),
        ),
        compiler_params=params(),
        name="pack",
    )(half, u, v, t, mask)


CONTRACT = (((1,), (1,)), ((), ()))


def zonal_kernel(v_ref, m_ref, d_ref, o_ref):
    rows, samples, levels, lon = v_ref.shape
    ones = jnp.ones((8, lon), BF16)
    for j in range(rows):
        keep = m_ref[j].astype(F32).astype(BF16)
        v = (v_ref[j] * keep[None]).reshape(samples * levels, lon)
        o_ref[j : j + 1, :] = lax.dot_general(ones, v, CONTRACT, preferred_element_type=F32)[0:1]
        full = jnp.broadcast_to(keep[None], (samples, levels, lon)).reshape(samples * levels, lon)
        o_ref[rows + j : rows + j + 1, :] = lax.dot_general(
            ones, full, CONTRACT, preferred_element_type=F32
        )[0:1]
    o_ref[2 * rows : 3 * rows, :] = d_ref[...]
    o_ref[3 * rows :, :] = jnp.zeros((1, o_ref.shape[1]), F32)


def zonal(v, mask, desired):
    rows, samples, levels, _ = v.shape
    return pl.pallas_call(
        zonal_kernel,
        out_shape=jax.ShapeDtypeStruct((3 * rows + 1, samples * levels), F32),
        compiler_params=params(),
        name="zonal",
    )(v, mask, desired)


def wave_kernel(half_ref, table_ref, own_ref, got_ref, o_ref):
    def lay(ref):
        x = ref[0]
        return jnp.concatenate([x, x[2 * x.shape[0] // 3 :]])

    table = table_ref[0]
    near = lax.dot_general(table, lay(own_ref), CONTRACT, preferred_element_type=F32)
    far = lax.dot_general(table, lay(got_ref), CONTRACT, preferred_element_type=F32)
    n = near.shape[0] // 2
    odd = lax.broadcasted_iota(jnp.int32, (n, 1), 0) % 2 == 0
    sign = jnp.where(odd, -1.0, 1.0).astype(F32)
    cos = near[:n] + sign * far[:n]
    sin = near[n:] + sign * far[n:]
    w = cos.shape[1] // 2
    scale = 2.0 / (MERIDIANS * MERIDIANS)
    o_ref[0] = (scale * (cos[:, :w] * cos[:, w:] + sin[:, :w] * sin[:, w:])).astype(o_ref.dtype)


def waves(half, table, own, got, dtype):
    rows, cols, lon = own.shape
    n = table.shape[1] // 2
    unit = pl.BlockSpec((1, cols, lon), lambda i, s: (i, 0, 0))
    return pl.pallas_call(
        wave_kernel,
        out_shape=jax.ShapeDtypeStruct((rows, n, 2 * cols // 3), dtype),
        grid_spec=pltpu.PrefetchScalarGridSpec(
            num_scalar_prefetch=1,
            grid=(rows,),
            in_specs=[pl.BlockSpec((1, 2 * n, lon), lambda i, s: (s[0], 0, 0)), unit, unit],
            out_specs=pl.BlockSpec((1, n, 2 * cols // 3), lambda i, s: (i, 0, 0)),
        ),
        compiler_params=params(),
        name="waves",
    )(half, table, own, got)


def join_kernel(half_ref, own_ref, got_ref, heat_in, mom_in, heat_ref, mom_ref):
    own = own_ref[0]
    got = got_ref[0].astype(F32)
    first = half_ref[0] == 0
    a = jnp.where(first, own, got)
    b = jnp.where(first, got, own)
    w = own.shape[1] // 2
    low = lax.broadcasted_iota(jnp.int32, own.shape, 1) < w
    heat_ref[0] = jnp.where(low, a, pltpu.roll(b, w, 1))
    mom_ref[0] = jnp.where(low, pltpu.roll(a, w, 1), b)


def join(half, own, got, outs, rows, total):
    first = rows[0]
    n, width = own.shape[1:]
    unit = pl.BlockSpec((1, n, width), lambda i, s: (i, 0, 0))
    plane = pl.BlockSpec((1, n, width), lambda i, s: (i + first, 0, 0))
    shape = jax.ShapeDtypeStruct((total, n, width), F32)
    body = join_kernel
    extra = {}
    args = (half, own, got)
    specs = [unit, unit]
    if outs is None:
        body = lambda h, a, b, x, y: join_kernel(h, a, b, None, None, x, y)
    else:
        args += outs
        specs += [pl.BlockSpec(memory_space=pl.ANY)] * 2
        extra = {"input_output_aliases": {3: 0, 4: 1}}
    return pl.pallas_call(
        body,
        out_shape=(shape, shape),
        grid_spec=pltpu.PrefetchScalarGridSpec(
            num_scalar_prefetch=1, grid=(len(rows),), in_specs=specs, out_specs=(plane, plane)
        ),
        compiler_params=params(),
        name="join",
        **extra,
    )(*args)


def cosines(first, rows, total):
    index = lax.broadcasted_iota(jnp.int32, (rows, 1), 0) + first
    return jnp.cos(((index.astype(F32) + 0.5) / total - 0.5) * math.pi)


def weigh_kernel(total, place_ref, own_ref, lon_ref, lat_ref, diag_ref, depth_ref, o_ref):
    rows = (own_ref.shape[0] - 1) // 3
    north = place_ref[0] == 1
    depth = depth_ref[0:1, :]

    def both(near, far, first):
        mean = (near[0:rows] + far[0:rows]) / jnp.maximum(
            near[rows : 2 * rows] + far[rows : 2 * rows], 1.0
        )
        return mean * cosines(first, rows, total) * depth, near[2 * rows : 3 * rows]

    mine = both(own_ref, lon_ref, place_ref[1])
    other = both(lat_ref, diag_ref, place_ref[2])
    for i in range(2):
        o_ref[0, i] = jnp.where(north, other[i], mine[i])
        o_ref[1, i] = jnp.where(north, mine[i], other[i])


def band_kernel(total, place_ref, g_ref, l_ref, s_ref, w_ref):
    peers, _, _, rows, width = g_ref.shape
    span = peers * rows
    lane = lax.broadcasted_iota(jnp.int32, (1, width), 1) % 32
    for half in range(2):
        so_far = jnp.zeros((1, width), F32)
        for p in range(peers):
            for r in range(rows):
                so_far = so_far + g_ref[p, half, 0, r : r + 1, :]
                w_ref[p * rows + r : p * rows + r + 1, :] = so_far
        run = w_ref[0:span, :]
        for step in (1, 2, 4, 8, 16):
            run = run + jnp.where(lane >= step, pltpu.roll(run, step, 1), 0.0)
        l_ref[half] = run
        want = jnp.concatenate([g_ref[p, half, 1] for p in range(peers)])
        cosine = cosines(place_ref[half], span, total)
        stats = (
            run[span - 1 : span],
            jnp.max(run, axis=0, keepdims=True),
            jnp.min(run, axis=0, keepdims=True),
            jnp.sum(cosine * run, axis=0, keepdims=True),
            jnp.sum(cosine * run * run, axis=0, keepdims=True),
            jnp.sum(cosine * want, axis=0, keepdims=True),
            jnp.sum(cosine * run * want, axis=0, keepdims=True),
            jnp.sum(cosine * want * want, axis=0, keepdims=True),
        )
        for i, stat in enumerate(stats):
            s_ref[8 * half + i : 8 * half + i + 1, :] = stat


def finish_kernel(total, span, place_ref, own_ref, s_ref, psi_ref, loss_ref):
    blocks, _, width = s_ref.shape
    offset = jnp.zeros((1, width), F32)
    mine = offset
    peak = offset
    square = offset
    cross = offset
    want = offset
    for half in range(2):
        for z in range(blocks):
            at = 8 * half
            s, hi, lo, run1, run2, want1, cross1, want2 = (
                s_ref[z, at + i : at + i + 1, :] for i in range(8)
            )
            here = half * blocks + z
            first = here * span
            weight = float(
                np.sum(np.cos(((np.arange(first, first + span) + 0.5) / total - 0.5) * math.pi))
            )
            mine = jnp.where(place_ref[0] == here, offset, mine)
            peak = jnp.maximum(peak, jnp.maximum(jnp.abs(offset + hi), jnp.abs(offset + lo)))
            square = square + (run2 + 2.0 * offset * run1 + offset * offset * weight)
            cross = cross + (cross1 + offset * want1)
            want = want + want2
            offset = offset + s
    scale = jnp.max(peak, axis=1, keepdims=True) + EPSILON
    psi_ref[...] = (own_ref[...] + mine) / scale
    a = jnp.sum(square, axis=1, keepdims=True)
    b = jnp.sum(cross, axis=1, keepdims=True)
    c = jnp.sum(want, axis=1, keepdims=True)
    loss = (a / scale / scale - 2.0 * (b / scale) + c) / (width * total)
    loss_ref[...] = jnp.broadcast_to(loss, loss_ref.shape)


def all_of(x, axes):
    return lax.all_to_all(
        jnp.broadcast_to(x, (lax.axis_size(axes), *x.shape)), axes, split_axis=0, concat_axis=0, tiled=True
    )


def per_device(u, v, t, mask, depth, desired):
    bands, samples, levels, lon = v.shape
    width = samples * levels
    half = lax.axis_index("lon")
    near = half[None].astype(jnp.int32)
    far = 1 - near
    total = bands * lax.axis_size(LAT_LEV)
    smem = pl.BlockSpec(memory_space=pltpu.SMEM)
    vmem = pl.BlockSpec(memory_space=pltpu.VMEM)

    across = [(0, 1), (1, 0)]
    with jax.named_scope("send"):
        sent = [lax.ppermute(pack(far, u, v, t, mask, rows), "lon", across) for rows in GROUPS]
    own = [pack(near, u, v, t, mask, rows) for rows in GROUPS]

    with jax.named_scope("small"):
        sums = zonal(v, mask, desired.reshape(bands, width))
        by_lon = lax.ppermute(sums, "lon", across)
        by_lat = lax.ppermute(sums, "lat", across)
        by_both = lax.ppermute(sums, ("lat", "lon"), [(i, 3 - i) for i in range(4)])
    per_half = bands * lax.axis_size(("lev_0", "lev_1", "lev_2"))
    lat = lax.axis_index("lat")
    band = lax.axis_index(("lev_0", "lev_1", "lev_2"))
    inner = lax.axis_index(("lev_1", "lev_2"))
    outer = lax.axis_index("lev_0")
    span = bands * lax.axis_size(("lev_1", "lev_2"))
    place = jnp.stack(
        [lat, lat * per_half + band * bands, (1 - lat) * per_half + band * bands]
    ).astype(jnp.int32)
    spread = jnp.tile(depth, samples)[None]
    rows4 = pl.pallas_call(
        lambda *refs: weigh_kernel(total, *refs),
        out_shape=jax.ShapeDtypeStruct((2, 2, bands, width), F32),
        in_specs=[smem] + [vmem] * 5,
        out_specs=vmem,
        name="weigh",
    )(place, sums, by_lon, by_lat, by_both, spread)
    near_bands = all_of(rows4, ("lev_1", "lev_2"))
    place = jnp.stack([outer * span, per_half + outer * span]).astype(jnp.int32)
    runs, stats = pl.pallas_call(
        lambda *refs: band_kernel(total, *refs),
        out_shape=(
            jax.ShapeDtypeStruct((2, span, width), F32),
            jax.ShapeDtypeStruct((16, width), F32),
        ),
        in_specs=[smem, vmem],
        out_specs=(vmem, vmem),
        scratch_shapes=[pltpu.VMEM((span, width), F32)],
        name="bands",
    )(place, near_bands)
    all_stats = all_of(stats, "lev_0")
    mine = lax.dynamic_slice(runs, (lat, inner * bands, 0), (1, bands, width))[0]
    place = (lat * lax.axis_size("lev_0") + outer)[None].astype(jnp.int32)
    psi, loss = pl.pallas_call(
        lambda *refs: finish_kernel(total, span, *refs),
        out_shape=(
            jax.ShapeDtypeStruct((bands, width), F32),
            jax.ShapeDtypeStruct((1, width), F32),
        ),
        in_specs=[smem, vmem, vmem],
        out_specs=(vmem, vmem),
        name="finish",
    )(place, mine, all_stats)

    table = jnp.asarray(half_table(lon), BF16)
    outs = None
    back = []
    kept = []
    for mine, got in zip(own, sent):
        with jax.named_scope("back"):
            back.append(lax.ppermute(waves(far, table, mine, got, BF16), "lon", across))
        kept.append(waves(near, table, mine, got, F32))
    for rows, mine, got in zip(GROUPS, kept, back):
        outs = join(near, mine, got, outs, rows, bands)
    heat, momentum = (jnp.transpose(x, (1, 0, 2)) for x in outs)
    return psi.reshape(bands, samples, levels), heat, momentum, loss[0, 0]


def solution(mesh):
    torus = Mesh(
        mesh.devices.reshape(mesh.shape["lat"], mesh.shape["lon"], 8, 4, 2),
        ("lat", "lon", "lev_0", "lev_1", "lev_2"),
    )
    in_specs = (
        P(LAT_LEV, None, None, "lon"),
        P(LAT_LEV, None, None, "lon"),
        P(LAT_LEV, None, None, "lon"),
        P(LAT_LEV, None, "lon"),
        P(),
        P(LAT_LEV, None, None),
    )
    out_specs = (P(LAT_LEV, None, None), P("lon", LAT_LEV, None), P("lon", LAT_LEV, None), P())
    return jax.shard_map(
        per_device, mesh=torus, in_specs=in_specs, out_specs=out_specs, check_vma=False
    )
```

```python
import math

import jax
import jax.numpy as jnp
import numpy as np
from jax import lax
from jax.experimental import pallas as pl
from jax.experimental.pallas import tpu as pltpu
from jax.sharding import Mesh
from jax.sharding import PartitionSpec as P


MERIDIANS = 1440
ORDERS = 720
LAT_LEV = ("lat", "lev_0", "lev_1", "lev_2")
INNER = ("lev_1", "lev_2")
EPSILON = 1e-06
GROUPS = ((0,), (1, 2), (3, 4))
F32 = jnp.float32
BF16 = jnp.bfloat16
MIB = 1024 * 1024
CONTRACT = (((1,), (1,)), ((), ()))
SMEM = pl.BlockSpec(memory_space=pltpu.SMEM)
VMEM = pl.BlockSpec(memory_space=pltpu.VMEM)
HBM = pl.BlockSpec(memory_space=pltpu.HBM)
ANY = pl.BlockSpec(memory_space=pl.ANY)


def half_table(lon):
    order = np.arange(1, ORDERS + 1, dtype=np.int64)
    turns = (order[:, None] * np.arange(lon, dtype=np.int64)[None, :]) % MERIDIANS
    angle = turns.astype(np.float32) * np.float32(2.0 * math.pi / MERIDIANS)
    both = np.stack([np.cos(angle), np.sin(angle)]).reshape(2, 2, ORDERS // 2, lon)
    return np.ascontiguousarray(both.transpose(1, 0, 2, 3)).reshape(2, ORDERS, lon)


def params(mib):
    return pltpu.CompilerParams(vmem_limit_bytes=mib * MIB)


def keep_of(mask):
    return mask.astype(F32).astype(BF16)


def pack_kernel(rows, flip, half_ref, u_ref, v_ref, t_ref, m_ref, o_ref, fields, masks, sems):
    part = fields.shape[2]
    half = 1 - half_ref[0] if flip else half_ref[0]
    copies = []
    for i, row in enumerate(rows):
        group = [pltpu.make_async_copy(m_ref.at[row], masks.at[i], sems.at[i, 3])]
        for f, ref in enumerate((t_ref, u_ref, v_ref)):
            group.append(
                pltpu.make_async_copy(
                    ref.at[row, pl.ds(half * part, part)], fields.at[i, f], sems.at[i, f]
                )
            )
        for c in group:
            c.start()
        copies.append(group)
    size = part * fields.shape[3]
    for i, group in enumerate(copies):
        for c in group:
            c.wait()
        keep = keep_of(masks[i])[None]
        for f in range(3):
            o_ref[i, f * size : (f + 1) * size, :] = (fields[i, f] * keep).reshape(size, -1)


def pack(half, u, v, t, mask, rows, flip):
    _, samples, levels, lon = u.shape
    part = samples // 2
    n = len(rows)
    return pl.pallas_call(
        lambda *refs: pack_kernel(rows, flip, *refs),
        out_shape=jax.ShapeDtypeStruct((n, 3 * part * levels, lon), BF16),
        in_specs=[SMEM, HBM, HBM, HBM, HBM],
        out_specs=VMEM,
        scratch_shapes=[
            pltpu.VMEM((n, 3, part, levels, lon), BF16),
            pltpu.VMEM((n, levels, lon), jnp.int32),
            pltpu.SemaphoreType.DMA((n, 4)),
        ],
        compiler_params=params(60),
        name="pack",
    )(half, u, v, t, mask)


def send_kernel(groups, half_ref, u_ref, v_ref, t_ref, m_ref, _, *rest):
    outs, (sums_ref, us, vs, ts, masks, sems) = rest[: len(groups)], rest[len(groups) :]
    rows, samples, levels, lon = vs.shape
    part = samples // 2
    size = part * levels
    far = 1 - half_ref[0]
    wanted = [row for group in groups for row in group]
    copies = {}
    for j in range(rows):
        group = [
            pltpu.make_async_copy(m_ref.at[j], masks.at[j], sems.at[j, 0]),
            pltpu.make_async_copy(v_ref.at[j], vs.at[j], sems.at[j, 1]),
        ]
        if j in wanted:
            at = pl.ds(far * part, part)
            group.append(pltpu.make_async_copy(u_ref.at[j, at], us.at[j], sems.at[j, 2]))
            group.append(pltpu.make_async_copy(t_ref.at[j, at], ts.at[j], sems.at[j, 3]))
        for c in group:
            c.start()
        copies[j] = group
    ones = jnp.ones((8, lon), BF16)
    for j in range(rows):
        for c in copies[j]:
            c.wait()
        keep = keep_of(masks[j])
        v = (vs[j] * keep[None]).reshape(samples * levels, lon)
        sums_ref[j : j + 1, :] = lax.dot_general(ones, v, CONTRACT, preferred_element_type=F32)[0:1]
        full = jnp.broadcast_to(keep[None], (samples, levels, lon)).reshape(samples * levels, lon)
        sums_ref[rows + j : rows + j + 1, :] = lax.dot_general(
            ones, full, CONTRACT, preferred_element_type=F32
        )[0:1]
        for g, group in enumerate(groups):
            if j in group:
                i = group.index(j)
                outs[g][i, 0:size, :] = (ts[j] * keep[None]).reshape(size, lon)
                outs[g][i, size : 2 * size, :] = (us[j] * keep[None]).reshape(size, lon)
                mine = vs[j, pl.ds(far * part, part)] * keep[None]
                outs[g][i, 2 * size :, :] = mine.reshape(size, lon)


def send(half, u, v, t, mask, after, groups):
    rows, samples, levels, lon = v.shape
    part = samples // 2
    return pl.pallas_call(
        lambda *refs: send_kernel(groups, *refs),
        out_shape=(
            *(jax.ShapeDtypeStruct((len(g), 3 * part * levels, lon), BF16) for g in groups),
            jax.ShapeDtypeStruct((2 * rows, samples * levels), F32),
        ),
        in_specs=[SMEM, HBM, HBM, HBM, HBM, ANY],
        out_specs=(VMEM,) * (len(groups) + 1),
        scratch_shapes=[
            pltpu.VMEM((rows, part, levels, lon), BF16),
            pltpu.VMEM((rows, samples, levels, lon), BF16),
            pltpu.VMEM((rows, part, levels, lon), BF16),
            pltpu.VMEM((rows, levels, lon), jnp.int32),
            pltpu.SemaphoreType.DMA((rows, 4)),
        ],
        compiler_params=params(60),
        name="send",
    )(half, u, v, t, mask, after)


def wave_kernel(flip, half_ref, table_ref, own_ref, got_ref, _, o_ref):
    def lay(x):
        return jnp.concatenate([x, x[2 * x.shape[0] // 3 :]])

    table = table_ref[1 - half_ref[0] if flip else half_ref[0]]
    n = table.shape[0] // 2
    odd = lax.broadcasted_iota(jnp.int32, (n, 1), 0) % 2 == 0
    sign = jnp.where(odd, -1.0, 1.0).astype(F32)
    scale = 2.0 / (MERIDIANS * MERIDIANS)
    for i in range(got_ref.shape[0]):
        near = lax.dot_general(table, lay(own_ref[i]), CONTRACT, preferred_element_type=F32)
        far = lax.dot_general(table, lay(got_ref[i]), CONTRACT, preferred_element_type=F32)
        cos = near[:n] + sign * far[:n]
        sin = near[n:] + sign * far[n:]
        w = cos.shape[1] // 2
        both = cos[:, :w] * cos[:, w:] + sin[:, :w] * sin[:, w:]
        o_ref[i] = (scale * both).astype(o_ref.dtype)


def waves(half, table, own, got, after, flip, dtype):
    rows, cols, _ = got.shape
    return pl.pallas_call(
        lambda *refs: wave_kernel(flip, *refs),
        out_shape=jax.ShapeDtypeStruct((rows, table.shape[1] // 2, 2 * cols // 3), dtype),
        in_specs=[SMEM, VMEM, VMEM, VMEM, ANY],
        out_specs=VMEM,
        compiler_params=params(16),
        name="waves",
    )(half, table, own, got, after)


def join_kernel(first, half_ref, own_ref, got_ref, heat_in, mom_in, heat_ref, mom_ref, heat, mom, sems):
    copies = []
    for i in range(own_ref.shape[0]):
        own = own_ref[i]
        got = got_ref[i].astype(F32)
        zero = half_ref[0] == 0
        a = jnp.where(zero, own, got)
        b = jnp.where(zero, got, own)
        w = own.shape[1] // 2
        low = lax.broadcasted_iota(jnp.int32, own.shape, 1) < w
        heat[i] = jnp.where(low, a, pltpu.roll(b, w, 1))
        mom[i] = jnp.where(low, pltpu.roll(a, w, 1), b)
        for k, (x, ref) in enumerate(((heat, heat_ref), (mom, mom_ref))):
            c = pltpu.make_async_copy(x.at[i], ref.at[first + i], sems.at[i, k])
            c.start()
            copies.append(c)
    for c in copies:
        c.wait()


def join(half, own, got, outs, rows, total):
    n, width = own.shape[1:]
    shape = jax.ShapeDtypeStruct((total, n, width), F32)
    args = (half, own, got)
    specs = [SMEM, VMEM, VMEM]
    extra = {}
    first = rows[0]
    if outs is None:
        body = lambda h, a, b, *refs: join_kernel(first, h, a, b, None, None, *refs)
    else:
        body = lambda *refs: join_kernel(first, *refs)
        args += outs
        specs += [HBM, HBM]
        extra = {"input_output_aliases": {3: 0, 4: 1}}
    return pl.pallas_call(
        body,
        out_shape=(shape, shape),
        in_specs=specs,
        out_specs=(HBM, HBM),
        scratch_shapes=[
            pltpu.VMEM((len(rows), n, width), F32),
            pltpu.VMEM((len(rows), n, width), F32),
            pltpu.SemaphoreType.DMA((len(rows), 2)),
        ],
        compiler_params=params(8),
        name="join",
        **extra,
    )(*args)


def cosines(first, rows, total):
    index = lax.broadcasted_iota(jnp.int32, (rows, 1), 0) + first
    return jnp.cos(((index.astype(F32) + 0.5) / total - 0.5) * math.pi)


def weight_of(first, rows, total):
    latitude = ((np.arange(first, first + rows) + 0.5) / total - 0.5) * math.pi
    return float(np.sum(np.cos(latitude)))


def weigh_kernel(total, place_ref, own_ref, lon_ref, depth_ref, d_ref, o_ref):
    rows, samples, levels = d_ref.shape
    band = place_ref[0] // 128 * 64 + place_ref[0] % 64
    depth = depth_ref[...]
    spread = jnp.concatenate([depth] * samples, axis=1)
    kept = own_ref[rows : 2 * rows] + lon_ref[rows : 2 * rows]
    mean = (own_ref[0:rows] + lon_ref[0:rows]) / jnp.maximum(kept, 1.0)
    weighted = mean * cosines(band * rows, rows, total) * spread
    for p in range(o_ref.shape[0]):
        o_ref[p, 0:rows, :] = weighted
        for b in range(samples):
            o_ref[p, 8 : 8 + rows, b * levels : (b + 1) * levels] = d_ref[:, b, :]


def band_kernel(total, rows, levels, place_ref, g_ref, mine_ref, s_ref, w_ref):
    peers, _, width = g_ref.shape
    span = peers * rows
    lane = lax.broadcasted_iota(jnp.int32, (1, width), 1) % levels
    so_far = jnp.zeros((1, width), F32)
    for p in range(peers):
        for r in range(rows):
            so_far = so_far + g_ref[p, r : r + 1, :]
            w_ref[p * rows + r : p * rows + r + 1, :] = so_far
            w_ref[span + p * rows + r : span + p * rows + r + 1, :] = g_ref[p, 8 + r : 9 + r, :]
    run = w_ref[0:span, :]
    step = 1
    while step < levels:
        run = run + jnp.where(lane >= step, pltpu.roll(run, step, 1), 0.0)
        step *= 2
    want = w_ref[span:, :]
    block = place_ref[0] // 128 * 8 + place_ref[0] % 64 // 8
    cosine = cosines(block * span, span, total)
    stats = (
        run[span - 1 : span],
        jnp.max(run, axis=0, keepdims=True),
        jnp.min(run, axis=0, keepdims=True),
        jnp.sum(cosine * run, axis=0, keepdims=True),
        jnp.sum(cosine * run * run, axis=0, keepdims=True),
        jnp.sum(cosine * want, axis=0, keepdims=True),
        jnp.sum(cosine * run * want, axis=0, keepdims=True),
        jnp.sum(cosine * want * want, axis=0, keepdims=True),
    )
    for p in range(s_ref.shape[0]):
        for i, stat in enumerate(stats):
            s_ref[p, i : i + 1, :] = stat
    w_ref[0:span, :] = run
    for p in range(peers):

        @pl.when(place_ref[0] % 8 == p)
        def _():
            mine_ref[...] = w_ref[p * rows : (p + 1) * rows, :]


def add_block(so_far, block, weight):
    s, hi, lo, run1, run2, want1, cross, want2 = block
    if so_far is None:
        return block
    off = so_far[0]
    return (
        off + s,
        jnp.maximum(so_far[1], off + hi),
        jnp.minimum(so_far[2], off + lo),
        so_far[3] + (run1 + off * weight),
        so_far[4] + (run2 + 2.0 * off * run1 + off * off * weight),
        so_far[5] + want1,
        so_far[6] + (cross + off * want1),
        so_far[7] + want2,
    )


def half_kernel(total, span, place_ref, mine_ref, s_ref, own_ref, half_ref):
    blocks = s_ref.shape[0]
    here = place_ref[0] % 64 // 8
    north = place_ref[0] // 128 == 1
    stats = None
    offset = jnp.zeros((1, s_ref.shape[2]), F32)
    for z in range(blocks):
        if z:
            offset = jnp.where(here == z, stats[0], offset)
        weights = [weight_of((h * blocks + z) * span, span, total) for h in range(2)]
        weight = jnp.where(north, weights[1], weights[0])
        stats = add_block(stats, [s_ref[z, i : i + 1, :] for i in range(8)], weight)
    own_ref[...] = mine_ref[...] + offset
    for i, stat in enumerate(stats):
        half_ref[i : i + 1, :] = stat


def finish_kernel(total, place_ref, own_ref, near_ref, far_ref, psi_ref, loss_ref):
    _, samples, levels = psi_ref.shape
    north = place_ref[0] // 128 == 1
    near = near_ref[...]
    far = far_ref[...]
    south_half = jnp.where(north, far, near)
    north_half = jnp.where(north, near, far)
    weight = weight_of(total // 2, total // 2, total)
    stats = add_block(
        [south_half[i : i + 1] for i in range(8)], [north_half[i : i + 1] for i in range(8)], weight
    )
    peak = jnp.max(jnp.maximum(jnp.abs(stats[1]), jnp.abs(stats[2])), axis=1, keepdims=True)
    scale = peak + EPSILON
    psi = (own_ref[...] + jnp.where(north, far[0:1], 0.0)) / scale
    for b in range(samples):
        psi_ref[:, b, :] = psi[:, b * levels : (b + 1) * levels]
    a, b, c = (jnp.sum(stats[i], axis=1, keepdims=True) for i in (4, 6, 7))
    loss = (a / scale / scale - 2.0 * (b / scale) + c) / (samples * levels * total)
    loss_ref[...] = jnp.broadcast_to(loss, loss_ref.shape)


def small(body, out_shape, *args, scratch=(), after=None):
    many = isinstance(out_shape, tuple)
    specs = [SMEM] + [VMEM] * (len(args) - 1)
    if after is not None:
        plain, count = body, len(args)
        body = lambda *refs: plain(*refs[:count], *refs[count + 1 :])
        args += (after,)
        specs.append(ANY)
    return pl.pallas_call(
        body,
        out_shape=out_shape,
        in_specs=specs,
        out_specs=(VMEM,) * len(out_shape) if many else VMEM,
        scratch_shapes=scratch,
        compiler_params=params(2),
    )(*args)


def all_of(x, axes):
    return lax.all_to_all(x, axes, split_axis=0, concat_axis=0, tiled=True)


def floats(*shape):
    return jax.ShapeDtypeStruct(shape, F32)


def per_device(u, v, t, mask, depth, desired):
    bands, samples, levels, lon = v.shape
    width = samples * levels
    total = bands * lax.axis_size(LAT_LEV)
    half = lax.axis_index("lon")[None].astype(jnp.int32)
    place = lax.axis_index(("lat", "lon", "lev_0", "lev_1", "lev_2"))[None].astype(jnp.int32)
    across = [(0, 1), (1, 0)]
    table = jnp.asarray(half_table(lon), BF16)

    def swap(x):
        return lax.ppermute(x, "lon", across)

    sent = [pack(half, u, v, t, mask, GROUPS[0], True)]
    *rest, sums = send(half, u, v, t, mask, sent[0], GROUPS[1:])
    sent += rest
    got = [swap(sent[0])]
    by_lon = swap(sums)
    got += [swap(x) for x in rest]
    own = [pack(half, u, v, t, mask, group, False) for group in GROUPS]

    def both(g, after):
        far = waves(half, table, own[g], got[g], after, True, BF16)
        return far, waves(half, table, own[g], got[g], far, False, F32)

    peers = lax.axis_size(INNER)
    outer = lax.axis_size("lev_0")
    rows = small(
        lambda *refs: weigh_kernel(total, *refs),
        floats(peers, 16, width),
        place,
        sums,
        by_lon,
        depth[None],
        desired,
        after=own[0],
    )
    near_bands = all_of(rows, INNER)
    far0, near0 = both(0, rows)
    span = bands * peers
    mine, stats = small(
        lambda *refs: band_kernel(total, bands, levels, *refs),
        (floats(bands, width), floats(outer, 8, width)),
        place,
        near_bands,
        scratch=[pltpu.VMEM((2 * span, width), F32)],
        after=near0,
    )
    all_stats = all_of(stats, "lev_0")
    far1, near1 = both(1, stats)
    mine, near_half = small(
        lambda *refs: half_kernel(total, span, *refs),
        (floats(bands, width), floats(8, width)),
        place,
        mine,
        all_stats,
        after=far1,
    )
    far_half = lax.ppermute(near_half, "lat", across)
    far2, near2 = both(2, near_half)
    psi, loss = small(
        lambda *refs: finish_kernel(total, *refs),
        (floats(bands, samples, levels), floats(1, width)),
        place,
        mine,
        near_half,
        far_half,
        after=near2,
    )

    back = [swap(x) for x in (far0, far1, far2)]
    kept = [near0, near1, near2]
    outs = None
    for group, mine, far in zip(GROUPS, kept, back):
        outs = join(half, mine, far, outs, group, bands)
    heat, momentum = (jnp.transpose(x, (1, 0, 2)) for x in outs)
    return psi, heat, momentum, loss[0, 0]


def solution(mesh):
    torus = Mesh(
        mesh.devices.reshape(mesh.shape["lat"], mesh.shape["lon"], 8, 4, 2),
        ("lat", "lon", "lev_0", "lev_1", "lev_2"),
    )
    in_specs = (
        P(LAT_LEV, None, None, "lon"),
        P(LAT_LEV, None, None, "lon"),
        P(LAT_LEV, None, None, "lon"),
        P(LAT_LEV, None, "lon"),
        P(),
        P(LAT_LEV, None, None),
    )
    out_specs = (P(LAT_LEV, None, None), P("lon", LAT_LEV, None), P("lon", LAT_LEV, None), P())

    return jax.shard_map(
        per_device, mesh=torus, in_specs=in_specs, out_specs=out_specs, check_vma=False
    )
```

```python
import math

import jax
import jax.numpy as jnp
import numpy as np
from jax import lax
from jax.experimental import pallas as pl
from jax.experimental.pallas import tpu as pltpu
from jax.sharding import Mesh
from jax.sharding import PartitionSpec as P


MERIDIANS = 1440
ORDERS = 720
LAT_LEV = ("lat", "lev_0", "lev_1", "lev_2")
INNER = ("lev_1", "lev_2")
EPSILON = 1e-06
GROUPS = ((0,), (1, 2), (3, 4))
F32 = jnp.float32
BF16 = jnp.bfloat16
MIB = 1024 * 1024
CONTRACT = (((1,), (1,)), ((), ()))
SMEM = pl.BlockSpec(memory_space=pltpu.SMEM)
VMEM = pl.BlockSpec(memory_space=pltpu.VMEM)
HBM = pl.BlockSpec(memory_space=pltpu.HBM)
ANY = pl.BlockSpec(memory_space=pl.ANY)


def half_table(lon):
    order = np.arange(1, ORDERS + 1, dtype=np.int64)
    turns = (order[:, None] * np.arange(lon, dtype=np.int64)[None, :]) % MERIDIANS
    angle = turns.astype(np.float32) * np.float32(2.0 * math.pi / MERIDIANS)
    both = np.stack([np.cos(angle), np.sin(angle)]).reshape(2, 2, ORDERS // 2, lon)
    return np.ascontiguousarray(both.transpose(1, 0, 2, 3)).reshape(2, ORDERS, lon)


def params(mib):
    return pltpu.CompilerParams(vmem_limit_bytes=mib * MIB)


def keep_of(mask):
    return mask.astype(F32).astype(BF16)


def pack_kernel(rows, flip, half_ref, u_ref, v_ref, t_ref, m_ref, o_ref, fields, masks, sems):
    part = fields.shape[2]
    half = 1 - half_ref[0] if flip else half_ref[0]
    copies = []
    for i, row in enumerate(rows):
        group = [pltpu.make_async_copy(m_ref.at[row], masks.at[i], sems.at[i, 3])]
        for f, ref in enumerate((t_ref, u_ref, v_ref)):
            group.append(
                pltpu.make_async_copy(
                    ref.at[row, pl.ds(half * part, part)], fields.at[i, f], sems.at[i, f]
                )
            )
        for c in group:
            c.start()
        copies.append(group)
    size = part * fields.shape[3]
    for i, group in enumerate(copies):
        for c in group:
            c.wait()
        keep = keep_of(masks[i])[None]
        for f in range(3):
            o_ref[i, f * size : (f + 1) * size, :] = (fields[i, f] * keep).reshape(size, -1)


def pack(half, u, v, t, mask, rows, flip):
    _, samples, levels, lon = u.shape
    part = samples // 2
    n = len(rows)
    return pl.pallas_call(
        lambda *refs: pack_kernel(rows, flip, *refs),
        out_shape=jax.ShapeDtypeStruct((n, 3 * part * levels, lon), BF16),
        in_specs=[SMEM, HBM, HBM, HBM, HBM],
        out_specs=VMEM,
        scratch_shapes=[
            pltpu.VMEM((n, 3, part, levels, lon), BF16),
            pltpu.VMEM((n, levels, lon), jnp.int32),
            pltpu.SemaphoreType.DMA((n, 4)),
        ],
        compiler_params=params(60),
        name="pack",
    )(half, u, v, t, mask)


def send_kernel(groups, half_ref, u_ref, v_ref, t_ref, m_ref, _, *rest):
    n = len(groups)
    far_refs, near_refs, sums_ref = rest[: n - 1], rest[n - 1 : 2 * n - 1], rest[2 * n - 1]
    us, vs, ts, masks, fars, nears, sems, out_sems = rest[2 * n :]
    rows, samples, levels, lon = vs.shape
    part = samples // 2
    size = part * levels
    near = half_ref[0]
    far = 1 - near
    copies = []
    for j in range(rows):
        group = [
            pltpu.make_async_copy(m_ref.at[j], masks.at[j], sems.at[j, 0]),
            pltpu.make_async_copy(v_ref.at[j], vs.at[j], sems.at[j, 1]),
            pltpu.make_async_copy(u_ref.at[j], us.at[j], sems.at[j, 2]),
            pltpu.make_async_copy(t_ref.at[j], ts.at[j], sems.at[j, 3]),
        ]
        for c in group:
            c.start()
        copies.append(group)
    ones = jnp.ones((8, lon), BF16)
    done = []
    for g, group in enumerate(groups):
        for i, j in enumerate(group):
            for c in copies[j]:
                c.wait()
            keep = keep_of(masks[j])
            v = (vs[j] * keep[None]).reshape(samples * levels, lon)
            sums_ref[j : j + 1, :] = lax.dot_general(
                ones, v, CONTRACT, preferred_element_type=F32
            )[0:1]
            full = jnp.broadcast_to(keep[None], (samples, levels, lon)).reshape(-1, lon)
            sums_ref[rows + j : rows + j + 1, :] = lax.dot_general(
                ones, full, CONTRACT, preferred_element_type=F32
            )[0:1]
            for k, (where, box) in enumerate(((far, fars), (near, nears))):
                if k == 0 and g == 0:
                    continue
                ref = far_refs[g - 1] if k == 0 else near_refs[g]
                for f, field in enumerate((ts, us, vs)):
                    mine = field[j, pl.ds(where * part, part)] * keep[None]
                    box[j, f * size : (f + 1) * size, :] = mine.reshape(size, lon)
                c = pltpu.make_async_copy(box.at[j], ref.at[i], out_sems.at[j, k])
                c.start()
                done.append(c)
    for c in done:
        c.wait()


def send(half, u, v, t, mask, after, groups):
    rows, samples, levels, lon = v.shape
    part = samples // 2
    unit = 3 * part * levels
    n = len(groups)
    packed = [jax.ShapeDtypeStruct((len(g), unit, lon), BF16) for g in groups]
    return pl.pallas_call(
        lambda *refs: send_kernel(groups, *refs),
        out_shape=(
            *packed[1:],
            *packed,
            jax.ShapeDtypeStruct((2 * rows, samples * levels), F32),
        ),
        in_specs=[SMEM, HBM, HBM, HBM, HBM, ANY],
        out_specs=(HBM,) * (2 * n - 1) + (VMEM,),
        scratch_shapes=[
            pltpu.VMEM((rows, samples, levels, lon), BF16),
            pltpu.VMEM((rows, samples, levels, lon), BF16),
            pltpu.VMEM((rows, samples, levels, lon), BF16),
            pltpu.VMEM((rows, levels, lon), jnp.int32),
            pltpu.VMEM((rows, unit, lon), BF16),
            pltpu.VMEM((rows, unit, lon), BF16),
            pltpu.SemaphoreType.DMA((rows, 4)),
            pltpu.SemaphoreType.DMA((rows, 2)),
        ],
        compiler_params=params(60),
        name="send",
    )(half, u, v, t, mask, after)


def wave_kernel(flip, half_ref, table_ref, own_ref, got_ref, _, o_ref):
    def lay(x):
        return jnp.concatenate([x, x[2 * x.shape[0] // 3 :]])

    table = table_ref[1 - half_ref[0] if flip else half_ref[0]]
    n = table.shape[0] // 2
    odd = lax.broadcasted_iota(jnp.int32, (n, 1), 0) % 2 == 0
    sign = jnp.where(odd, -1.0, 1.0).astype(F32)
    scale = 2.0 / (MERIDIANS * MERIDIANS)
    for i in range(got_ref.shape[0]):
        near = lax.dot_general(table, lay(own_ref[i]), CONTRACT, preferred_element_type=F32)
        far = lax.dot_general(table, lay(got_ref[i]), CONTRACT, preferred_element_type=F32)
        cos = near[:n] + sign * far[:n]
        sin = near[n:] + sign * far[n:]
        w = cos.shape[1] // 2
        both = cos[:, :w] * cos[:, w:] + sin[:, :w] * sin[:, w:]
        o_ref[i] = (scale * both).astype(o_ref.dtype)


def waves(half, table, own, got, after, flip, dtype):
    rows, cols, _ = got.shape
    return pl.pallas_call(
        lambda *refs: wave_kernel(flip, *refs),
        out_shape=jax.ShapeDtypeStruct((rows, table.shape[1] // 2, 2 * cols // 3), dtype),
        in_specs=[SMEM, VMEM, VMEM, VMEM, ANY],
        out_specs=VMEM,
        compiler_params=params(16),
        name="waves",
    )(half, table, own, got, after)


def join_kernel(first, parts, half_ref, *refs):
    own_refs, got_refs = refs[:parts], refs[parts : 2 * parts]
    heat_ref, mom_ref, heat, mom, sems = refs[-5:]
    copies = []
    at = 0
    for own_ref, got_ref in zip(own_refs, got_refs):
        for i in range(own_ref.shape[0]):
            own = own_ref[i]
            got = got_ref[i].astype(F32)
            zero = half_ref[0] == 0
            a = jnp.where(zero, own, got)
            b = jnp.where(zero, got, own)
            w = own.shape[1] // 2
            low = lax.broadcasted_iota(jnp.int32, own.shape, 1) < w
            heat[at] = jnp.where(low, a, pltpu.roll(b, w, 1))
            mom[at] = jnp.where(low, pltpu.roll(a, w, 1), b)
            for k, (x, ref) in enumerate(((heat, heat_ref), (mom, mom_ref))):
                c = pltpu.make_async_copy(x.at[at], ref.at[first + at], sems.at[at, k])
                c.start()
                copies.append(c)
            at += 1
    for c in copies:
        c.wait()


def join(half, own, got, outs, rows, total):
    n, width = own[0].shape[1:]
    shape = jax.ShapeDtypeStruct((total, n, width), F32)
    parts = len(own)
    args = (half, *own, *got)
    specs = [SMEM] + [VMEM] * (2 * parts)
    extra = {}
    if outs is not None:
        extra = {"input_output_aliases": {len(args): 0, len(args) + 1: 1}}
        args += outs
        specs += [HBM, HBM]
    return pl.pallas_call(
        lambda *refs: join_kernel(rows[0], parts, *refs),
        out_shape=(shape, shape),
        in_specs=specs,
        out_specs=(HBM, HBM),
        scratch_shapes=[
            pltpu.VMEM((len(rows), n, width), F32),
            pltpu.VMEM((len(rows), n, width), F32),
            pltpu.SemaphoreType.DMA((len(rows), 2)),
        ],
        compiler_params=params(8),
        name="join",
        **extra,
    )(*args)


def cosines(first, rows, total):
    index = lax.broadcasted_iota(jnp.int32, (rows, 1), 0) + first
    return jnp.cos(((index.astype(F32) + 0.5) / total - 0.5) * math.pi)


def weight_of(first, rows, total):
    latitude = ((np.arange(first, first + rows) + 0.5) / total - 0.5) * math.pi
    return float(np.sum(np.cos(latitude)))


def weigh_kernel(total, place_ref, own_ref, lon_ref, depth_ref, d_ref, o_ref):
    rows, samples, levels = d_ref.shape
    band = place_ref[0] // 128 * 64 + place_ref[0] % 64
    depth = depth_ref[...]
    spread = jnp.concatenate([depth] * samples, axis=1)
    kept = own_ref[rows : 2 * rows] + lon_ref[rows : 2 * rows]
    mean = (own_ref[0:rows] + lon_ref[0:rows]) / jnp.maximum(kept, 1.0)
    weighted = mean * cosines(band * rows, rows, total) * spread
    for p in range(o_ref.shape[0]):
        o_ref[p, 0:rows, :] = weighted
        for b in range(samples):
            o_ref[p, 8 : 8 + rows, b * levels : (b + 1) * levels] = d_ref[:, b, :]


def band_kernel(total, rows, levels, place_ref, g_ref, mine_ref, s_ref, w_ref):
    peers, _, width = g_ref.shape
    span = peers * rows
    lane = lax.broadcasted_iota(jnp.int32, (1, width), 1) % levels
    so_far = jnp.zeros((1, width), F32)
    for p in range(peers):
        for r in range(rows):
            so_far = so_far + g_ref[p, r : r + 1, :]
            w_ref[p * rows + r : p * rows + r + 1, :] = so_far
            w_ref[span + p * rows + r : span + p * rows + r + 1, :] = g_ref[p, 8 + r : 9 + r, :]
    run = w_ref[0:span, :]
    step = 1
    while step < levels:
        run = run + jnp.where(lane >= step, pltpu.roll(run, step, 1), 0.0)
        step *= 2
    want = w_ref[span:, :]
    block = place_ref[0] // 128 * 8 + place_ref[0] % 64 // 8
    cosine = cosines(block * span, span, total)
    stats = (
        run[span - 1 : span],
        jnp.max(run, axis=0, keepdims=True),
        jnp.min(run, axis=0, keepdims=True),
        jnp.sum(cosine * run, axis=0, keepdims=True),
        jnp.sum(cosine * run * run, axis=0, keepdims=True),
        jnp.sum(cosine * want, axis=0, keepdims=True),
        jnp.sum(cosine * run * want, axis=0, keepdims=True),
        jnp.sum(cosine * want * want, axis=0, keepdims=True),
    )
    for p in range(s_ref.shape[0]):
        for i, stat in enumerate(stats):
            s_ref[p, i : i + 1, :] = stat
    w_ref[0:span, :] = run
    for p in range(peers):

        @pl.when(place_ref[0] % 8 == p)
        def _():
            mine_ref[...] = w_ref[p * rows : (p + 1) * rows, :]


def add_block(so_far, block, weight):
    s, hi, lo, run1, run2, want1, cross, want2 = block
    if so_far is None:
        return block
    off = so_far[0]
    return (
        off + s,
        jnp.maximum(so_far[1], off + hi),
        jnp.minimum(so_far[2], off + lo),
        so_far[3] + (run1 + off * weight),
        so_far[4] + (run2 + 2.0 * off * run1 + off * off * weight),
        so_far[5] + want1,
        so_far[6] + (cross + off * want1),
        so_far[7] + want2,
    )


def half_kernel(total, span, place_ref, mine_ref, s_ref, own_ref, half_ref):
    blocks = s_ref.shape[0]
    here = place_ref[0] % 64 // 8
    north = place_ref[0] // 128 == 1
    stats = None
    offset = jnp.zeros((1, s_ref.shape[2]), F32)
    for z in range(blocks):
        if z:
            offset = jnp.where(here == z, stats[0], offset)
        weights = [weight_of((h * blocks + z) * span, span, total) for h in range(2)]
        weight = jnp.where(north, weights[1], weights[0])
        stats = add_block(stats, [s_ref[z, i : i + 1, :] for i in range(8)], weight)
    own_ref[...] = mine_ref[...] + offset
    for i, stat in enumerate(stats):
        half_ref[i : i + 1, :] = stat


def finish_kernel(total, place_ref, own_ref, near_ref, far_ref, psi_ref, loss_ref):
    _, samples, levels = psi_ref.shape
    north = place_ref[0] // 128 == 1
    near = near_ref[...]
    far = far_ref[...]
    south_half = jnp.where(north, far, near)
    north_half = jnp.where(north, near, far)
    weight = weight_of(total // 2, total // 2, total)
    stats = add_block(
        [south_half[i : i + 1] for i in range(8)], [north_half[i : i + 1] for i in range(8)], weight
    )
    peak = jnp.max(jnp.maximum(jnp.abs(stats[1]), jnp.abs(stats[2])), axis=1, keepdims=True)
    scale = peak + EPSILON
    psi = (own_ref[...] + jnp.where(north, far[0:1], 0.0)) / scale
    for b in range(samples):
        psi_ref[:, b, :] = psi[:, b * levels : (b + 1) * levels]
    a, b, c = (jnp.sum(stats[i], axis=1, keepdims=True) for i in (4, 6, 7))
    loss = (a / scale / scale - 2.0 * (b / scale) + c) / (samples * levels * total)
    loss_ref[...] = jnp.broadcast_to(loss, loss_ref.shape)


def small(body, out_shape, *args, scratch=(), after=None):
    many = isinstance(out_shape, tuple)
    specs = [SMEM] + [VMEM] * (len(args) - 1)
    if after is not None:
        plain, count = body, len(args)
        body = lambda *refs: plain(*refs[:count], *refs[count + 1 :])
        args += (after,)
        specs.append(ANY)
    return pl.pallas_call(
        body,
        out_shape=out_shape,
        in_specs=specs,
        out_specs=(VMEM,) * len(out_shape) if many else VMEM,
        scratch_shapes=scratch,
        compiler_params=params(2),
    )(*args)


def all_of(x, axes):
    return lax.all_to_all(x, axes, split_axis=0, concat_axis=0, tiled=True)


def floats(*shape):
    return jax.ShapeDtypeStruct(shape, F32)


def per_device(u, v, t, mask, depth, desired):
    bands, samples, levels, lon = v.shape
    width = samples * levels
    total = bands * lax.axis_size(LAT_LEV)
    half = lax.axis_index("lon")[None].astype(jnp.int32)
    place = lax.axis_index(("lat", "lon", "lev_0", "lev_1", "lev_2"))[None].astype(jnp.int32)
    across = [(0, 1), (1, 0)]
    table = jnp.asarray(half_table(lon), BF16)

    def swap(x):
        return lax.ppermute(x, "lon", across)

    first = pack(half, u, v, t, mask, GROUPS[0], True)
    *packed, sums = send(half, u, v, t, mask, first, GROUPS)
    rest, own = packed[: len(GROUPS) - 1], packed[len(GROUPS) - 1 :]
    got = [swap(first)]
    by_lon = swap(sums)
    got += [swap(x) for x in rest]

    def both(g, after):
        far = waves(half, table, own[g], got[g], after, True, BF16)
        return far, waves(half, table, own[g], got[g], far, False, F32)

    peers = lax.axis_size(INNER)
    outer = lax.axis_size("lev_0")
    rows = small(
        lambda *refs: weigh_kernel(total, *refs),
        floats(peers, 16, width),
        place,
        sums,
        by_lon,
        depth[None],
        desired,
    )
    near_bands = all_of(rows, INNER)
    far0, near0 = both(0, rows)
    span = bands * peers
    mine, stats = small(
        lambda *refs: band_kernel(total, bands, levels, *refs),
        (floats(bands, width), floats(outer, 8, width)),
        place,
        near_bands,
        scratch=[pltpu.VMEM((2 * span, width), F32)],
        after=near0,
    )
    all_stats = all_of(stats, "lev_0")
    far1, near1 = both(1, stats)
    mine, near_half = small(
        lambda *refs: half_kernel(total, span, *refs),
        (floats(bands, width), floats(8, width)),
        place,
        mine,
        all_stats,
        after=near1,
    )
    far_half = lax.ppermute(near_half, "lat", across)
    far2, near2 = both(2, near_half)
    psi, loss = small(
        lambda *refs: finish_kernel(total, *refs),
        (floats(bands, samples, levels), floats(1, width)),
        place,
        mine,
        near_half,
        far_half,
        after=near2,
    )

    back = [swap(x) for x in (far0, far1, far2)]
    kept = [near0, near1, near2]
    outs = join(half, kept[:2], back[:2], None, GROUPS[0] + GROUPS[1], bands)
    outs = join(half, kept[2:], back[2:], outs, GROUPS[2], bands)
    heat, momentum = (jnp.transpose(x, (1, 0, 2)) for x in outs)
    return psi, heat, momentum, loss[0, 0]


def solution(mesh):
    torus = Mesh(
        mesh.devices.reshape(mesh.shape["lat"], mesh.shape["lon"], 8, 4, 2),
        ("lat", "lon", "lev_0", "lev_1", "lev_2"),
    )
    in_specs = (
        P(LAT_LEV, None, None, "lon"),
        P(LAT_LEV, None, None, "lon"),
        P(LAT_LEV, None, None, "lon"),
        P(LAT_LEV, None, "lon"),
        P(),
        P(LAT_LEV, None, None),
    )
    out_specs = (P(LAT_LEV, None, None), P("lon", LAT_LEV, None), P("lon", LAT_LEV, None), P())

    return jax.shard_map(
        per_device, mesh=torus, in_specs=in_specs, out_specs=out_specs, check_vma=False
    )
```

```python
import functools
import math

import jax
import jax.numpy as jnp
import numpy as np
from jax import lax
from jax.experimental import pallas as pl
from jax.experimental.pallas import tpu as pltpu
from jax.sharding import Mesh
from jax.sharding import PartitionSpec as P


MERIDIANS = 1440
ORDERS = 720
LAT_LEV = ("lat", "lev_0", "lev_1", "lev_2")
INNER = ("lev_1", "lev_2")
OUTER = ("lat", "lev_0")
EPSILON = 1e-06
GROUPS = ((0,), (1, 2), (3, 4))
F32 = jnp.float32
BF16 = jnp.bfloat16
MIB = 1024 * 1024
CONTRACT = (((1,), (1,)), ((), ()))
SMEM = pl.BlockSpec(memory_space=pltpu.SMEM)
VMEM = pl.BlockSpec(memory_space=pltpu.VMEM)
HBM = pl.BlockSpec(memory_space=pltpu.HBM)
ANY = pl.BlockSpec(memory_space=pl.ANY)


def half_table(lon):
    order = np.arange(1, ORDERS + 1, dtype=np.int64)
    turns = (order[:, None] * np.arange(lon, dtype=np.int64)[None, :]) % MERIDIANS
    angle = turns.astype(np.float32) * np.float32(2.0 * math.pi / MERIDIANS)
    both = np.stack([np.cos(angle), np.sin(angle)]).reshape(2, 2, ORDERS // 2, lon)
    return np.ascontiguousarray(both.transpose(1, 0, 2, 3)).reshape(2, ORDERS, lon)


def params(mib):
    return pltpu.CompilerParams(vmem_limit_bytes=mib * MIB)


def keep_of(mask):
    return mask.astype(F32).astype(BF16)


def pack_kernel(rows, flip, half_ref, u_ref, v_ref, t_ref, m_ref, o_ref, fields, masks, sems):
    part = fields.shape[2]
    half = 1 - half_ref[0] if flip else half_ref[0]
    copies = []
    for i, row in enumerate(rows):
        group = [pltpu.make_async_copy(m_ref.at[row], masks.at[i], sems.at[i, 3])]
        for f, ref in enumerate((t_ref, u_ref, v_ref)):
            group.append(
                pltpu.make_async_copy(
                    ref.at[row, pl.ds(half * part, part)], fields.at[i, f], sems.at[i, f]
                )
            )
        for c in group:
            c.start()
        copies.append(group)
    size = part * fields.shape[3]
    for i, group in enumerate(copies):
        for c in group:
            c.wait()
        keep = keep_of(masks[i])[None]
        for f in range(3):
            o_ref[i, f * size : (f + 1) * size, :] = (fields[i, f] * keep).reshape(size, -1)


def pack(half, u, v, t, mask, rows, flip):
    _, samples, levels, lon = u.shape
    part = samples // 2
    n = len(rows)
    return pl.pallas_call(
        lambda *refs: pack_kernel(rows, flip, *refs),
        out_shape=jax.ShapeDtypeStruct((n, 3 * part * levels, lon), BF16),
        in_specs=[SMEM, HBM, HBM, HBM, HBM],
        out_specs=VMEM,
        scratch_shapes=[
            pltpu.VMEM((n, 3, part, levels, lon), BF16),
            pltpu.VMEM((n, levels, lon), jnp.int32),
            pltpu.SemaphoreType.DMA((n, 4)),
        ],
        compiler_params=params(60),
        name="pack",
    )(half, u, v, t, mask)


def send_kernel(groups, half_ref, u_ref, v_ref, t_ref, m_ref, _, *rest):
    n = len(groups)
    far_refs, near_refs, sums_ref = rest[: n - 1], rest[n - 1 : 2 * n - 1], rest[2 * n - 1]
    us, vs, ts, masks, fars, nears, sems, out_sems = rest[2 * n :]
    rows, samples, levels, lon = vs.shape
    part = samples // 2
    size = part * levels
    near = half_ref[0]
    far = 1 - near
    copies = []
    for j in range(rows):
        group = [
            pltpu.make_async_copy(m_ref.at[j], masks.at[j], sems.at[j, 0]),
            pltpu.make_async_copy(v_ref.at[j], vs.at[j], sems.at[j, 1]),
            pltpu.make_async_copy(u_ref.at[j], us.at[j], sems.at[j, 2]),
            pltpu.make_async_copy(t_ref.at[j], ts.at[j], sems.at[j, 3]),
        ]
        for c in group:
            c.start()
        copies.append(group)
    ones = jnp.ones((8, lon), BF16)
    done = []
    for g, group in enumerate(groups):
        for i, j in enumerate(group):
            for c in copies[j]:
                c.wait()
            keep = keep_of(masks[j])
            v = (vs[j] * keep[None]).reshape(samples * levels, lon)
            sums_ref[j : j + 1, :] = lax.dot_general(
                ones, v, CONTRACT, preferred_element_type=F32
            )[0:1]
            full = jnp.broadcast_to(keep[None], (samples, levels, lon)).reshape(-1, lon)
            sums_ref[rows + j : rows + j + 1, :] = lax.dot_general(
                ones, full, CONTRACT, preferred_element_type=F32
            )[0:1]
            for k, (where, box) in enumerate(((far, fars), (near, nears))):
                if k == 0 and g == 0:
                    continue
                ref = far_refs[g - 1] if k == 0 else near_refs[g]
                for f, field in enumerate((ts, us, vs)):
                    mine = field[j, pl.ds(where * part, part)] * keep[None]
                    box[j, f * size : (f + 1) * size, :] = mine.reshape(size, lon)
                c = pltpu.make_async_copy(box.at[j], ref.at[i], out_sems.at[j, k])
                c.start()
                done.append(c)
    for c in done:
        c.wait()


def send(half, u, v, t, mask, after, groups):
    rows, samples, levels, lon = v.shape
    part = samples // 2
    unit = 3 * part * levels
    n = len(groups)
    packed = [jax.ShapeDtypeStruct((len(g), unit, lon), BF16) for g in groups]
    return pl.pallas_call(
        lambda *refs: send_kernel(groups, *refs),
        out_shape=(
            *packed[1:],
            *packed,
            jax.ShapeDtypeStruct((2 * rows, samples * levels), F32),
        ),
        in_specs=[SMEM, HBM, HBM, HBM, HBM, ANY],
        out_specs=(HBM,) * (2 * n - 1) + (VMEM,),
        scratch_shapes=[
            pltpu.VMEM((rows, samples, levels, lon), BF16),
            pltpu.VMEM((rows, samples, levels, lon), BF16),
            pltpu.VMEM((rows, samples, levels, lon), BF16),
            pltpu.VMEM((rows, levels, lon), jnp.int32),
            pltpu.VMEM((rows, unit, lon), BF16),
            pltpu.VMEM((rows, unit, lon), BF16),
            pltpu.SemaphoreType.DMA((rows, 4)),
            pltpu.SemaphoreType.DMA((rows, 2)),
        ],
        compiler_params=params(60),
        name="send",
    )(half, u, v, t, mask, after)


def wave_kernel(half_ref, table_ref, own_ref, got_ref, _, *o_refs, flips):
    def lay(x):
        return jnp.concatenate([x, x[2 * x.shape[0] // 3 :]])

    n = table_ref.shape[1] // 2
    odd = lax.broadcasted_iota(jnp.int32, (n, 1), 0) % 2 == 0
    sign = jnp.where(odd, -1.0, 1.0).astype(F32)
    scale = 2.0 / (MERIDIANS * MERIDIANS)
    for flip, o_ref in zip(flips, o_refs):
        table = table_ref[1 - half_ref[0] if flip else half_ref[0]]
        for i in range(got_ref.shape[0]):
            near = lax.dot_general(table, lay(own_ref[i]), CONTRACT, preferred_element_type=F32)
            far = lax.dot_general(table, lay(got_ref[i]), CONTRACT, preferred_element_type=F32)
            cos = near[:n] + sign * far[:n]
            sin = near[n:] + sign * far[n:]
            w = cos.shape[1] // 2
            both = cos[:, :w] * cos[:, w:] + sin[:, :w] * sin[:, w:]
            o_ref[i] = (scale * both).astype(o_ref.dtype)


def waves(half, table, own, got, after, *flips):
    rows, cols, _ = got.shape
    shape = (rows, table.shape[1] // 2, 2 * cols // 3)
    return pl.pallas_call(
        functools.partial(wave_kernel, flips=flips),
        out_shape=tuple(jax.ShapeDtypeStruct(shape, BF16 if f else F32) for f in flips),
        in_specs=[SMEM, VMEM, VMEM, VMEM, ANY],
        out_specs=(VMEM,) * len(flips),
        compiler_params=params(16),
        name="waves",
    )(half, table, own, got, after)


def join_kernel(first, parts, half_ref, *refs):
    own_refs, got_refs = refs[:parts], refs[parts : 2 * parts]
    heat_ref, mom_ref, heat, mom, sems = refs[-5:]
    copies = []
    at = 0
    for own_ref, got_ref in zip(own_refs, got_refs):
        for i in range(own_ref.shape[0]):
            own = own_ref[i]
            got = got_ref[i].astype(F32)
            zero = half_ref[0] == 0
            a = jnp.where(zero, own, got)
            b = jnp.where(zero, got, own)
            w = own.shape[1] // 2
            low = lax.broadcasted_iota(jnp.int32, own.shape, 1) < w
            heat[at] = jnp.where(low, a, pltpu.roll(b, w, 1))
            mom[at] = jnp.where(low, pltpu.roll(a, w, 1), b)
            for k, (x, ref) in enumerate(((heat, heat_ref), (mom, mom_ref))):
                c = pltpu.make_async_copy(x.at[at], ref.at[first + at], sems.at[at, k])
                c.start()
                copies.append(c)
            at += 1
    for c in copies:
        c.wait()


def join(half, own, got, outs, rows, total):
    n, width = own[0].shape[1:]
    shape = jax.ShapeDtypeStruct((total, n, width), F32)
    parts = len(own)
    args = (half, *own, *got)
    specs = [SMEM] + [VMEM] * (2 * parts)
    extra = {}
    if outs is not None:
        extra = {"input_output_aliases": {len(args): 0, len(args) + 1: 1}}
        args += outs
        specs += [HBM, HBM]
    return pl.pallas_call(
        lambda *refs: join_kernel(rows[0], parts, *refs),
        out_shape=(shape, shape),
        in_specs=specs,
        out_specs=(HBM, HBM),
        scratch_shapes=[
            pltpu.VMEM((len(rows), n, width), F32),
            pltpu.VMEM((len(rows), n, width), F32),
            pltpu.SemaphoreType.DMA((len(rows), 2)),
        ],
        compiler_params=params(8),
        name="join",
        **extra,
    )(*args)


def cosines(first, rows, total):
    index = lax.broadcasted_iota(jnp.int32, (rows, 1), 0) + first
    return jnp.cos(((index.astype(F32) + 0.5) / total - 0.5) * math.pi)


def weight_of(first, rows, total):
    latitude = ((np.arange(first, first + rows) + 0.5) / total - 0.5) * math.pi
    return float(np.sum(np.cos(latitude)))


def weigh_kernel(total, place_ref, own_ref, lon_ref, depth_ref, d_ref, o_ref):
    rows, samples, levels = d_ref.shape
    band = place_ref[0] // 128 * 64 + place_ref[0] % 64
    depth = depth_ref[...]
    spread = jnp.concatenate([depth] * samples, axis=1)
    kept = own_ref[rows : 2 * rows] + lon_ref[rows : 2 * rows]
    mean = (own_ref[0:rows] + lon_ref[0:rows]) / jnp.maximum(kept, 1.0)
    weighted = mean * cosines(band * rows, rows, total) * spread
    for p in range(o_ref.shape[0]):
        o_ref[p, 0:rows, :] = weighted
        for b in range(samples):
            o_ref[p, 8 : 8 + rows, b * levels : (b + 1) * levels] = d_ref[:, b, :]


def band_kernel(total, rows, levels, place_ref, g_ref, mine_ref, s_ref, w_ref):
    peers, _, width = g_ref.shape
    span = peers * rows
    lane = lax.broadcasted_iota(jnp.int32, (1, width), 1) % levels
    so_far = jnp.zeros((1, width), F32)
    for p in range(peers):
        for r in range(rows):
            so_far = so_far + g_ref[p, r : r + 1, :]
            w_ref[p * rows + r : p * rows + r + 1, :] = so_far
            w_ref[span + p * rows + r : span + p * rows + r + 1, :] = g_ref[p, 8 + r : 9 + r, :]
    run = w_ref[0:span, :]
    step = 1
    while step < levels:
        run = run + jnp.where(lane >= step, pltpu.roll(run, step, 1), 0.0)
        step *= 2
    want = w_ref[span:, :]
    block = place_ref[0] // 128 * 8 + place_ref[0] % 64 // 8
    cosine = cosines(block * span, span, total)
    stats = (
        run[span - 1 : span],
        jnp.max(run, axis=0, keepdims=True),
        jnp.min(run, axis=0, keepdims=True),
        jnp.sum(cosine * run, axis=0, keepdims=True),
        jnp.sum(cosine * run * run, axis=0, keepdims=True),
        jnp.sum(cosine * want, axis=0, keepdims=True),
        jnp.sum(cosine * run * want, axis=0, keepdims=True),
        jnp.sum(cosine * want * want, axis=0, keepdims=True),
    )
    for p in range(s_ref.shape[0]):
        for i, stat in enumerate(stats):
            s_ref[p, i : i + 1, :] = stat
    w_ref[0:span, :] = run
    for p in range(peers):

        @pl.when(place_ref[0] % 8 == p)
        def _():
            mine_ref[...] = w_ref[p * rows : (p + 1) * rows, :]


def add_block(so_far, block, weight):
    s, hi, lo, run1, run2, want1, cross, want2 = block
    if so_far is None:
        return block
    off = so_far[0]
    return (
        off + s,
        jnp.maximum(so_far[1], off + hi),
        jnp.minimum(so_far[2], off + lo),
        so_far[3] + (run1 + off * weight),
        so_far[4] + (run2 + 2.0 * off * run1 + off * off * weight),
        so_far[5] + want1,
        so_far[6] + (cross + off * want1),
        so_far[7] + want2,
    )


def finish_kernel(total, span, place_ref, mine_ref, s_ref, psi_ref, loss_ref):
    _, samples, levels = psi_ref.shape
    blocks = s_ref.shape[0]
    here = place_ref[0] // 128 * (blocks // 2) + place_ref[0] % 64 // 8
    stats = None
    offset = jnp.zeros((1, s_ref.shape[2]), F32)
    for z in range(blocks):
        if z:
            offset = jnp.where(here == z, stats[0], offset)
        stats = add_block(
            stats, [s_ref[z, i : i + 1, :] for i in range(8)], weight_of(z * span, span, total)
        )
    peak = jnp.max(jnp.maximum(jnp.abs(stats[1]), jnp.abs(stats[2])), axis=1, keepdims=True)
    scale = peak + EPSILON
    psi = (mine_ref[...] + offset) / scale
    for b in range(samples):
        psi_ref[:, b, :] = psi[:, b * levels : (b + 1) * levels]
    a, b, c = (jnp.sum(stats[i], axis=1, keepdims=True) for i in (4, 6, 7))
    loss = (a / scale / scale - 2.0 * (b / scale) + c) / (samples * levels * total)
    loss_ref[...] = jnp.broadcast_to(loss, loss_ref.shape)


def small(body, out_shape, *args, scratch=(), after=None):
    many = isinstance(out_shape, tuple)
    specs = [SMEM] + [VMEM] * (len(args) - 1)
    if after is not None:
        plain, count = body, len(args)
        body = lambda *refs: plain(*refs[:count], *refs[count + 1 :])
        args += (after,)
        specs.append(ANY)
    return pl.pallas_call(
        body,
        out_shape=out_shape,
        in_specs=specs,
        out_specs=(VMEM,) * len(out_shape) if many else VMEM,
        scratch_shapes=scratch,
        compiler_params=params(2),
    )(*args)


def all_of(x, axes):
    return lax.all_to_all(x, axes, split_axis=0, concat_axis=0, tiled=True)


def floats(*shape):
    return jax.ShapeDtypeStruct(shape, F32)


def per_device(u, v, t, mask, depth, desired):
    bands, samples, levels, lon = v.shape
    width = samples * levels
    total = bands * lax.axis_size(LAT_LEV)
    half = lax.axis_index("lon")[None].astype(jnp.int32)
    place = lax.axis_index(("lat", "lon", "lev_0", "lev_1", "lev_2"))[None].astype(jnp.int32)
    across = [(0, 1), (1, 0)]
    table = jnp.asarray(half_table(lon), BF16)

    def swap(x):
        return lax.ppermute(x, "lon", across)

    first = pack(half, u, v, t, mask, GROUPS[0], True)
    *packed, sums = send(half, u, v, t, mask, first, GROUPS)
    rest, own = packed[: len(GROUPS) - 1], packed[len(GROUPS) - 1 :]
    got = [swap(first)]
    by_lon = swap(sums)
    got += [swap(x) for x in rest]

    peers = lax.axis_size(INNER)
    outer = lax.axis_size(OUTER)
    rows = small(
        lambda *refs: weigh_kernel(total, *refs),
        floats(peers, 16, width),
        place,
        sums,
        by_lon,
        depth[None],
        desired,
    )
    near_bands = all_of(rows, INNER)
    far0, near0 = waves(half, table, own[0], got[0], rows, True, False)
    far1, near1 = waves(half, table, own[1], got[1], near0, True, False)
    span = bands * peers
    mine, stats = small(
        lambda *refs: band_kernel(total, bands, levels, *refs),
        (floats(bands, width), floats(outer, 8, width)),
        place,
        near_bands,
        scratch=[pltpu.VMEM((2 * span, width), F32)],
        after=near1,
    )
    all_stats = all_of(stats, OUTER)
    (far2,) = waves(half, table, own[2], got[2], stats, True)
    (near2,) = waves(half, table, own[2], got[2], stats, False)
    psi, loss = small(
        lambda *refs: finish_kernel(total, span, *refs),
        (floats(bands, samples, levels), floats(1, width)),
        place,
        mine,
        all_stats,
        after=near2,
    )

    back = [swap(x) for x in (far0, far1, far2)]
    kept = [near0, near1, near2]
    outs = join(half, kept[:2], back[:2], None, GROUPS[0] + GROUPS[1], bands)
    outs = join(half, kept[2:], back[2:], outs, GROUPS[2], bands)
    heat, momentum = (jnp.transpose(x, (1, 0, 2)) for x in outs)
    return psi, heat, momentum, loss[0, 0]


def solution(mesh):
    torus = Mesh(
        mesh.devices.reshape(mesh.shape["lat"], mesh.shape["lon"], 8, 4, 2),
        ("lat", "lon", "lev_0", "lev_1", "lev_2"),
    )
    in_specs = (
        P(LAT_LEV, None, None, "lon"),
        P(LAT_LEV, None, None, "lon"),
        P(LAT_LEV, None, None, "lon"),
        P(LAT_LEV, None, "lon"),
        P(),
        P(LAT_LEV, None, None),
    )
    out_specs = (P(LAT_LEV, None, None), P("lon", LAT_LEV, None), P("lon", LAT_LEV, None), P())

    return jax.shard_map(
        per_device, mesh=torus, in_specs=in_specs, out_specs=out_specs, check_vma=False
    )
```

```python
import functools
import math

import jax
import jax.numpy as jnp
import numpy as np
from jax import lax
from jax.experimental import pallas as pl
from jax.experimental.pallas import tpu as pltpu
from jax.sharding import Mesh
from jax.sharding import PartitionSpec as P


MERIDIANS = 1440
ORDERS = 720
LAT_LEV = ("lat", "lev_0", "lev_1", "lev_2")
INNER = ("lev_1", "lev_2")
OUTER = "lev_0"
EPSILON = 1e-06
GROUPS = ((0,), (1, 2), (3, 4))
F32 = jnp.float32
BF16 = jnp.bfloat16
MIB = 1024 * 1024
CONTRACT = (((1,), (1,)), ((), ()))
SMEM = pl.BlockSpec(memory_space=pltpu.SMEM)
VMEM = pl.BlockSpec(memory_space=pltpu.VMEM)
HBM = pl.BlockSpec(memory_space=pltpu.HBM)
ANY = pl.BlockSpec(memory_space=pl.ANY)


def half_table(lon):
    order = np.arange(1, ORDERS + 1, dtype=np.int64)
    turns = (order[:, None] * np.arange(lon, dtype=np.int64)[None, :]) % MERIDIANS
    angle = turns.astype(np.float32) * np.float32(2.0 * math.pi / MERIDIANS)
    both = np.stack([np.cos(angle), np.sin(angle)]).reshape(2, 2, ORDERS // 2, lon)
    return np.ascontiguousarray(both.transpose(1, 0, 2, 3)).reshape(2, ORDERS, lon)


def params(mib):
    return pltpu.CompilerParams(vmem_limit_bytes=mib * MIB)


def keep_of(mask):
    return mask.astype(F32).astype(BF16)


def pack_kernel(rows, flip, half_ref, u_ref, v_ref, t_ref, m_ref, o_ref, fields, masks, sems):
    part = fields.shape[2]
    half = 1 - half_ref[0] if flip else half_ref[0]
    copies = []
    for i, row in enumerate(rows):
        group = [pltpu.make_async_copy(m_ref.at[row], masks.at[i], sems.at[i, 3])]
        for f, ref in enumerate((t_ref, u_ref, v_ref)):
            group.append(
                pltpu.make_async_copy(
                    ref.at[row, pl.ds(half * part, part)], fields.at[i, f], sems.at[i, f]
                )
            )
        for c in group:
            c.start()
        copies.append(group)
    size = part * fields.shape[3]
    for i, group in enumerate(copies):
        for c in group:
            c.wait()
        keep = keep_of(masks[i])[None]
        for f in range(3):
            o_ref[i, f * size : (f + 1) * size, :] = (fields[i, f] * keep).reshape(size, -1)


def pack(half, u, v, t, mask, rows, flip):
    _, samples, levels, lon = u.shape
    part = samples // 2
    n = len(rows)
    return pl.pallas_call(
        lambda *refs: pack_kernel(rows, flip, *refs),
        out_shape=jax.ShapeDtypeStruct((n, 3 * part * levels, lon), BF16),
        in_specs=[SMEM, HBM, HBM, HBM, HBM],
        out_specs=VMEM,
        scratch_shapes=[
            pltpu.VMEM((n, 3, part, levels, lon), BF16),
            pltpu.VMEM((n, levels, lon), jnp.int32),
            pltpu.SemaphoreType.DMA((n, 4)),
        ],
        compiler_params=params(60),
        name="pack",
    )(half, u, v, t, mask)


def send_kernel(groups, half_ref, u_ref, v_ref, t_ref, m_ref, _, *rest):
    n = len(groups)
    far_refs, near_refs, sums_ref = rest[: n - 1], rest[n - 1 : 2 * n - 1], rest[2 * n - 1]
    us, vs, ts, masks, fars, nears, sems, out_sems = rest[2 * n :]
    rows, samples, levels, lon = vs.shape
    part = samples // 2
    size = part * levels
    near = half_ref[0]
    far = 1 - near
    copies = []
    for j in range(rows):
        group = [
            pltpu.make_async_copy(m_ref.at[j], masks.at[j], sems.at[j, 0]),
            pltpu.make_async_copy(v_ref.at[j], vs.at[j], sems.at[j, 1]),
            pltpu.make_async_copy(u_ref.at[j], us.at[j], sems.at[j, 2]),
            pltpu.make_async_copy(t_ref.at[j], ts.at[j], sems.at[j, 3]),
        ]
        for c in group:
            c.start()
        copies.append(group)
    ones = jnp.ones((8, lon), BF16)
    done = []
    for g, group in enumerate(groups):
        for i, j in enumerate(group):
            for c in copies[j]:
                c.wait()
            keep = keep_of(masks[j])
            v = (vs[j] * keep[None]).reshape(samples * levels, lon)
            sums_ref[j : j + 1, :] = lax.dot_general(
                ones, v, CONTRACT, preferred_element_type=F32
            )[0:1]
            full = jnp.broadcast_to(keep[None], (samples, levels, lon)).reshape(-1, lon)
            sums_ref[rows + j : rows + j + 1, :] = lax.dot_general(
                ones, full, CONTRACT, preferred_element_type=F32
            )[0:1]
            for k, (where, box) in enumerate(((far, fars), (near, nears))):
                if k == 0 and g == 0:
                    continue
                ref = far_refs[g - 1] if k == 0 else near_refs[g]
                for f, field in enumerate((ts, us, vs)):
                    mine = field[j, pl.ds(where * part, part)] * keep[None]
                    box[j, f * size : (f + 1) * size, :] = mine.reshape(size, lon)
                c = pltpu.make_async_copy(box.at[j], ref.at[i], out_sems.at[j, k])
                c.start()
                done.append(c)
    for c in done:
        c.wait()


def send(half, u, v, t, mask, after, groups):
    rows, samples, levels, lon = v.shape
    part = samples // 2
    unit = 3 * part * levels
    n = len(groups)
    packed = [jax.ShapeDtypeStruct((len(g), unit, lon), BF16) for g in groups]
    return pl.pallas_call(
        lambda *refs: send_kernel(groups, *refs),
        out_shape=(
            *packed[1:],
            *packed,
            jax.ShapeDtypeStruct((2 * rows, samples * levels), F32),
        ),
        in_specs=[SMEM, HBM, HBM, HBM, HBM, ANY],
        out_specs=(HBM,) * (2 * n - 1) + (VMEM,),
        scratch_shapes=[
            pltpu.VMEM((rows, samples, levels, lon), BF16),
            pltpu.VMEM((rows, samples, levels, lon), BF16),
            pltpu.VMEM((rows, samples, levels, lon), BF16),
            pltpu.VMEM((rows, levels, lon), jnp.int32),
            pltpu.VMEM((rows, unit, lon), BF16),
            pltpu.VMEM((rows, unit, lon), BF16),
            pltpu.SemaphoreType.DMA((rows, 4)),
            pltpu.SemaphoreType.DMA((rows, 2)),
        ],
        compiler_params=params(60),
        name="send",
    )(half, u, v, t, mask, after)


def wave_kernel(half_ref, table_ref, own_ref, got_ref, _, *o_refs, flips):
    def lay(x):
        return jnp.concatenate([x, x[2 * x.shape[0] // 3 :]])

    n = table_ref.shape[1] // 2
    odd = lax.broadcasted_iota(jnp.int32, (n, 1), 0) % 2 == 0
    sign = jnp.where(odd, -1.0, 1.0).astype(F32)
    scale = 2.0 / (MERIDIANS * MERIDIANS)
    for flip, o_ref in zip(flips, o_refs):
        table = table_ref[1 - half_ref[0] if flip else half_ref[0]]
        for i in range(got_ref.shape[0]):
            near = lax.dot_general(table, lay(own_ref[i]), CONTRACT, preferred_element_type=F32)
            far = lax.dot_general(table, lay(got_ref[i]), CONTRACT, preferred_element_type=F32)
            cos = near[:n] + sign * far[:n]
            sin = near[n:] + sign * far[n:]
            w = cos.shape[1] // 2
            both = cos[:, :w] * cos[:, w:] + sin[:, :w] * sin[:, w:]
            o_ref[i] = (scale * both).astype(o_ref.dtype)


def waves(half, table, own, got, after, *flips):
    rows, cols, _ = got.shape
    shape = (rows, table.shape[1] // 2, 2 * cols // 3)
    return pl.pallas_call(
        functools.partial(wave_kernel, flips=flips),
        out_shape=tuple(jax.ShapeDtypeStruct(shape, BF16 if f else F32) for f in flips),
        in_specs=[SMEM, VMEM, VMEM, VMEM, ANY],
        out_specs=(VMEM,) * len(flips),
        compiler_params=params(16),
        name="waves",
    )(half, table, own, got, after)


def join_kernel(first, parts, half_ref, *refs):
    own_refs, got_refs = refs[:parts], refs[parts : 2 * parts]
    heat_ref, mom_ref, heat, mom, sems = refs[-5:]
    copies = []
    at = 0
    for own_ref, got_ref in zip(own_refs, got_refs):
        for i in range(own_ref.shape[0]):
            own = own_ref[i]
            got = got_ref[i].astype(F32)
            zero = half_ref[0] == 0
            a = jnp.where(zero, own, got)
            b = jnp.where(zero, got, own)
            w = own.shape[1] // 2
            low = lax.broadcasted_iota(jnp.int32, own.shape, 1) < w
            heat[at] = jnp.where(low, a, pltpu.roll(b, w, 1))
            mom[at] = jnp.where(low, pltpu.roll(a, w, 1), b)
            for k, (x, ref) in enumerate(((heat, heat_ref), (mom, mom_ref))):
                c = pltpu.make_async_copy(x.at[at], ref.at[first + at], sems.at[at, k])
                c.start()
                copies.append(c)
            at += 1
    for c in copies:
        c.wait()


def join(half, own, got, outs, rows, total):
    n, width = own[0].shape[1:]
    shape = jax.ShapeDtypeStruct((total, n, width), F32)
    parts = len(own)
    args = (half, *own, *got)
    specs = [SMEM] + [VMEM] * (2 * parts)
    extra = {}
    if outs is not None:
        extra = {"input_output_aliases": {len(args): 0, len(args) + 1: 1}}
        args += outs
        specs += [HBM, HBM]
    return pl.pallas_call(
        lambda *refs: join_kernel(rows[0], parts, *refs),
        out_shape=(shape, shape),
        in_specs=specs,
        out_specs=(HBM, HBM),
        scratch_shapes=[
            pltpu.VMEM((len(rows), n, width), F32),
            pltpu.VMEM((len(rows), n, width), F32),
            pltpu.SemaphoreType.DMA((len(rows), 2)),
        ],
        compiler_params=params(8),
        name="join",
        **extra,
    )(*args)


def cosines(first, rows, total):
    index = lax.broadcasted_iota(jnp.int32, (rows, 1), 0) + first
    return jnp.cos(((index.astype(F32) + 0.5) / total - 0.5) * math.pi)


def weight_of(first, rows, total):
    latitude = ((np.arange(first, first + rows) + 0.5) / total - 0.5) * math.pi
    return float(np.sum(np.cos(latitude)))


def weigh_kernel(total, place_ref, own_ref, lon_ref, depth_ref, d_ref, o_ref):
    rows, samples, levels = d_ref.shape
    band = place_ref[0] // 128 * 64 + place_ref[0] % 64
    depth = depth_ref[...]
    spread = jnp.concatenate([depth] * samples, axis=1)
    kept = own_ref[rows : 2 * rows] + lon_ref[rows : 2 * rows]
    mean = (own_ref[0:rows] + lon_ref[0:rows]) / jnp.maximum(kept, 1.0)
    weighted = mean * cosines(band * rows, rows, total) * spread
    for p in range(o_ref.shape[0]):
        o_ref[p, 0:rows, :] = weighted
        for b in range(samples):
            o_ref[p, 8 : 8 + rows, b * levels : (b + 1) * levels] = d_ref[:, b, :]


def band_kernel(total, rows, levels, place_ref, g_ref, mine_ref, s_ref, w_ref):
    peers, _, width = g_ref.shape
    span = peers * rows
    lane = lax.broadcasted_iota(jnp.int32, (1, width), 1) % levels
    so_far = jnp.zeros((1, width), F32)
    for p in range(peers):
        for r in range(rows):
            so_far = so_far + g_ref[p, r : r + 1, :]
            w_ref[p * rows + r : p * rows + r + 1, :] = so_far
            w_ref[span + p * rows + r : span + p * rows + r + 1, :] = g_ref[p, 8 + r : 9 + r, :]
    run = w_ref[0:span, :]
    step = 1
    while step < levels:
        run = run + jnp.where(lane >= step, pltpu.roll(run, step, 1), 0.0)
        step *= 2
    want = w_ref[span:, :]
    block = place_ref[0] // 128 * 8 + place_ref[0] % 64 // 8
    cosine = cosines(block * span, span, total)
    stats = (
        run[span - 1 : span],
        jnp.max(run, axis=0, keepdims=True),
        jnp.min(run, axis=0, keepdims=True),
        jnp.sum(cosine * run, axis=0, keepdims=True),
        jnp.sum(cosine * run * run, axis=0, keepdims=True),
        jnp.sum(cosine * want, axis=0, keepdims=True),
        jnp.sum(cosine * run * want, axis=0, keepdims=True),
        jnp.sum(cosine * want * want, axis=0, keepdims=True),
    )
    for p in range(s_ref.shape[0]):
        for i, stat in enumerate(stats):
            s_ref[p, i : i + 1, :] = stat
    w_ref[0:span, :] = run
    for p in range(peers):

        @pl.when(place_ref[0] % 8 == p)
        def _():
            mine_ref[...] = w_ref[p * rows : (p + 1) * rows, :]


def add_block(so_far, block, weight):
    s, hi, lo, run1, run2, want1, cross, want2 = block
    if so_far is None:
        return block
    off = so_far[0]
    return (
        off + s,
        jnp.maximum(so_far[1], off + hi),
        jnp.minimum(so_far[2], off + lo),
        so_far[3] + (run1 + off * weight),
        so_far[4] + (run2 + 2.0 * off * run1 + off * off * weight),
        so_far[5] + want1,
        so_far[6] + (cross + off * want1),
        so_far[7] + want2,
    )


def half_kernel(total, span, place_ref, mine_ref, s_ref, own_ref, half_ref):
    blocks = s_ref.shape[0]
    here = place_ref[0] % 64 // 8
    north = place_ref[0] // 128 == 1
    stats = None
    offset = jnp.zeros((1, s_ref.shape[2]), F32)
    for z in range(blocks):
        if z:
            offset = jnp.where(here == z, stats[0], offset)
        weights = [weight_of((h * blocks + z) * span, span, total) for h in range(2)]
        weight = jnp.where(north, weights[1], weights[0])
        stats = add_block(stats, [s_ref[z, i : i + 1, :] for i in range(8)], weight)
    own_ref[...] = mine_ref[...] + offset
    for i, stat in enumerate(stats):
        half_ref[i : i + 1, :] = stat


def finish_kernel(total, place_ref, own_ref, near_ref, far_ref, psi_ref, loss_ref):
    _, samples, levels = psi_ref.shape
    north = place_ref[0] // 128 == 1
    near = near_ref[...]
    far = far_ref[...]
    south_half = jnp.where(north, far, near)
    north_half = jnp.where(north, near, far)
    weight = weight_of(total // 2, total // 2, total)
    stats = add_block(
        [south_half[i : i + 1] for i in range(8)], [north_half[i : i + 1] for i in range(8)], weight
    )
    peak = jnp.max(jnp.maximum(jnp.abs(stats[1]), jnp.abs(stats[2])), axis=1, keepdims=True)
    scale = peak + EPSILON
    psi = (own_ref[...] + jnp.where(north, far[0:1], 0.0)) / scale
    for b in range(samples):
        psi_ref[:, b, :] = psi[:, b * levels : (b + 1) * levels]
    a, b, c = (jnp.sum(stats[i], axis=1, keepdims=True) for i in (4, 6, 7))
    loss = (a / scale / scale - 2.0 * (b / scale) + c) / (samples * levels * total)
    loss_ref[...] = jnp.broadcast_to(loss, loss_ref.shape)


def small(body, out_shape, *args, scratch=(), after=None):
    many = isinstance(out_shape, tuple)
    specs = [SMEM] + [VMEM] * (len(args) - 1)
    if after is not None:
        plain, count = body, len(args)
        body = lambda *refs: plain(*refs[:count], *refs[count + 1 :])
        args += (after,)
        specs.append(ANY)
    return pl.pallas_call(
        body,
        out_shape=out_shape,
        in_specs=specs,
        out_specs=(VMEM,) * len(out_shape) if many else VMEM,
        scratch_shapes=scratch,
        compiler_params=params(2),
    )(*args)


def all_of(x, axes):
    return lax.all_to_all(x, axes, split_axis=0, concat_axis=0, tiled=True)


def floats(*shape):
    return jax.ShapeDtypeStruct(shape, F32)


def per_device(u, v, t, mask, depth, desired):
    bands, samples, levels, lon = v.shape
    width = samples * levels
    total = bands * lax.axis_size(LAT_LEV)
    half = lax.axis_index("lon")[None].astype(jnp.int32)
    place = lax.axis_index(("lat", "lon", "lev_0", "lev_1", "lev_2"))[None].astype(jnp.int32)
    across = [(0, 1), (1, 0)]
    table = jnp.asarray(half_table(lon), BF16)

    def swap(x):
        return lax.ppermute(x, "lon", across)

    first = pack(half, u, v, t, mask, GROUPS[0], True)
    *packed, sums = send(half, u, v, t, mask, first, GROUPS)
    rest, own = packed[: len(GROUPS) - 1], packed[len(GROUPS) - 1 :]
    got = [swap(first)]
    by_lon = swap(sums)
    got += [swap(x) for x in rest]

    peers = lax.axis_size(INNER)
    outer = lax.axis_size(OUTER)
    rows = small(
        lambda *refs: weigh_kernel(total, *refs),
        floats(peers, 16, width),
        place,
        sums,
        by_lon,
        depth[None],
        desired,
    )
    near_bands = all_of(rows, INNER)
    far0, near0 = waves(half, table, own[0], got[0], rows, True, False)
    span = bands * peers
    mine, stats = small(
        lambda *refs: band_kernel(total, bands, levels, *refs),
        (floats(bands, width), floats(outer, 8, width)),
        place,
        near_bands,
        scratch=[pltpu.VMEM((2 * span, width), F32)],
    )
    all_stats = all_of(stats, OUTER)
    mine, near_half = small(
        lambda *refs: half_kernel(total, span, *refs),
        (floats(bands, width), floats(8, width)),
        place,
        mine,
        all_stats,
    )
    far_half = lax.ppermute(near_half, "lat", across)
    far1, near1 = waves(half, table, own[1], got[1], near_half, True, False)
    (far2,) = waves(half, table, own[2], got[2], near1, True)
    (near2,) = waves(half, table, own[2], got[2], near1, False)
    psi, loss = small(
        lambda *refs: finish_kernel(total, *refs),
        (floats(bands, samples, levels), floats(1, width)),
        place,
        mine,
        near_half,
        far_half,
        after=near2,
    )

    back = [swap(x) for x in (far0, far1, far2)]
    kept = [near0, near1, near2]
    outs = join(half, kept[:2], back[:2], None, GROUPS[0] + GROUPS[1], bands)
    outs = join(half, kept[2:], back[2:], outs, GROUPS[2], bands)
    heat, momentum = (jnp.transpose(x, (1, 0, 2)) for x in outs)
    return psi, heat, momentum, loss[0, 0]


def solution(mesh):
    torus = Mesh(
        mesh.devices.reshape(mesh.shape["lat"], mesh.shape["lon"], 8, 4, 2),
        ("lat", "lon", "lev_0", "lev_1", "lev_2"),
    )
    in_specs = (
        P(LAT_LEV, None, None, "lon"),
        P(LAT_LEV, None, None, "lon"),
        P(LAT_LEV, None, None, "lon"),
        P(LAT_LEV, None, "lon"),
        P(),
        P(LAT_LEV, None, None),
    )
    out_specs = (P(LAT_LEV, None, None), P("lon", LAT_LEV, None), P("lon", LAT_LEV, None), P())

    return jax.shard_map(
        per_device, mesh=torus, in_specs=in_specs, out_specs=out_specs, check_vma=False
    )
```

```python
import functools
import math

import jax
import jax.numpy as jnp
import numpy as np
from jax import lax
from jax.experimental import pallas as pl
from jax.experimental.pallas import tpu as pltpu
from jax.sharding import Mesh
from jax.sharding import PartitionSpec as P


MERIDIANS = 1440
ORDERS = 720
PADDED = 184
LAT_LEV = ("lat", "lev_0", "lev_1", "lev_2")
INNER = ("lev_1", "lev_2")
OUTER = "lev_0"
EPSILON = 1e-06
GROUPS = ((0,), (1, 2), (3, 4))
F32 = jnp.float32
BF16 = jnp.bfloat16
MIB = 1024 * 1024
CONTRACT = (((1,), (1,)), ((), ()))
SMEM = pl.BlockSpec(memory_space=pltpu.SMEM)
VMEM = pl.BlockSpec(memory_space=pltpu.VMEM)
HBM = pl.BlockSpec(memory_space=pltpu.HBM)
ANY = pl.BlockSpec(memory_space=pl.ANY)


def half_table(lon):
    order = np.arange(1, ORDERS + 1, dtype=np.int64)
    turns = (order[:, None] * np.arange(lon, dtype=np.int64)[None, :]) % MERIDIANS
    angle = turns.astype(np.float32) * np.float32(2.0 * math.pi / MERIDIANS)
    both = np.stack([np.cos(angle), np.sin(angle)]).reshape(2, 2, ORDERS // 4, 2, lon)
    rows = np.zeros((2, 2, 2, PADDED, lon), np.float32)
    rows[:, :, :, : ORDERS // 4] = both.transpose(1, 3, 0, 2, 4)
    return rows.reshape(2, 2, 2 * PADDED, lon)


def params(mib):
    return pltpu.CompilerParams(vmem_limit_bytes=mib * MIB)


def keep_of(mask):
    return mask.astype(F32).astype(BF16)


def first_kernel(half_ref, u_ref, v_ref, t_ref, m_ref, o_ref, sums_ref, us, vs, ts, masks, sems):
    rows, samples, levels, lon = vs.shape
    part = samples // 2
    size = part * levels
    far = 1 - half_ref[0]
    at = pl.ds(far * part, part)
    copies = []
    for j in range(rows):
        copies.append(
            [
                pltpu.make_async_copy(m_ref.at[j], masks.at[j], sems.at[j, 0]),
                pltpu.make_async_copy(v_ref.at[j], vs.at[j], sems.at[j, 1]),
            ]
        )
    extra = [
        pltpu.make_async_copy(u_ref.at[0, at], us, sems.at[0, 2]),
        pltpu.make_async_copy(t_ref.at[0, at], ts, sems.at[0, 3]),
    ]
    for group in (copies[0], extra, *copies[1:]):
        for c in group:
            c.start()
    ones = jnp.ones((8, lon), BF16)
    for j in range(rows):
        for c in copies[j]:
            c.wait()
        keep = keep_of(masks[j])
        v = (vs[j] * keep[None]).reshape(samples * levels, lon)
        sums_ref[j : j + 1, :] = lax.dot_general(ones, v, CONTRACT, preferred_element_type=F32)[0:1]
        full = jnp.broadcast_to(keep[None], (samples, levels, lon)).reshape(samples * levels, lon)
        sums_ref[rows + j : rows + j + 1, :] = lax.dot_general(
            ones, full, CONTRACT, preferred_element_type=F32
        )[0:1]
    for c in extra:
        c.wait()
    keep = keep_of(masks[0])[None]
    for f, field in enumerate((ts[...], us[...], vs[0, at])):
        o_ref[0, f * size : (f + 1) * size, :] = (field * keep).reshape(size, lon)


def first_part(half, u, v, t, mask):
    rows, samples, levels, lon = v.shape
    part = samples // 2
    return pl.pallas_call(
        first_kernel,
        out_shape=(
            jax.ShapeDtypeStruct((1, 3 * part * levels, lon), BF16),
            jax.ShapeDtypeStruct((2 * rows, samples * levels), F32),
        ),
        in_specs=[SMEM, HBM, HBM, HBM, HBM],
        out_specs=(VMEM, VMEM),
        scratch_shapes=[
            pltpu.VMEM((part, levels, lon), BF16),
            pltpu.VMEM((rows, samples, levels, lon), BF16),
            pltpu.VMEM((part, levels, lon), BF16),
            pltpu.VMEM((rows, levels, lon), jnp.int32),
            pltpu.SemaphoreType.DMA((rows, 4)),
        ],
        compiler_params=params(60),
        name="sums",
    )(half, u, v, t, mask)


def send_kernel(groups, half_ref, u_ref, v_ref, t_ref, m_ref, _, *rest):
    n = len(groups)
    far_refs, near_refs = rest[: n - 1], rest[n - 1 : 2 * n - 1]
    us, vs, ts, masks, fars, nears, sems, out_sems = rest[2 * n - 1 :]
    rows, samples, levels, lon = vs.shape
    part = samples // 2
    size = part * levels
    near = half_ref[0]
    far = 1 - near
    copies = []
    for j in range(rows):
        group = [
            pltpu.make_async_copy(m_ref.at[j], masks.at[j], sems.at[j, 0]),
            pltpu.make_async_copy(v_ref.at[j], vs.at[j], sems.at[j, 1]),
            pltpu.make_async_copy(u_ref.at[j], us.at[j], sems.at[j, 2]),
            pltpu.make_async_copy(t_ref.at[j], ts.at[j], sems.at[j, 3]),
        ]
        for c in group:
            c.start()
        copies.append(group)
    done = []
    for g, group in enumerate(groups):
        for i, j in enumerate(group):
            for c in copies[j]:
                c.wait()
            keep = keep_of(masks[j])
            for k, (where, box) in enumerate(((far, fars), (near, nears))):
                if k == 0 and g == 0:
                    continue
                ref = far_refs[g - 1] if k == 0 else near_refs[g]
                for f, field in enumerate((ts, us, vs)):
                    mine = field[j, pl.ds(where * part, part)] * keep[None]
                    box[j, f * size : (f + 1) * size, :] = mine.reshape(size, lon)
                c = pltpu.make_async_copy(box.at[j], ref.at[i], out_sems.at[j, k])
                c.start()
                done.append(c)
    for c in done:
        c.wait()


def send(half, u, v, t, mask, after, groups):
    rows, samples, levels, lon = v.shape
    part = samples // 2
    unit = 3 * part * levels
    n = len(groups)
    packed = [jax.ShapeDtypeStruct((len(g), unit, lon), BF16) for g in groups]
    return pl.pallas_call(
        lambda *refs: send_kernel(groups, *refs),
        out_shape=(
            *packed[1:],
            *packed,
        ),
        in_specs=[SMEM, HBM, HBM, HBM, HBM, ANY],
        out_specs=(HBM,) * (2 * n - 1),
        scratch_shapes=[
            pltpu.VMEM((rows, samples, levels, lon), BF16),
            pltpu.VMEM((rows, samples, levels, lon), BF16),
            pltpu.VMEM((rows, samples, levels, lon), BF16),
            pltpu.VMEM((rows, levels, lon), jnp.int32),
            pltpu.VMEM((rows, unit, lon), BF16),
            pltpu.VMEM((rows, unit, lon), BF16),
            pltpu.SemaphoreType.DMA((rows, 4)),
            pltpu.SemaphoreType.DMA((rows, 2)),
        ],
        compiler_params=params(60),
        name="send",
    )(half, u, v, t, mask, after)


def wave_kernel(half_ref, table_ref, own_ref, got_ref, _, *o_refs, flips):
    n = table_ref.shape[2] // 2
    scale = 2.0 / (MERIDIANS * MERIDIANS)
    for i in range(got_ref.shape[0]):
        own, got = own_ref[i].astype(F32), got_ref[i].astype(F32)
        for p, mixed in enumerate(((own - got).astype(BF16), (own + got).astype(BF16))):
            x = jnp.concatenate([mixed, mixed[2 * mixed.shape[0] // 3 :]])
            w = x.shape[0] // 2
            for flip, o_ref in zip(flips, o_refs):
                table = table_ref[1 - half_ref[0] if flip else half_ref[0], p]
                c = lax.dot_general(table, x, CONTRACT, preferred_element_type=F32)
                both = c[:n, :w] * c[:n, w:] + c[n:, :w] * c[n:, w:]
                o_ref[i, p] = (scale * both).astype(o_ref.dtype)


def waves(half, table, own, got, after, *flips):
    rows, cols, _ = got.shape
    shape = (rows, 2, PADDED, 2 * cols // 3)
    return pl.pallas_call(
        functools.partial(wave_kernel, flips=flips),
        out_shape=tuple(jax.ShapeDtypeStruct(shape, BF16 if f else F32) for f in flips),
        in_specs=[SMEM, VMEM, VMEM, VMEM, ANY],
        out_specs=(VMEM,) * len(flips),
        compiler_params=params(16),
        name="waves",
    )(half, table, own, got, after)


def stream_kernel(half_ref, table_ref, own_ref, got_ref, _, far_ref, near_ref, table, owns, gots, far, near, sems, table_sems, out_sems):
    units = owns.shape[0]
    n = table.shape[2] // 2
    scale = 2.0 / (MERIDIANS * MERIDIANS)
    fields = []
    for i in range(units):
        fields.append(
            [
                pltpu.make_async_copy(own_ref.at[i], owns.at[i], sems.at[i, 0]),
                pltpu.make_async_copy(got_ref.at[i], gots.at[i], sems.at[i, 1]),
            ]
        )
    blocks = {}
    for p in range(2):
        for side in range(2):
            which = half_ref[0] if side else 1 - half_ref[0]
            blocks[p, side] = pltpu.make_async_copy(
                table_ref.at[which, p], table.at[side, p], table_sems.at[side, p]
            )
    for c in (*fields[0], *blocks.values(), *(c for group in fields[1:] for c in group)):
        c.start()
    outs = []
    for i in range(units):
        for c in fields[i]:
            c.wait()
        own, got = owns[i].astype(F32), gots[i].astype(F32)
        for p, mixed in enumerate(((own - got).astype(BF16), (own + got).astype(BF16))):
            x = jnp.concatenate([mixed, mixed[2 * mixed.shape[0] // 3 :]])
            w = x.shape[0] // 2
            for side, box in enumerate((far, near)):
                if i == 0:
                    blocks[p, side].wait()
                c = lax.dot_general(table[side, p], x, CONTRACT, preferred_element_type=F32)
                both = c[:n, :w] * c[:n, w:] + c[n:, :w] * c[n:, w:]
                box[i, p] = (scale * both).astype(box.dtype)
        for side, (box, ref) in enumerate(((far, far_ref), (near, near_ref))):
            c = pltpu.make_async_copy(box.at[i], ref.at[i], out_sems.at[i, side])
            c.start()
            outs.append(c)
    for c in outs:
        c.wait()


def stream(half, table, own, got, after):
    rows, cols, lon = got.shape
    shape = (rows, 2, PADDED, 2 * cols // 3)
    return pl.pallas_call(
        stream_kernel,
        out_shape=(jax.ShapeDtypeStruct(shape, BF16), jax.ShapeDtypeStruct(shape, F32)),
        in_specs=[SMEM, HBM, HBM, HBM, ANY],
        out_specs=(HBM, HBM),
        scratch_shapes=[
            pltpu.VMEM(table.shape, BF16),
            pltpu.VMEM((rows, cols, lon), BF16),
            pltpu.VMEM((rows, cols, lon), BF16),
            pltpu.VMEM(shape, BF16),
            pltpu.VMEM(shape, F32),
            pltpu.SemaphoreType.DMA((rows, 2)),
            pltpu.SemaphoreType.DMA((2, 2)),
            pltpu.SemaphoreType.DMA((rows, 2)),
        ],
        compiler_params=params(60),
        name="stream",
    )(half, table, own, got, after)


def join_kernel(first, parts, half_ref, *refs):
    own_refs, got_refs = refs[:parts], refs[parts : 2 * parts]
    heat_ref, mom_ref, heat, mom, sems = refs[-5:]
    copies = []
    at = 0
    for own_ref, got_ref in zip(own_refs, got_refs):
        for i in range(own_ref.shape[0]):
            zero = half_ref[0] == 0
            for p in range(2):
                own = own_ref[i, p]
                got = got_ref[i, p].astype(F32)
                a = jnp.where(zero, own, got)
                b = jnp.where(zero, got, own)
                w = own.shape[1] // 2
                low = lax.broadcasted_iota(jnp.int32, own.shape, 1) < w
                n = heat.shape[1] // 2
                every = pl.ds(p, n, stride=2)
                heat[at, every, :] = jnp.where(low, a, pltpu.roll(b, w, 1))[:n]
                mom[at, every, :] = jnp.where(low, pltpu.roll(a, w, 1), b)[:n]
            for k, (x, ref) in enumerate(((heat, heat_ref), (mom, mom_ref))):
                c = pltpu.make_async_copy(x.at[at], ref.at[first + at], sems.at[at, k])
                c.start()
                copies.append(c)
            at += 1
    for c in copies:
        c.wait()


def join(half, own, got, outs, rows, total):
    n, width = ORDERS // 2, own[0].shape[3]
    shape = jax.ShapeDtypeStruct((total, n, width), F32)
    parts = len(own)
    args = (half, *own, *got)
    specs = [SMEM] + [VMEM] * (2 * parts)
    extra = {}
    if outs is not None:
        extra = {"input_output_aliases": {len(args): 0, len(args) + 1: 1}}
        args += outs
        specs += [HBM, HBM]
    return pl.pallas_call(
        lambda *refs: join_kernel(rows[0], parts, *refs),
        out_shape=(shape, shape),
        in_specs=specs,
        out_specs=(HBM, HBM),
        scratch_shapes=[
            pltpu.VMEM((len(rows), n, width), F32),
            pltpu.VMEM((len(rows), n, width), F32),
            pltpu.SemaphoreType.DMA((len(rows), 2)),
        ],
        compiler_params=params(8),
        name="join",
        **extra,
    )(*args)


def cosines(first, rows, total):
    index = lax.broadcasted_iota(jnp.int32, (rows, 1), 0) + first
    return jnp.cos(((index.astype(F32) + 0.5) / total - 0.5) * math.pi)


def weight_of(first, rows, total):
    latitude = ((np.arange(first, first + rows) + 0.5) / total - 0.5) * math.pi
    return float(np.sum(np.cos(latitude)))


def weigh_kernel(total, place_ref, own_ref, lon_ref, depth_ref, d_ref, o_ref):
    rows, samples, levels = d_ref.shape
    band = place_ref[0] // 128 * 64 + place_ref[0] % 64
    depth = depth_ref[...]
    spread = jnp.concatenate([depth] * samples, axis=1)
    kept = own_ref[rows : 2 * rows] + lon_ref[rows : 2 * rows]
    mean = (own_ref[0:rows] + lon_ref[0:rows]) / jnp.maximum(kept, 1.0)
    weighted = mean * cosines(band * rows, rows, total) * spread
    for p in range(o_ref.shape[0]):
        o_ref[p, 0:rows, :] = weighted
        for b in range(samples):
            o_ref[p, 8 : 8 + rows, b * levels : (b + 1) * levels] = d_ref[:, b, :]


def band_kernel(total, rows, levels, place_ref, g_ref, mine_ref, s_ref, w_ref):
    peers, _, width = g_ref.shape
    span = peers * rows
    lane = lax.broadcasted_iota(jnp.int32, (1, width), 1) % levels
    so_far = jnp.zeros((1, width), F32)
    for p in range(peers):
        for r in range(rows):
            so_far = so_far + g_ref[p, r : r + 1, :]
            w_ref[p * rows + r : p * rows + r + 1, :] = so_far
            w_ref[span + p * rows + r : span + p * rows + r + 1, :] = g_ref[p, 8 + r : 9 + r, :]
    run = w_ref[0:span, :]
    step = 1
    while step < levels:
        run = run + jnp.where(lane >= step, pltpu.roll(run, step, 1), 0.0)
        step *= 2
    want = w_ref[span:, :]
    block = place_ref[0] // 128 * 8 + place_ref[0] % 64 // 8
    cosine = cosines(block * span, span, total)
    stats = (
        run[span - 1 : span],
        jnp.max(run, axis=0, keepdims=True),
        jnp.min(run, axis=0, keepdims=True),
        jnp.sum(cosine * run, axis=0, keepdims=True),
        jnp.sum(cosine * run * run, axis=0, keepdims=True),
        jnp.sum(cosine * want, axis=0, keepdims=True),
        jnp.sum(cosine * run * want, axis=0, keepdims=True),
        jnp.sum(cosine * want * want, axis=0, keepdims=True),
    )
    for p in range(s_ref.shape[0]):
        for i, stat in enumerate(stats):
            s_ref[p, i : i + 1, :] = stat
    w_ref[0:span, :] = run
    for p in range(peers):

        @pl.when(place_ref[0] % 8 == p)
        def _():
            mine_ref[...] = w_ref[p * rows : (p + 1) * rows, :]


def add_block(so_far, block, weight):
    s, hi, lo, run1, run2, want1, cross, want2 = block
    if so_far is None:
        return block
    off = so_far[0]
    return (
        off + s,
        jnp.maximum(so_far[1], off + hi),
        jnp.minimum(so_far[2], off + lo),
        so_far[3] + (run1 + off * weight),
        so_far[4] + (run2 + 2.0 * off * run1 + off * off * weight),
        so_far[5] + want1,
        so_far[6] + (cross + off * want1),
        so_far[7] + want2,
    )


def half_kernel(total, span, place_ref, mine_ref, s_ref, own_ref, half_ref):
    blocks = s_ref.shape[0]
    here = place_ref[0] % 64 // 8
    north = place_ref[0] // 128 == 1
    stats = None
    offset = jnp.zeros((1, s_ref.shape[2]), F32)
    for z in range(blocks):
        if z:
            offset = jnp.where(here == z, stats[0], offset)
        weights = [weight_of((h * blocks + z) * span, span, total) for h in range(2)]
        weight = jnp.where(north, weights[1], weights[0])
        stats = add_block(stats, [s_ref[z, i : i + 1, :] for i in range(8)], weight)
    own_ref[...] = mine_ref[...] + offset
    for i, stat in enumerate(stats):
        half_ref[i : i + 1, :] = stat


def finish_kernel(total, place_ref, own_ref, near_ref, far_ref, psi_ref, loss_ref):
    _, samples, levels = psi_ref.shape
    north = place_ref[0] // 128 == 1
    near = near_ref[...]
    far = far_ref[...]
    south_half = jnp.where(north, far, near)
    north_half = jnp.where(north, near, far)
    weight = weight_of(total // 2, total // 2, total)
    stats = add_block(
        [south_half[i : i + 1] for i in range(8)], [north_half[i : i + 1] for i in range(8)], weight
    )
    peak = jnp.max(jnp.maximum(jnp.abs(stats[1]), jnp.abs(stats[2])), axis=1, keepdims=True)
    scale = peak + EPSILON
    psi = (own_ref[...] + jnp.where(north, far[0:1], 0.0)) / scale
    for b in range(samples):
        psi_ref[:, b, :] = psi[:, b * levels : (b + 1) * levels]
    a, b, c = (jnp.sum(stats[i], axis=1, keepdims=True) for i in (4, 6, 7))
    loss = (a / scale / scale - 2.0 * (b / scale) + c) / (samples * levels * total)
    loss_ref[...] = jnp.broadcast_to(loss, loss_ref.shape)


def small(body, out_shape, *args, scratch=(), after=None):
    many = isinstance(out_shape, tuple)
    specs = [SMEM] + [VMEM] * (len(args) - 1)
    if after is not None:
        plain, count = body, len(args)
        body = lambda *refs: plain(*refs[:count], *refs[count + 1 :])
        args += (after,)
        specs.append(ANY)
    return pl.pallas_call(
        body,
        out_shape=out_shape,
        in_specs=specs,
        out_specs=(VMEM,) * len(out_shape) if many else VMEM,
        scratch_shapes=scratch,
        compiler_params=params(2),
    )(*args)


def all_of(x, axes):
    return lax.all_to_all(x, axes, split_axis=0, concat_axis=0, tiled=True)


def floats(*shape):
    return jax.ShapeDtypeStruct(shape, F32)


def per_device(u, v, t, mask, depth, desired):
    bands, samples, levels, lon = v.shape
    width = samples * levels
    total = bands * lax.axis_size(LAT_LEV)
    half = lax.axis_index("lon")[None].astype(jnp.int32)
    place = lax.axis_index(("lat", "lon", "lev_0", "lev_1", "lev_2"))[None].astype(jnp.int32)
    across = [(0, 1), (1, 0)]
    table = jnp.asarray(half_table(lon), BF16)

    def swap(x):
        return lax.ppermute(x, "lon", across)

    first, sums = first_part(half, u, v, t, mask)
    packed = send(half, u, v, t, mask, sums, GROUPS)
    rest, own = packed[: len(GROUPS) - 1], packed[len(GROUPS) - 1 :]
    got = [swap(first)]
    by_lon = swap(sums)
    got += [swap(x) for x in rest]

    peers = lax.axis_size(INNER)
    outer = lax.axis_size(OUTER)
    rows = small(
        lambda *refs: weigh_kernel(total, *refs),
        floats(peers, 16, width),
        place,
        sums,
        by_lon,
        depth[None],
        desired,
    )
    near_bands = all_of(rows, INNER)
    far0, near0 = stream(half, table, own[0], got[0], rows)
    span = bands * peers
    mine, stats = small(
        lambda *refs: band_kernel(total, bands, levels, *refs),
        (floats(bands, width), floats(outer, 8, width)),
        place,
        near_bands,
        scratch=[pltpu.VMEM((2 * span, width), F32)],
    )
    all_stats = all_of(stats, OUTER)
    mine, near_half = small(
        lambda *refs: half_kernel(total, span, *refs),
        (floats(bands, width), floats(8, width)),
        place,
        mine,
        all_stats,
    )
    far_half = lax.ppermute(near_half, "lat", across)
    far1, near1 = stream(half, table, own[1], got[1], stats)
    (far2,) = waves(half, table, own[2], got[2], near_half, True)
    (near2,) = waves(half, table, own[2], got[2], near_half, False)
    psi, loss = small(
        lambda *refs: finish_kernel(total, *refs),
        (floats(bands, samples, levels), floats(1, width)),
        place,
        mine,
        near_half,
        far_half,
        after=near2,
    )

    back = [swap(x) for x in (far0, far1, far2)]
    kept = [near0, near1, near2]
    outs = None
    for group, mine, far in zip(GROUPS, kept, back):
        outs = join(half, [mine], [far], outs, group, bands)
    heat, momentum = (jnp.transpose(x, (1, 0, 2)) for x in outs)
    return psi, heat, momentum, loss[0, 0]


def solution(mesh):
    torus = Mesh(
        mesh.devices.reshape(mesh.shape["lat"], mesh.shape["lon"], 8, 4, 2),
        ("lat", "lon", "lev_0", "lev_1", "lev_2"),
    )
    in_specs = (
        P(LAT_LEV, None, None, "lon"),
        P(LAT_LEV, None, None, "lon"),
        P(LAT_LEV, None, None, "lon"),
        P(LAT_LEV, None, "lon"),
        P(),
        P(LAT_LEV, None, None),
    )
    out_specs = (P(LAT_LEV, None, None), P("lon", LAT_LEV, None), P("lon", LAT_LEV, None), P())

    return jax.shard_map(
        per_device, mesh=torus, in_specs=in_specs, out_specs=out_specs, check_vma=False
    )
```

```python
import functools
import math

import jax
import jax.numpy as jnp
import numpy as np
from jax import lax
from jax.experimental import pallas as pl
from jax.experimental.pallas import tpu as pltpu
from jax.sharding import Mesh
from jax.sharding import PartitionSpec as P


MERIDIANS = 1440
ORDERS = 720
PADDED = 184
LAT_LEV = ("lat", "lev_0", "lev_1", "lev_2")
INNER = ("lev_1", "lev_2")
OUTER = "lev_0"
EPSILON = 1e-06
GROUPS = ((0,), (1, 2), (3, 4))
F32 = jnp.float32
BF16 = jnp.bfloat16
MIB = 1024 * 1024
CONTRACT = (((1,), (1,)), ((), ()))
SMEM = pl.BlockSpec(memory_space=pltpu.SMEM)
VMEM = pl.BlockSpec(memory_space=pltpu.VMEM)
HBM = pl.BlockSpec(memory_space=pltpu.HBM)
ANY = pl.BlockSpec(memory_space=pl.ANY)


def half_table(lon):
    order = np.arange(1, ORDERS + 1, dtype=np.int64)
    turns = (order[:, None] * np.arange(lon, dtype=np.int64)[None, :]) % MERIDIANS
    angle = turns.astype(np.float32) * np.float32(2.0 * math.pi / MERIDIANS)
    both = np.stack([np.cos(angle), np.sin(angle)]).reshape(2, 2, ORDERS // 4, 2, lon)
    rows = np.zeros((2, 2, 2, PADDED, lon), np.float32)
    rows[:, :, :, : ORDERS // 4] = both.transpose(1, 3, 0, 2, 4)
    return rows.reshape(2, 2, 2 * PADDED, lon)


def params(mib):
    return pltpu.CompilerParams(vmem_limit_bytes=mib * MIB)


def keep_of(mask):
    return mask.astype(F32).astype(BF16)


def first_kernel(half_ref, u_ref, v_ref, t_ref, m_ref, o_ref, sums_ref, us, vs, ts, masks, sems):
    rows, samples, levels, lon = vs.shape
    part = samples // 2
    size = part * levels
    far = 1 - half_ref[0]
    at = pl.ds(far * part, part)
    copies = []
    for j in range(rows):
        copies.append(
            [
                pltpu.make_async_copy(m_ref.at[j], masks.at[j], sems.at[j, 0]),
                pltpu.make_async_copy(v_ref.at[j], vs.at[j], sems.at[j, 1]),
            ]
        )
    extra = [
        pltpu.make_async_copy(u_ref.at[0, at], us, sems.at[0, 2]),
        pltpu.make_async_copy(t_ref.at[0, at], ts, sems.at[0, 3]),
    ]
    for group in (copies[0], extra, *copies[1:]):
        for c in group:
            c.start()
    ones = jnp.ones((8, lon), BF16)
    for j in range(rows):
        for c in copies[j]:
            c.wait()
        keep = keep_of(masks[j])
        v = (vs[j] * keep[None]).reshape(samples * levels, lon)
        sums_ref[j : j + 1, :] = lax.dot_general(ones, v, CONTRACT, preferred_element_type=F32)[0:1]
        full = jnp.broadcast_to(keep[None], (samples, levels, lon)).reshape(samples * levels, lon)
        sums_ref[rows + j : rows + j + 1, :] = lax.dot_general(
            ones, full, CONTRACT, preferred_element_type=F32
        )[0:1]
    for c in extra:
        c.wait()
    keep = keep_of(masks[0])[None]
    for f, field in enumerate((ts[...], us[...], vs[0, at])):
        o_ref[0, f * size : (f + 1) * size, :] = (field * keep).reshape(size, lon)


def first_part(half, u, v, t, mask):
    rows, samples, levels, lon = v.shape
    part = samples // 2
    return pl.pallas_call(
        first_kernel,
        out_shape=(
            jax.ShapeDtypeStruct((1, 3 * part * levels, lon), BF16),
            jax.ShapeDtypeStruct((2 * rows, samples * levels), F32),
        ),
        in_specs=[SMEM, HBM, HBM, HBM, HBM],
        out_specs=(VMEM, VMEM),
        scratch_shapes=[
            pltpu.VMEM((part, levels, lon), BF16),
            pltpu.VMEM((rows, samples, levels, lon), BF16),
            pltpu.VMEM((part, levels, lon), BF16),
            pltpu.VMEM((rows, levels, lon), jnp.int32),
            pltpu.SemaphoreType.DMA((rows, 4)),
        ],
        compiler_params=params(60),
        name="sums",
    )(half, u, v, t, mask)


def send_kernel(groups, half_ref, u_ref, v_ref, t_ref, m_ref, _, *rest):
    n = len(groups)
    far_refs, near_refs = rest[: n - 1], rest[n - 1 : 2 * n - 1]
    us, vs, ts, masks, fars, nears, sems, out_sems = rest[2 * n - 1 :]
    rows, samples, levels, lon = vs.shape
    part = samples // 2
    size = part * levels
    near = half_ref[0]
    far = 1 - near
    copies = []
    for j in range(rows):
        group = [
            pltpu.make_async_copy(m_ref.at[j], masks.at[j], sems.at[j, 0]),
            pltpu.make_async_copy(v_ref.at[j], vs.at[j], sems.at[j, 1]),
            pltpu.make_async_copy(u_ref.at[j], us.at[j], sems.at[j, 2]),
            pltpu.make_async_copy(t_ref.at[j], ts.at[j], sems.at[j, 3]),
        ]
        for c in group:
            c.start()
        copies.append(group)
    done = []
    for g, group in enumerate(groups):
        for i, j in enumerate(group):
            for c in copies[j]:
                c.wait()
            keep = keep_of(masks[j])
            for k, (where, box) in enumerate(((far, fars), (near, nears))):
                if k == 0 and g == 0:
                    continue
                ref = far_refs[g - 1] if k == 0 else near_refs[g]
                for f, field in enumerate((ts, us, vs)):
                    mine = field[j, pl.ds(where * part, part)] * keep[None]
                    box[j, f * size : (f + 1) * size, :] = mine.reshape(size, lon)
                c = pltpu.make_async_copy(box.at[j], ref.at[i], out_sems.at[j, k])
                c.start()
                done.append(c)
    for c in done:
        c.wait()


def send(half, u, v, t, mask, after, groups):
    rows, samples, levels, lon = v.shape
    part = samples // 2
    unit = 3 * part * levels
    n = len(groups)
    packed = [jax.ShapeDtypeStruct((len(g), unit, lon), BF16) for g in groups]
    return pl.pallas_call(
        lambda *refs: send_kernel(groups, *refs),
        out_shape=(
            *packed[1:],
            *packed,
        ),
        in_specs=[SMEM, HBM, HBM, HBM, HBM, ANY],
        out_specs=(HBM,) * (2 * n - 1),
        scratch_shapes=[
            pltpu.VMEM((rows, samples, levels, lon), BF16),
            pltpu.VMEM((rows, samples, levels, lon), BF16),
            pltpu.VMEM((rows, samples, levels, lon), BF16),
            pltpu.VMEM((rows, levels, lon), jnp.int32),
            pltpu.VMEM((rows, unit, lon), BF16),
            pltpu.VMEM((rows, unit, lon), BF16),
            pltpu.SemaphoreType.DMA((rows, 4)),
            pltpu.SemaphoreType.DMA((rows, 2)),
        ],
        compiler_params=params(60),
        name="send",
    )(half, u, v, t, mask, after)


def wave_kernel(half_ref, table_ref, own_ref, got_ref, _, *o_refs, flips):
    n = table_ref.shape[2] // 2
    scale = 2.0 / (MERIDIANS * MERIDIANS)
    for i in range(got_ref.shape[0]):
        own, got = own_ref[i].astype(F32), got_ref[i].astype(F32)
        for p, mixed in enumerate(((own - got).astype(BF16), (own + got).astype(BF16))):
            x = jnp.concatenate([mixed, mixed[2 * mixed.shape[0] // 3 :]])
            w = x.shape[0] // 2
            for flip, o_ref in zip(flips, o_refs):
                table = table_ref[1 - half_ref[0] if flip else half_ref[0], p]
                c = lax.dot_general(table, x, CONTRACT, preferred_element_type=F32)
                both = c[:n, :w] * c[:n, w:] + c[n:, :w] * c[n:, w:]
                o_ref[i, p] = (scale * both).astype(o_ref.dtype)


def waves(half, table, own, got, after, *flips):
    rows, cols, _ = got.shape
    shape = (rows, 2, PADDED, 2 * cols // 3)
    return pl.pallas_call(
        functools.partial(wave_kernel, flips=flips),
        out_shape=tuple(jax.ShapeDtypeStruct(shape, BF16 if f else F32) for f in flips),
        in_specs=[SMEM, VMEM, VMEM, VMEM, ANY],
        out_specs=(VMEM,) * len(flips),
        compiler_params=params(16),
        name="waves",
    )(half, table, own, got, after)


def join_kernel(first, parts, half_ref, *refs):
    own_refs, got_refs = refs[:parts], refs[parts : 2 * parts]
    heat_ref, mom_ref, heat, mom, sems = refs[-5:]
    copies = []
    at = 0
    for own_ref, got_ref in zip(own_refs, got_refs):
        for i in range(own_ref.shape[0]):
            zero = half_ref[0] == 0
            for p in range(2):
                own = own_ref[i, p]
                got = got_ref[i, p].astype(F32)
                a = jnp.where(zero, own, got)
                b = jnp.where(zero, got, own)
                w = own.shape[1] // 2
                low = lax.broadcasted_iota(jnp.int32, own.shape, 1) < w
                n = heat.shape[1] // 2
                every = pl.ds(p, n, stride=2)
                heat[at, every, :] = jnp.where(low, a, pltpu.roll(b, w, 1))[:n]
                mom[at, every, :] = jnp.where(low, pltpu.roll(a, w, 1), b)[:n]
            for k, (x, ref) in enumerate(((heat, heat_ref), (mom, mom_ref))):
                c = pltpu.make_async_copy(x.at[at], ref.at[first + at], sems.at[at, k])
                c.start()
                copies.append(c)
            at += 1
    for c in copies:
        c.wait()


def join(half, own, got, outs, rows, total):
    n, width = ORDERS // 2, own[0].shape[3]
    shape = jax.ShapeDtypeStruct((total, n, width), F32)
    parts = len(own)
    args = (half, *own, *got)
    specs = [SMEM] + [VMEM] * (2 * parts)
    extra = {}
    if outs is not None:
        extra = {"input_output_aliases": {len(args): 0, len(args) + 1: 1}}
        args += outs
        specs += [HBM, HBM]
    return pl.pallas_call(
        lambda *refs: join_kernel(rows[0], parts, *refs),
        out_shape=(shape, shape),
        in_specs=specs,
        out_specs=(HBM, HBM),
        scratch_shapes=[
            pltpu.VMEM((len(rows), n, width), F32),
            pltpu.VMEM((len(rows), n, width), F32),
            pltpu.SemaphoreType.DMA((len(rows), 2)),
        ],
        compiler_params=params(8),
        name="join",
        **extra,
    )(*args)


def cosines(first, rows, total):
    index = lax.broadcasted_iota(jnp.int32, (rows, 1), 0) + first
    return jnp.cos(((index.astype(F32) + 0.5) / total - 0.5) * math.pi)


def weight_of(first, rows, total):
    latitude = ((np.arange(first, first + rows) + 0.5) / total - 0.5) * math.pi
    return float(np.sum(np.cos(latitude)))


def weigh_kernel(total, place_ref, own_ref, lon_ref, depth_ref, d_ref, o_ref):
    rows, samples, levels = d_ref.shape
    band = place_ref[0] // 128 * 64 + place_ref[0] % 64
    depth = depth_ref[...]
    spread = jnp.concatenate([depth] * samples, axis=1)
    kept = own_ref[rows : 2 * rows] + lon_ref[rows : 2 * rows]
    mean = (own_ref[0:rows] + lon_ref[0:rows]) / jnp.maximum(kept, 1.0)
    weighted = mean * cosines(band * rows, rows, total) * spread
    for p in range(o_ref.shape[0]):
        o_ref[p, 0:rows, :] = weighted
        for b in range(samples):
            o_ref[p, 8 : 8 + rows, b * levels : (b + 1) * levels] = d_ref[:, b, :]


def band_kernel(total, rows, levels, place_ref, g_ref, mine_ref, s_ref, w_ref):
    peers, _, width = g_ref.shape
    span = peers * rows
    lane = lax.broadcasted_iota(jnp.int32, (1, width), 1) % levels
    so_far = jnp.zeros((1, width), F32)
    for p in range(peers):
        for r in range(rows):
            so_far = so_far + g_ref[p, r : r + 1, :]
            w_ref[p * rows + r : p * rows + r + 1, :] = so_far
            w_ref[span + p * rows + r : span + p * rows + r + 1, :] = g_ref[p, 8 + r : 9 + r, :]
    run = w_ref[0:span, :]
    step = 1
    while step < levels:
        run = run + jnp.where(lane >= step, pltpu.roll(run, step, 1), 0.0)
        step *= 2
    want = w_ref[span:, :]
    block = place_ref[0] // 128 * 8 + place_ref[0] % 64 // 8
    cosine = cosines(block * span, span, total)
    stats = (
        run[span - 1 : span],
        jnp.max(run, axis=0, keepdims=True),
        jnp.min(run, axis=0, keepdims=True),
        jnp.sum(cosine * run, axis=0, keepdims=True),
        jnp.sum(cosine * run * run, axis=0, keepdims=True),
        jnp.sum(cosine * want, axis=0, keepdims=True),
        jnp.sum(cosine * run * want, axis=0, keepdims=True),
        jnp.sum(cosine * want * want, axis=0, keepdims=True),
    )
    for p in range(s_ref.shape[0]):
        for i, stat in enumerate(stats):
            s_ref[p, i : i + 1, :] = stat
    w_ref[0:span, :] = run
    for p in range(peers):

        @pl.when(place_ref[0] % 8 == p)
        def _():
            mine_ref[...] = w_ref[p * rows : (p + 1) * rows, :]


def add_block(so_far, block, weight):
    s, hi, lo, run1, run2, want1, cross, want2 = block
    if so_far is None:
        return block
    off = so_far[0]
    return (
        off + s,
        jnp.maximum(so_far[1], off + hi),
        jnp.minimum(so_far[2], off + lo),
        so_far[3] + (run1 + off * weight),
        so_far[4] + (run2 + 2.0 * off * run1 + off * off * weight),
        so_far[5] + want1,
        so_far[6] + (cross + off * want1),
        so_far[7] + want2,
    )


def half_kernel(total, span, place_ref, mine_ref, s_ref, own_ref, half_ref):
    blocks = s_ref.shape[0]
    here = place_ref[0] % 64 // 8
    north = place_ref[0] // 128 == 1
    stats = None
    offset = jnp.zeros((1, s_ref.shape[2]), F32)
    for z in range(blocks):
        if z:
            offset = jnp.where(here == z, stats[0], offset)
        weights = [weight_of((h * blocks + z) * span, span, total) for h in range(2)]
        weight = jnp.where(north, weights[1], weights[0])
        stats = add_block(stats, [s_ref[z, i : i + 1, :] for i in range(8)], weight)
    own_ref[...] = mine_ref[...] + offset
    for i, stat in enumerate(stats):
        half_ref[i : i + 1, :] = stat


def finish_kernel(total, place_ref, own_ref, near_ref, far_ref, psi_ref, loss_ref):
    _, samples, levels = psi_ref.shape
    north = place_ref[0] // 128 == 1
    near = near_ref[...]
    far = far_ref[...]
    south_half = jnp.where(north, far, near)
    north_half = jnp.where(north, near, far)
    weight = weight_of(total // 2, total // 2, total)
    stats = add_block(
        [south_half[i : i + 1] for i in range(8)], [north_half[i : i + 1] for i in range(8)], weight
    )
    peak = jnp.max(jnp.maximum(jnp.abs(stats[1]), jnp.abs(stats[2])), axis=1, keepdims=True)
    scale = peak + EPSILON
    psi = (own_ref[...] + jnp.where(north, far[0:1], 0.0)) / scale
    for b in range(samples):
        psi_ref[:, b, :] = psi[:, b * levels : (b + 1) * levels]
    a, b, c = (jnp.sum(stats[i], axis=1, keepdims=True) for i in (4, 6, 7))
    loss = (a / scale / scale - 2.0 * (b / scale) + c) / (samples * levels * total)
    loss_ref[...] = jnp.broadcast_to(loss, loss_ref.shape)


def small(body, out_shape, *args, scratch=(), after=None):
    many = isinstance(out_shape, tuple)
    specs = [SMEM] + [VMEM] * (len(args) - 1)
    if after is not None:
        plain, count = body, len(args)
        body = lambda *refs: plain(*refs[:count], *refs[count + 1 :])
        args += (after,)
        specs.append(ANY)
    return pl.pallas_call(
        body,
        out_shape=out_shape,
        in_specs=specs,
        out_specs=(VMEM,) * len(out_shape) if many else VMEM,
        scratch_shapes=scratch,
        compiler_params=params(2),
    )(*args)


def all_of(x, axes):
    return lax.all_to_all(x, axes, split_axis=0, concat_axis=0, tiled=True)


def floats(*shape):
    return jax.ShapeDtypeStruct(shape, F32)


def per_device(u, v, t, mask, depth, desired):
    bands, samples, levels, lon = v.shape
    width = samples * levels
    total = bands * lax.axis_size(LAT_LEV)
    half = lax.axis_index("lon")[None].astype(jnp.int32)
    place = lax.axis_index(("lat", "lon", "lev_0", "lev_1", "lev_2"))[None].astype(jnp.int32)
    across = [(0, 1), (1, 0)]
    table = jnp.asarray(half_table(lon), BF16)

    def swap(x):
        return lax.ppermute(x, "lon", across)

    first, sums = first_part(half, u, v, t, mask)
    packed = send(half, u, v, t, mask, sums, GROUPS)
    rest, own = packed[: len(GROUPS) - 1], packed[len(GROUPS) - 1 :]
    got = [swap(first)]
    by_lon = swap(sums)
    got += [swap(x) for x in rest]

    peers = lax.axis_size(INNER)
    outer = lax.axis_size(OUTER)
    rows = small(
        lambda *refs: weigh_kernel(total, *refs),
        floats(peers, 16, width),
        place,
        sums,
        by_lon,
        depth[None],
        desired,
    )
    near_bands = all_of(rows, INNER)
    far0, near0 = waves(half, table, own[0], got[0], rows, True, False)
    span = bands * peers
    mine, stats = small(
        lambda *refs: band_kernel(total, bands, levels, *refs),
        (floats(bands, width), floats(outer, 8, width)),
        place,
        near_bands,
        scratch=[pltpu.VMEM((2 * span, width), F32)],
    )
    all_stats = all_of(stats, OUTER)
    mine, near_half = small(
        lambda *refs: half_kernel(total, span, *refs),
        (floats(bands, width), floats(8, width)),
        place,
        mine,
        all_stats,
    )
    far_half = lax.ppermute(near_half, ("lat", "lon"), [(i, 3 - i) for i in range(4)])
    far1, near1 = waves(half, table, own[1], got[1], stats, True, False)
    (far2,) = waves(half, table, own[2], got[2], near_half, True)
    (near2,) = waves(half, table, own[2], got[2], near_half, False)
    psi, loss = small(
        lambda *refs: finish_kernel(total, *refs),
        (floats(bands, samples, levels), floats(1, width)),
        place,
        mine,
        near_half,
        far_half,
        after=near2,
    )

    back = [swap(x) for x in (far0, far1, far2)]
    kept = [near0, near1, near2]
    outs = join(half, kept[:2], back[:2], None, GROUPS[0] + GROUPS[1], bands)
    outs = join(half, kept[2:], back[2:], outs, GROUPS[2], bands)
    heat, momentum = (jnp.transpose(x, (1, 0, 2)) for x in outs)
    return psi, heat, momentum, loss[0, 0]


def solution(mesh):
    torus = Mesh(
        mesh.devices.reshape(mesh.shape["lat"], mesh.shape["lon"], 8, 4, 2),
        ("lat", "lon", "lev_0", "lev_1", "lev_2"),
    )
    in_specs = (
        P(LAT_LEV, None, None, "lon"),
        P(LAT_LEV, None, None, "lon"),
        P(LAT_LEV, None, None, "lon"),
        P(LAT_LEV, None, "lon"),
        P(),
        P(LAT_LEV, None, None),
    )
    out_specs = (P(LAT_LEV, None, None), P("lon", LAT_LEV, None), P("lon", LAT_LEV, None), P())

    return jax.shard_map(
        per_device, mesh=torus, in_specs=in_specs, out_specs=out_specs, check_vma=False
    )
```

```python
import functools
import math

import jax
import jax.numpy as jnp
import numpy as np
from jax import lax
from jax.experimental import pallas as pl
from jax.experimental.pallas import tpu as pltpu
from jax.sharding import Mesh
from jax.sharding import PartitionSpec as P


MERIDIANS = 1440
ORDERS = 720
PADDED = 184
LAT_LEV = ("lat", "lev_0", "lev_1", "lev_2")
INNER = ("lev_1", "lev_2")
OUTER = "lev_0"
EPSILON = 1e-06
GROUPS = ((0,), (1, 2), (3, 4))
F32 = jnp.float32
BF16 = jnp.bfloat16
MIB = 1024 * 1024
CONTRACT = (((1,), (1,)), ((), ()))
SMEM = pl.BlockSpec(memory_space=pltpu.SMEM)
VMEM = pl.BlockSpec(memory_space=pltpu.VMEM)
HBM = pl.BlockSpec(memory_space=pltpu.HBM)
ANY = pl.BlockSpec(memory_space=pl.ANY)


def half_table(lon):
    order = np.arange(1, ORDERS + 1, dtype=np.int64)
    turns = (order[:, None] * np.arange(lon, dtype=np.int64)[None, :]) % MERIDIANS
    angle = turns.astype(np.float32) * np.float32(2.0 * math.pi / MERIDIANS)
    both = np.stack([np.cos(angle), np.sin(angle)]).reshape(2, 2, ORDERS // 4, 2, lon)
    rows = np.zeros((2, 2, 2, PADDED, lon), np.float32)
    rows[:, :, :, : ORDERS // 4] = both.transpose(1, 3, 0, 2, 4)
    return rows.reshape(2, 2, 2 * PADDED, lon)


def params(mib):
    return pltpu.CompilerParams(vmem_limit_bytes=mib * MIB)


def keep_of(mask):
    return mask.astype(F32).astype(BF16)


def pack_kernel(half_ref, u_ref, v_ref, t_ref, m_ref, o_ref, fields, mask, sems):
    part = fields.shape[1]
    at = pl.ds((1 - half_ref[0]) * part, part)
    copies = [pltpu.make_async_copy(m_ref.at[0], mask, sems.at[3])]
    for f, ref in enumerate((t_ref, u_ref, v_ref)):
        copies.append(pltpu.make_async_copy(ref.at[0, at], fields.at[f], sems.at[f]))
    for c in copies:
        c.start()
    for c in copies:
        c.wait()
    size = part * fields.shape[2]
    keep = keep_of(mask[...])[None]
    for f in range(3):
        o_ref[0, f * size : (f + 1) * size, :] = (fields[f] * keep).reshape(size, -1)


def pack(half, u, v, t, mask):
    _, samples, levels, lon = u.shape
    part = samples // 2
    return pl.pallas_call(
        pack_kernel,
        out_shape=jax.ShapeDtypeStruct((1, 3 * part * levels, lon), BF16),
        in_specs=[SMEM, HBM, HBM, HBM, HBM],
        out_specs=VMEM,
        scratch_shapes=[
            pltpu.VMEM((3, part, levels, lon), BF16),
            pltpu.VMEM((levels, lon), jnp.int32),
            pltpu.SemaphoreType.DMA((4,)),
        ],
        compiler_params=params(60),
        name="pack",
    )(half, u, v, t, mask)


def sums_kernel(v_ref, m_ref, _, sums_ref, vs, masks, sems):
    rows, samples, levels, lon = vs.shape
    copies = [
        (
            pltpu.make_async_copy(m_ref.at[j], masks.at[j], sems.at[j, 0]),
            pltpu.make_async_copy(v_ref.at[j], vs.at[j], sems.at[j, 1]),
        )
        for j in range(rows)
    ]
    for group in copies:
        for c in group:
            c.start()
    ones = jnp.ones((8, lon), BF16)
    for j in range(rows):
        for c in copies[j]:
            c.wait()
        keep = keep_of(masks[j])
        v = (vs[j] * keep[None]).reshape(samples * levels, lon)
        sums_ref[j : j + 1, :] = lax.dot_general(ones, v, CONTRACT, preferred_element_type=F32)[0:1]
        kept = lax.dot_general(ones, keep, CONTRACT, preferred_element_type=F32)[0:1]
        sums_ref[rows + j : rows + j + 1, :] = jnp.concatenate([kept] * samples, axis=1)


def zonal(v, mask, after):
    rows, samples, levels, lon = v.shape
    return pl.pallas_call(
        sums_kernel,
        out_shape=jax.ShapeDtypeStruct((2 * rows, samples * levels), F32),
        in_specs=[HBM, HBM, ANY],
        out_specs=VMEM,
        scratch_shapes=[
            pltpu.VMEM((rows, samples, levels, lon), BF16),
            pltpu.VMEM((rows, levels, lon), jnp.int32),
            pltpu.SemaphoreType.DMA((rows, 2)),
        ],
        compiler_params=params(60),
        name="sums",
    )(v, mask, after)


def send_kernel(groups, half_ref, u_ref, v_ref, t_ref, m_ref, _, *rest):
    n = len(groups)
    far_refs, near_refs = rest[: n - 1], rest[n - 1 : 2 * n - 1]
    us, vs, ts, masks, fars, nears, sems, out_sems = rest[2 * n - 1 :]
    rows, samples, levels, lon = vs.shape
    part = samples // 2
    size = part * levels
    near = half_ref[0]
    far = 1 - near
    copies = []
    for j in range(rows):
        group = [
            pltpu.make_async_copy(m_ref.at[j], masks.at[j], sems.at[j, 0]),
            pltpu.make_async_copy(v_ref.at[j], vs.at[j], sems.at[j, 1]),
            pltpu.make_async_copy(u_ref.at[j], us.at[j], sems.at[j, 2]),
            pltpu.make_async_copy(t_ref.at[j], ts.at[j], sems.at[j, 3]),
        ]
        for c in group:
            c.start()
        copies.append(group)
    done = []
    for g, group in enumerate(groups):
        for i, j in enumerate(group):
            for c in copies[j]:
                c.wait()
            keep = keep_of(masks[j])
            for k, (where, box) in enumerate(((far, fars), (near, nears))):
                if k == 0 and g == 0:
                    continue
                ref = far_refs[g - 1] if k == 0 else near_refs[g]
                for f, field in enumerate((ts, us, vs)):
                    mine = field[j, pl.ds(where * part, part)] * keep[None]
                    box[j, f * size : (f + 1) * size, :] = mine.reshape(size, lon)
                c = pltpu.make_async_copy(box.at[j], ref.at[i], out_sems.at[j, k])
                c.start()
                done.append(c)
    for c in done:
        c.wait()


def send(half, u, v, t, mask, after, groups):
    rows, samples, levels, lon = v.shape
    part = samples // 2
    unit = 3 * part * levels
    n = len(groups)
    packed = [jax.ShapeDtypeStruct((len(g), unit, lon), BF16) for g in groups]
    return pl.pallas_call(
        lambda *refs: send_kernel(groups, *refs),
        out_shape=(
            *packed[1:],
            *packed,
        ),
        in_specs=[SMEM, HBM, HBM, HBM, HBM, ANY],
        out_specs=(HBM,) * (2 * n - 1),
        scratch_shapes=[
            pltpu.VMEM((rows, samples, levels, lon), BF16),
            pltpu.VMEM((rows, samples, levels, lon), BF16),
            pltpu.VMEM((rows, samples, levels, lon), BF16),
            pltpu.VMEM((rows, levels, lon), jnp.int32),
            pltpu.VMEM((rows, unit, lon), BF16),
            pltpu.VMEM((rows, unit, lon), BF16),
            pltpu.SemaphoreType.DMA((rows, 4)),
            pltpu.SemaphoreType.DMA((rows, 2)),
        ],
        compiler_params=params(60),
        name="send",
    )(half, u, v, t, mask, after)


def wave_kernel(half_ref, table_ref, own_ref, got_ref, _, *o_refs, flips):
    n = table_ref.shape[2] // 2
    scale = 2.0 / (MERIDIANS * MERIDIANS)
    for i in range(got_ref.shape[0]):
        own, got = own_ref[i].astype(F32), got_ref[i].astype(F32)
        for p, mixed in enumerate(((own - got).astype(BF16), (own + got).astype(BF16))):
            x = jnp.concatenate([mixed, mixed[2 * mixed.shape[0] // 3 :]])
            w = x.shape[0] // 2
            for flip, o_ref in zip(flips, o_refs):
                table = table_ref[1 - half_ref[0] if flip else half_ref[0], p]
                c = lax.dot_general(table, x, CONTRACT, preferred_element_type=F32)
                both = c[:n, :w] * c[:n, w:] + c[n:, :w] * c[n:, w:]
                o_ref[i, p] = (scale * both).astype(o_ref.dtype)


def waves(half, table, own, got, after, *flips):
    rows, cols, _ = got.shape
    shape = (rows, 2, PADDED, 2 * cols // 3)
    return pl.pallas_call(
        functools.partial(wave_kernel, flips=flips),
        out_shape=tuple(jax.ShapeDtypeStruct(shape, BF16 if f else F32) for f in flips),
        in_specs=[SMEM, VMEM, VMEM, VMEM, ANY],
        out_specs=(VMEM,) * len(flips),
        compiler_params=params(16),
        name="waves",
    )(half, table, own, got, after)


def join_kernel(first, parts, half_ref, *refs):
    own_refs, got_refs = refs[:parts], refs[parts : 2 * parts]
    heat_ref, mom_ref, heat, mom, sems = refs[-5:]
    copies = []
    at = 0
    for own_ref, got_ref in zip(own_refs, got_refs):
        for i in range(own_ref.shape[0]):
            zero = half_ref[0] == 0
            for p in range(2):
                own = own_ref[i, p]
                got = got_ref[i, p].astype(F32)
                a = jnp.where(zero, own, got)
                b = jnp.where(zero, got, own)
                w = own.shape[1] // 2
                low = lax.broadcasted_iota(jnp.int32, own.shape, 1) < w
                n = heat.shape[1] // 2
                every = pl.ds(p, n, stride=2)
                heat[at, every, :] = jnp.where(low, a, pltpu.roll(b, w, 1))[:n]
                mom[at, every, :] = jnp.where(low, pltpu.roll(a, w, 1), b)[:n]
            for k, (x, ref) in enumerate(((heat, heat_ref), (mom, mom_ref))):
                c = pltpu.make_async_copy(x.at[at], ref.at[first + at], sems.at[at, k])
                c.start()
                copies.append(c)
            at += 1
    for c in copies:
        c.wait()


def join(half, own, got, outs, rows, total):
    n, width = ORDERS // 2, own[0].shape[3]
    shape = jax.ShapeDtypeStruct((total, n, width), F32)
    parts = len(own)
    args = (half, *own, *got)
    specs = [SMEM] + [VMEM] * (2 * parts)
    extra = {}
    if outs is not None:
        extra = {"input_output_aliases": {len(args): 0, len(args) + 1: 1}}
        args += outs
        specs += [HBM, HBM]
    return pl.pallas_call(
        lambda *refs: join_kernel(rows[0], parts, *refs),
        out_shape=(shape, shape),
        in_specs=specs,
        out_specs=(HBM, HBM),
        scratch_shapes=[
            pltpu.VMEM((len(rows), n, width), F32),
            pltpu.VMEM((len(rows), n, width), F32),
            pltpu.SemaphoreType.DMA((len(rows), 2)),
        ],
        compiler_params=params(8),
        name="join",
        **extra,
    )(*args)


def cosines(first, rows, total):
    index = lax.broadcasted_iota(jnp.int32, (rows, 1), 0) + first
    return jnp.cos(((index.astype(F32) + 0.5) / total - 0.5) * math.pi)


def weight_of(first, rows, total):
    latitude = ((np.arange(first, first + rows) + 0.5) / total - 0.5) * math.pi
    return float(np.sum(np.cos(latitude)))


def weigh_kernel(total, place_ref, own_ref, lon_ref, depth_ref, d_ref, o_ref):
    rows, samples, levels = d_ref.shape
    band = place_ref[0] // 128 * 64 + place_ref[0] % 64
    depth = depth_ref[...]
    spread = jnp.concatenate([depth] * samples, axis=1)
    kept = own_ref[rows : 2 * rows] + lon_ref[rows : 2 * rows]
    mean = (own_ref[0:rows] + lon_ref[0:rows]) / jnp.maximum(kept, 1.0)
    weighted = mean * cosines(band * rows, rows, total) * spread
    for p in range(o_ref.shape[0]):
        o_ref[p, 0:rows, :] = weighted
        for b in range(samples):
            o_ref[p, 8 : 8 + rows, b * levels : (b + 1) * levels] = d_ref[:, b, :]


def band_kernel(total, rows, levels, place_ref, g_ref, mine_ref, s_ref, w_ref):
    peers, _, width = g_ref.shape
    span = peers * rows
    lane = lax.broadcasted_iota(jnp.int32, (1, width), 1) % levels
    so_far = jnp.zeros((1, width), F32)
    for p in range(peers):
        for r in range(rows):
            so_far = so_far + g_ref[p, r : r + 1, :]
            w_ref[p * rows + r : p * rows + r + 1, :] = so_far
            w_ref[span + p * rows + r : span + p * rows + r + 1, :] = g_ref[p, 8 + r : 9 + r, :]
    run = w_ref[0:span, :]
    step = 1
    while step < levels:
        run = run + jnp.where(lane >= step, pltpu.roll(run, step, 1), 0.0)
        step *= 2
    want = w_ref[span:, :]
    block = place_ref[0] // 128 * 8 + place_ref[0] % 64 // 8
    cosine = cosines(block * span, span, total)
    stats = (
        run[span - 1 : span],
        jnp.max(run, axis=0, keepdims=True),
        jnp.min(run, axis=0, keepdims=True),
        jnp.sum(cosine * run, axis=0, keepdims=True),
        jnp.sum(cosine * run * run, axis=0, keepdims=True),
        jnp.sum(cosine * want, axis=0, keepdims=True),
        jnp.sum(cosine * run * want, axis=0, keepdims=True),
        jnp.sum(cosine * want * want, axis=0, keepdims=True),
    )
    for p in range(s_ref.shape[0]):
        for i, stat in enumerate(stats):
            s_ref[p, i : i + 1, :] = stat
    w_ref[0:span, :] = run
    for p in range(peers):

        @pl.when(place_ref[0] % 8 == p)
        def _():
            mine_ref[...] = w_ref[p * rows : (p + 1) * rows, :]


def add_block(so_far, block, weight):
    s, hi, lo, run1, run2, want1, cross, want2 = block
    if so_far is None:
        return block
    off = so_far[0]
    return (
        off + s,
        jnp.maximum(so_far[1], off + hi),
        jnp.minimum(so_far[2], off + lo),
        so_far[3] + (run1 + off * weight),
        so_far[4] + (run2 + 2.0 * off * run1 + off * off * weight),
        so_far[5] + want1,
        so_far[6] + (cross + off * want1),
        so_far[7] + want2,
    )


def half_kernel(total, span, place_ref, mine_ref, s_ref, own_ref, half_ref):
    blocks = s_ref.shape[0]
    here = place_ref[0] % 64 // 8
    north = place_ref[0] // 128 == 1
    stats = None
    offset = jnp.zeros((1, s_ref.shape[2]), F32)
    for z in range(blocks):
        if z:
            offset = jnp.where(here == z, stats[0], offset)
        weights = [weight_of((h * blocks + z) * span, span, total) for h in range(2)]
        weight = jnp.where(north, weights[1], weights[0])
        stats = add_block(stats, [s_ref[z, i : i + 1, :] for i in range(8)], weight)
    own_ref[...] = mine_ref[...] + offset
    for i, stat in enumerate(stats):
        half_ref[i : i + 1, :] = stat


def finish_kernel(total, place_ref, own_ref, near_ref, far_ref, psi_ref, loss_ref):
    _, samples, levels = psi_ref.shape
    north = place_ref[0] // 128 == 1
    near = near_ref[...]
    far = far_ref[...]
    south_half = jnp.where(north, far, near)
    north_half = jnp.where(north, near, far)
    weight = weight_of(total // 2, total // 2, total)
    stats = add_block(
        [south_half[i : i + 1] for i in range(8)], [north_half[i : i + 1] for i in range(8)], weight
    )
    peak = jnp.max(jnp.maximum(jnp.abs(stats[1]), jnp.abs(stats[2])), axis=1, keepdims=True)
    scale = peak + EPSILON
    psi = (own_ref[...] + jnp.where(north, far[0:1], 0.0)) / scale
    for b in range(samples):
        psi_ref[:, b, :] = psi[:, b * levels : (b + 1) * levels]
    a, b, c = (jnp.sum(stats[i], axis=1, keepdims=True) for i in (4, 6, 7))
    loss = (a / scale / scale - 2.0 * (b / scale) + c) / (samples * levels * total)
    loss_ref[...] = jnp.broadcast_to(loss, loss_ref.shape)


def small(body, out_shape, *args, scratch=(), after=None):
    many = isinstance(out_shape, tuple)
    specs = [SMEM] + [VMEM] * (len(args) - 1)
    if after is not None:
        plain, count = body, len(args)
        body = lambda *refs: plain(*refs[:count], *refs[count + 1 :])
        args += (after,)
        specs.append(ANY)
    return pl.pallas_call(
        body,
        out_shape=out_shape,
        in_specs=specs,
        out_specs=(VMEM,) * len(out_shape) if many else VMEM,
        scratch_shapes=scratch,
        compiler_params=params(2),
    )(*args)


def all_of(x, axes):
    return lax.all_to_all(x, axes, split_axis=0, concat_axis=0, tiled=True)


def floats(*shape):
    return jax.ShapeDtypeStruct(shape, F32)


def per_device(u, v, t, mask, depth, desired):
    bands, samples, levels, lon = v.shape
    width = samples * levels
    total = bands * lax.axis_size(LAT_LEV)
    half = lax.axis_index("lon")[None].astype(jnp.int32)
    place = lax.axis_index(("lat", "lon", "lev_0", "lev_1", "lev_2"))[None].astype(jnp.int32)
    across = [(0, 1), (1, 0)]
    table = jnp.asarray(half_table(lon), BF16)

    def swap(x):
        return lax.ppermute(x, "lon", across)

    first = pack(half, u, v, t, mask)
    sums = zonal(v, mask, first)
    packed = send(half, u, v, t, mask, sums, GROUPS)
    rest, own = packed[: len(GROUPS) - 1], packed[len(GROUPS) - 1 :]
    got = [swap(first)]
    by_lon = swap(sums)
    got += [swap(x) for x in rest]

    peers = lax.axis_size(INNER)
    outer = lax.axis_size(OUTER)
    rows = small(
        lambda *refs: weigh_kernel(total, *refs),
        floats(peers, 16, width),
        place,
        sums,
        by_lon,
        depth[None],
        desired,
    )
    near_bands = all_of(rows, INNER)
    far0, near0 = waves(half, table, own[0], got[0], rows, True, False)
    span = bands * peers
    mine, stats = small(
        lambda *refs: band_kernel(total, bands, levels, *refs),
        (floats(bands, width), floats(outer, 8, width)),
        place,
        near_bands,
        scratch=[pltpu.VMEM((2 * span, width), F32)],
    )
    all_stats = all_of(stats, OUTER)
    mine, near_half = small(
        lambda *refs: half_kernel(total, span, *refs),
        (floats(bands, width), floats(8, width)),
        place,
        mine,
        all_stats,
    )
    far_half = lax.ppermute(near_half, ("lat", "lon"), [(i, 3 - i) for i in range(4)])
    far1, near1 = waves(half, table, own[1], got[1], stats, True, False)
    (far2,) = waves(half, table, own[2], got[2], near_half, True)
    (near2,) = waves(half, table, own[2], got[2], near_half, False)
    psi, loss = small(
        lambda *refs: finish_kernel(total, *refs),
        (floats(bands, samples, levels), floats(1, width)),
        place,
        mine,
        near_half,
        far_half,
        after=near2,
    )

    back = [swap(x) for x in (far0, far1, far2)]
    kept = [near0, near1, near2]
    outs = join(half, kept[:2], back[:2], None, GROUPS[0] + GROUPS[1], bands)
    outs = join(half, kept[2:], back[2:], outs, GROUPS[2], bands)
    heat, momentum = (jnp.transpose(x, (1, 0, 2)) for x in outs)
    return psi, heat, momentum, loss[0, 0]


def solution(mesh):
    torus = Mesh(
        mesh.devices.reshape(mesh.shape["lat"], mesh.shape["lon"], 8, 4, 2),
        ("lat", "lon", "lev_0", "lev_1", "lev_2"),
    )
    in_specs = (
        P(LAT_LEV, None, None, "lon"),
        P(LAT_LEV, None, None, "lon"),
        P(LAT_LEV, None, None, "lon"),
        P(LAT_LEV, None, "lon"),
        P(),
        P(LAT_LEV, None, None),
    )
    out_specs = (P(LAT_LEV, None, None), P("lon", LAT_LEV, None), P("lon", LAT_LEV, None), P())

    return jax.shard_map(
        per_device, mesh=torus, in_specs=in_specs, out_specs=out_specs, check_vma=False
    )
```

```python
import functools
import math

import jax
import jax.numpy as jnp
import numpy as np
from jax import lax
from jax.experimental import pallas as pl
from jax.experimental.pallas import tpu as pltpu
from jax.sharding import Mesh
from jax.sharding import PartitionSpec as P


MERIDIANS = 1440
ORDERS = 720
PADDED = 184
LAT_LEV = ("lat", "lev_0", "lev_1", "lev_2")
INNER = ("lev_1", "lev_2")
OUTER = "lev_0"
EPSILON = 1e-06
GROUPS = ((0,), (1, 2, 3), (4,))
F32 = jnp.float32
BF16 = jnp.bfloat16
MIB = 1024 * 1024
CONTRACT = (((1,), (1,)), ((), ()))
SMEM = pl.BlockSpec(memory_space=pltpu.SMEM)
VMEM = pl.BlockSpec(memory_space=pltpu.VMEM)
HBM = pl.BlockSpec(memory_space=pltpu.HBM)
ANY = pl.BlockSpec(memory_space=pl.ANY)


def half_table(lon):
    order = np.arange(1, ORDERS + 1, dtype=np.int64)
    turns = (order[:, None] * np.arange(lon, dtype=np.int64)[None, :]) % MERIDIANS
    angle = turns.astype(np.float32) * np.float32(2.0 * math.pi / MERIDIANS)
    both = np.stack([np.cos(angle), np.sin(angle)]).reshape(2, 2, ORDERS // 4, 2, lon)
    rows = np.zeros((2, 2, 2, PADDED, lon), np.float32)
    rows[:, :, :, : ORDERS // 4] = both.transpose(1, 3, 0, 2, 4)
    return rows.reshape(2, 2, 2 * PADDED, lon)


def params(mib):
    return pltpu.CompilerParams(vmem_limit_bytes=mib * MIB)


def keep_of(mask):
    return mask.astype(F32).astype(BF16)


def pack_kernel(half_ref, u_ref, v_ref, t_ref, m_ref, o_ref, fields, mask, sems):
    part = fields.shape[1]
    at = pl.ds((1 - half_ref[0]) * part, part)
    copies = [pltpu.make_async_copy(m_ref.at[0], mask, sems.at[3])]
    for f, ref in enumerate((t_ref, u_ref, v_ref)):
        copies.append(pltpu.make_async_copy(ref.at[0, at], fields.at[f], sems.at[f]))
    for c in copies:
        c.start()
    for c in copies:
        c.wait()
    size = part * fields.shape[2]
    keep = keep_of(mask[...])[None]
    for f in range(3):
        o_ref[0, f * size : (f + 1) * size, :] = (fields[f] * keep).reshape(size, -1)


def pack(half, u, v, t, mask):
    _, samples, levels, lon = u.shape
    part = samples // 2
    return pl.pallas_call(
        pack_kernel,
        out_shape=jax.ShapeDtypeStruct((1, 3 * part * levels, lon), BF16),
        in_specs=[SMEM, HBM, HBM, HBM, HBM],
        out_specs=VMEM,
        scratch_shapes=[
            pltpu.VMEM((3, part, levels, lon), BF16),
            pltpu.VMEM((levels, lon), jnp.int32),
            pltpu.SemaphoreType.DMA((4,)),
        ],
        compiler_params=params(60),
        name="pack",
    )(half, u, v, t, mask)


def sums_kernel(v_ref, m_ref, _, sums_ref, vs, masks, sems):
    rows, samples, levels, lon = vs.shape
    copies = [
        (
            pltpu.make_async_copy(m_ref.at[j], masks.at[j], sems.at[j, 0]),
            pltpu.make_async_copy(v_ref.at[j], vs.at[j], sems.at[j, 1]),
        )
        for j in range(rows)
    ]
    for group in copies:
        for c in group:
            c.start()
    ones = jnp.ones((8, lon), BF16)
    for j in range(rows):
        for c in copies[j]:
            c.wait()
        keep = keep_of(masks[j])
        v = (vs[j] * keep[None]).reshape(samples * levels, lon)
        sums_ref[j : j + 1, :] = lax.dot_general(ones, v, CONTRACT, preferred_element_type=F32)[0:1]
        kept = lax.dot_general(ones, keep, CONTRACT, preferred_element_type=F32)[0:1]
        sums_ref[rows + j : rows + j + 1, :] = jnp.concatenate([kept] * samples, axis=1)


def zonal(v, mask, after):
    rows, samples, levels, lon = v.shape
    return pl.pallas_call(
        sums_kernel,
        out_shape=jax.ShapeDtypeStruct((2 * rows, samples * levels), F32),
        in_specs=[HBM, HBM, ANY],
        out_specs=VMEM,
        scratch_shapes=[
            pltpu.VMEM((rows, samples, levels, lon), BF16),
            pltpu.VMEM((rows, levels, lon), jnp.int32),
            pltpu.SemaphoreType.DMA((rows, 2)),
        ],
        compiler_params=params(60),
        name="sums",
    )(v, mask, after)


def send_kernel(groups, half_ref, u_ref, v_ref, t_ref, m_ref, _, *rest):
    n = len(groups)
    far_refs, near_refs = rest[: n - 1], rest[n - 1 : 2 * n - 1]
    us, vs, ts, masks, fars, nears, sems, out_sems = rest[2 * n - 1 :]
    rows, samples, levels, lon = vs.shape
    part = samples // 2
    size = part * levels
    near = half_ref[0]
    far = 1 - near
    copies = []
    for j in range(rows):
        group = [
            pltpu.make_async_copy(m_ref.at[j], masks.at[j], sems.at[j, 0]),
            pltpu.make_async_copy(v_ref.at[j], vs.at[j], sems.at[j, 1]),
            pltpu.make_async_copy(u_ref.at[j], us.at[j], sems.at[j, 2]),
            pltpu.make_async_copy(t_ref.at[j], ts.at[j], sems.at[j, 3]),
        ]
        for c in group:
            c.start()
        copies.append(group)
    done = []
    for g, group in enumerate(groups):
        for i, j in enumerate(group):
            for c in copies[j]:
                c.wait()
            keep = keep_of(masks[j])
            for k, (where, box) in enumerate(((far, fars), (near, nears))):
                if k == 0 and g == 0:
                    continue
                ref = far_refs[g - 1] if k == 0 else near_refs[g]
                for f, field in enumerate((ts, us, vs)):
                    mine = field[j, pl.ds(where * part, part)] * keep[None]
                    box[j, f * size : (f + 1) * size, :] = mine.reshape(size, lon)
                c = pltpu.make_async_copy(box.at[j], ref.at[i], out_sems.at[j, k])
                c.start()
                done.append(c)
    for c in done:
        c.wait()


def send(half, u, v, t, mask, after, groups):
    rows, samples, levels, lon = v.shape
    part = samples // 2
    unit = 3 * part * levels
    n = len(groups)
    packed = [jax.ShapeDtypeStruct((len(g), unit, lon), BF16) for g in groups]
    return pl.pallas_call(
        lambda *refs: send_kernel(groups, *refs),
        out_shape=(
            *packed[1:],
            *packed,
        ),
        in_specs=[SMEM, HBM, HBM, HBM, HBM, ANY],
        out_specs=(HBM,) * (2 * n - 1),
        scratch_shapes=[
            pltpu.VMEM((rows, samples, levels, lon), BF16),
            pltpu.VMEM((rows, samples, levels, lon), BF16),
            pltpu.VMEM((rows, samples, levels, lon), BF16),
            pltpu.VMEM((rows, levels, lon), jnp.int32),
            pltpu.VMEM((rows, unit, lon), BF16),
            pltpu.VMEM((rows, unit, lon), BF16),
            pltpu.SemaphoreType.DMA((rows, 4)),
            pltpu.SemaphoreType.DMA((rows, 2)),
        ],
        compiler_params=params(60),
        name="send",
    )(half, u, v, t, mask, after)


def wave_kernel(half_ref, table_ref, own_ref, got_ref, _, *o_refs, flips):
    n = table_ref.shape[2] // 2
    scale = 2.0 / (MERIDIANS * MERIDIANS)
    for i in range(got_ref.shape[0]):
        own, got = own_ref[i].astype(F32), got_ref[i].astype(F32)
        for p, mixed in enumerate(((own - got).astype(BF16), (own + got).astype(BF16))):
            x = jnp.concatenate([mixed, mixed[2 * mixed.shape[0] // 3 :]])
            w = x.shape[0] // 2
            for flip, o_ref in zip(flips, o_refs):
                table = table_ref[1 - half_ref[0] if flip else half_ref[0], p]
                c = lax.dot_general(table, x, CONTRACT, preferred_element_type=F32)
                both = c[:n, :w] * c[:n, w:] + c[n:, :w] * c[n:, w:]
                o_ref[i, p] = (scale * both).astype(o_ref.dtype)


def waves(half, table, own, got, after, *flips):
    rows, cols, _ = got.shape
    shape = (rows, 2, PADDED, 2 * cols // 3)
    return pl.pallas_call(
        functools.partial(wave_kernel, flips=flips),
        out_shape=tuple(jax.ShapeDtypeStruct(shape, BF16 if f else F32) for f in flips),
        in_specs=[SMEM, VMEM, VMEM, VMEM, ANY],
        out_specs=(VMEM,) * len(flips),
        compiler_params=params(16),
        name="waves",
    )(half, table, own, got, after)


def join_kernel(first, parts, half_ref, *refs):
    own_refs, got_refs = refs[:parts], refs[parts : 2 * parts]
    heat_ref, mom_ref, heat, mom, sems = refs[-5:]
    copies = []
    at = 0
    for own_ref, got_ref in zip(own_refs, got_refs):
        for i in range(own_ref.shape[0]):
            zero = half_ref[0] == 0
            for p in range(2):
                own = own_ref[i, p]
                got = got_ref[i, p].astype(F32)
                a = jnp.where(zero, own, got)
                b = jnp.where(zero, got, own)
                w = own.shape[1] // 2
                low = lax.broadcasted_iota(jnp.int32, own.shape, 1) < w
                n = heat.shape[1] // 2
                every = pl.ds(p, n, stride=2)
                heat[at, every, :] = jnp.where(low, a, pltpu.roll(b, w, 1))[:n]
                mom[at, every, :] = jnp.where(low, pltpu.roll(a, w, 1), b)[:n]
            for k, (x, ref) in enumerate(((heat, heat_ref), (mom, mom_ref))):
                c = pltpu.make_async_copy(x.at[at], ref.at[first + at], sems.at[at, k])
                c.start()
                copies.append(c)
            at += 1
    for c in copies:
        c.wait()


def join(half, own, got, outs, rows, total):
    n, width = ORDERS // 2, own[0].shape[3]
    shape = jax.ShapeDtypeStruct((total, n, width), F32)
    parts = len(own)
    args = (half, *own, *got)
    specs = [SMEM] + [VMEM] * (2 * parts)
    extra = {}
    if outs is not None:
        extra = {"input_output_aliases": {len(args): 0, len(args) + 1: 1}}
        args += outs
        specs += [HBM, HBM]
    return pl.pallas_call(
        lambda *refs: join_kernel(rows[0], parts, *refs),
        out_shape=(shape, shape),
        in_specs=specs,
        out_specs=(HBM, HBM),
        scratch_shapes=[
            pltpu.VMEM((len(rows), n, width), F32),
            pltpu.VMEM((len(rows), n, width), F32),
            pltpu.SemaphoreType.DMA((len(rows), 2)),
        ],
        compiler_params=params(8),
        name="join",
        **extra,
    )(*args)


def cosines(first, rows, total):
    index = lax.broadcasted_iota(jnp.int32, (rows, 1), 0) + first
    return jnp.cos(((index.astype(F32) + 0.5) / total - 0.5) * math.pi)


def weight_of(first, rows, total):
    latitude = ((np.arange(first, first + rows) + 0.5) / total - 0.5) * math.pi
    return float(np.sum(np.cos(latitude)))


def weigh_kernel(total, place_ref, own_ref, lon_ref, depth_ref, d_ref, o_ref):
    rows, samples, levels = d_ref.shape
    band = place_ref[0] // 128 * 64 + place_ref[0] % 64
    depth = depth_ref[...]
    spread = jnp.concatenate([depth] * samples, axis=1)
    kept = own_ref[rows : 2 * rows] + lon_ref[rows : 2 * rows]
    mean = (own_ref[0:rows] + lon_ref[0:rows]) / jnp.maximum(kept, 1.0)
    weighted = mean * cosines(band * rows, rows, total) * spread
    for p in range(o_ref.shape[0]):
        o_ref[p, 0:rows, :] = weighted
        for b in range(samples):
            o_ref[p, 8 : 8 + rows, b * levels : (b + 1) * levels] = d_ref[:, b, :]


def band_kernel(total, rows, levels, place_ref, g_ref, mine_ref, s_ref, w_ref):
    peers, _, width = g_ref.shape
    span = peers * rows
    lane = lax.broadcasted_iota(jnp.int32, (1, width), 1) % levels
    so_far = jnp.zeros((1, width), F32)
    for p in range(peers):
        for r in range(rows):
            so_far = so_far + g_ref[p, r : r + 1, :]
            w_ref[p * rows + r : p * rows + r + 1, :] = so_far
            w_ref[span + p * rows + r : span + p * rows + r + 1, :] = g_ref[p, 8 + r : 9 + r, :]
    run = w_ref[0:span, :]
    step = 1
    while step < levels:
        run = run + jnp.where(lane >= step, pltpu.roll(run, step, 1), 0.0)
        step *= 2
    want = w_ref[span:, :]
    block = place_ref[0] // 128 * 8 + place_ref[0] % 64 // 8
    cosine = cosines(block * span, span, total)
    stats = (
        run[span - 1 : span],
        jnp.max(run, axis=0, keepdims=True),
        jnp.min(run, axis=0, keepdims=True),
        jnp.sum(cosine * run, axis=0, keepdims=True),
        jnp.sum(cosine * run * run, axis=0, keepdims=True),
        jnp.sum(cosine * want, axis=0, keepdims=True),
        jnp.sum(cosine * run * want, axis=0, keepdims=True),
        jnp.sum(cosine * want * want, axis=0, keepdims=True),
    )
    for p in range(s_ref.shape[0]):
        for i, stat in enumerate(stats):
            s_ref[p, i : i + 1, :] = stat
    w_ref[0:span, :] = run
    for p in range(peers):

        @pl.when(place_ref[0] % 8 == p)
        def _():
            mine_ref[...] = w_ref[p * rows : (p + 1) * rows, :]


def add_block(so_far, block, weight):
    s, hi, lo, run1, run2, want1, cross, want2 = block
    if so_far is None:
        return block
    off = so_far[0]
    return (
        off + s,
        jnp.maximum(so_far[1], off + hi),
        jnp.minimum(so_far[2], off + lo),
        so_far[3] + (run1 + off * weight),
        so_far[4] + (run2 + 2.0 * off * run1 + off * off * weight),
        so_far[5] + want1,
        so_far[6] + (cross + off * want1),
        so_far[7] + want2,
    )


def half_kernel(total, span, place_ref, mine_ref, s_ref, own_ref, half_ref):
    blocks = s_ref.shape[0]
    here = place_ref[0] % 64 // 8
    north = place_ref[0] // 128 == 1
    stats = None
    offset = jnp.zeros((1, s_ref.shape[2]), F32)
    for z in range(blocks):
        if z:
            offset = jnp.where(here == z, stats[0], offset)
        weights = [weight_of((h * blocks + z) * span, span, total) for h in range(2)]
        weight = jnp.where(north, weights[1], weights[0])
        stats = add_block(stats, [s_ref[z, i : i + 1, :] for i in range(8)], weight)
    own_ref[...] = mine_ref[...] + offset
    for i, stat in enumerate(stats):
        half_ref[i : i + 1, :] = stat


def finish_kernel(total, place_ref, own_ref, near_ref, far_ref, psi_ref, loss_ref):
    _, samples, levels = psi_ref.shape
    north = place_ref[0] // 128 == 1
    near = near_ref[...]
    far = far_ref[...]
    south_half = jnp.where(north, far, near)
    north_half = jnp.where(north, near, far)
    weight = weight_of(total // 2, total // 2, total)
    stats = add_block(
        [south_half[i : i + 1] for i in range(8)], [north_half[i : i + 1] for i in range(8)], weight
    )
    peak = jnp.max(jnp.maximum(jnp.abs(stats[1]), jnp.abs(stats[2])), axis=1, keepdims=True)
    scale = peak + EPSILON
    psi = (own_ref[...] + jnp.where(north, far[0:1], 0.0)) / scale
    for b in range(samples):
        psi_ref[:, b, :] = psi[:, b * levels : (b + 1) * levels]
    a, b, c = (jnp.sum(stats[i], axis=1, keepdims=True) for i in (4, 6, 7))
    loss = (a / scale / scale - 2.0 * (b / scale) + c) / (samples * levels * total)
    loss_ref[...] = jnp.broadcast_to(loss, loss_ref.shape)


def small(body, out_shape, *args, scratch=(), after=None):
    many = isinstance(out_shape, tuple)
    specs = [SMEM] + [VMEM] * (len(args) - 1)
    if after is not None:
        plain, count = body, len(args)
        body = lambda *refs: plain(*refs[:count], *refs[count + 1 :])
        args += (after,)
        specs.append(ANY)
    return pl.pallas_call(
        body,
        out_shape=out_shape,
        in_specs=specs,
        out_specs=(VMEM,) * len(out_shape) if many else VMEM,
        scratch_shapes=scratch,
        compiler_params=params(2),
    )(*args)


def all_of(x, axes):
    return lax.all_to_all(x, axes, split_axis=0, concat_axis=0, tiled=True)


def floats(*shape):
    return jax.ShapeDtypeStruct(shape, F32)


def per_device(u, v, t, mask, depth, desired):
    bands, samples, levels, lon = v.shape
    width = samples * levels
    total = bands * lax.axis_size(LAT_LEV)
    half = lax.axis_index("lon")[None].astype(jnp.int32)
    place = lax.axis_index(("lat", "lon", "lev_0", "lev_1", "lev_2"))[None].astype(jnp.int32)
    across = [(0, 1), (1, 0)]
    table = jnp.asarray(half_table(lon), BF16)

    def swap(x):
        return lax.ppermute(x, "lon", across)

    first = pack(half, u, v, t, mask)
    sums = zonal(v, mask, first)
    packed = send(half, u, v, t, mask, sums, GROUPS)
    rest, own = packed[: len(GROUPS) - 1], packed[len(GROUPS) - 1 :]
    got = [swap(first)]
    by_lon = swap(sums)
    got += [swap(x) for x in rest]

    peers = lax.axis_size(INNER)
    outer = lax.axis_size(OUTER)
    rows = small(
        lambda *refs: weigh_kernel(total, *refs),
        floats(peers, 16, width),
        place,
        sums,
        by_lon,
        depth[None],
        desired,
    )
    near_bands = all_of(rows, INNER)
    far0, near0 = waves(half, table, own[0], got[0], rows, True, False)
    span = bands * peers
    mine, stats = small(
        lambda *refs: band_kernel(total, bands, levels, *refs),
        (floats(bands, width), floats(outer, 8, width)),
        place,
        near_bands,
        scratch=[pltpu.VMEM((2 * span, width), F32)],
    )
    all_stats = all_of(stats, OUTER)
    mine, near_half = small(
        lambda *refs: half_kernel(total, span, *refs),
        (floats(bands, width), floats(8, width)),
        place,
        mine,
        all_stats,
    )
    far_half = lax.ppermute(near_half, ("lat", "lon"), [(i, 3 - i) for i in range(4)])
    far1, near1 = waves(half, table, own[1], got[1], stats, True, False)
    (far2,) = waves(half, table, own[2], got[2], near_half, True)
    (near2,) = waves(half, table, own[2], got[2], near_half, False)
    psi, loss = small(
        lambda *refs: finish_kernel(total, *refs),
        (floats(bands, samples, levels), floats(1, width)),
        place,
        mine,
        near_half,
        far_half,
        after=near2,
    )

    back = [swap(x) for x in (far0, far1, far2)]
    kept = [near0, near1, near2]
    outs = None
    for group, mine, far in zip(GROUPS, kept, back):
        outs = join(half, [mine], [far], outs, group, bands)
    heat, momentum = (jnp.transpose(x, (1, 0, 2)) for x in outs)
    return psi, heat, momentum, loss[0, 0]


def solution(mesh):
    torus = Mesh(
        mesh.devices.reshape(mesh.shape["lat"], mesh.shape["lon"], 8, 4, 2),
        ("lat", "lon", "lev_0", "lev_1", "lev_2"),
    )
    in_specs = (
        P(LAT_LEV, None, None, "lon"),
        P(LAT_LEV, None, None, "lon"),
        P(LAT_LEV, None, None, "lon"),
        P(LAT_LEV, None, "lon"),
        P(),
        P(LAT_LEV, None, None),
    )
    out_specs = (P(LAT_LEV, None, None), P("lon", LAT_LEV, None), P("lon", LAT_LEV, None), P())

    return jax.shard_map(
        per_device, mesh=torus, in_specs=in_specs, out_specs=out_specs, check_vma=False
    )
```

```python
import functools
import math

import jax
import jax.numpy as jnp
import numpy as np
from jax import lax
from jax.experimental import pallas as pl
from jax.experimental.pallas import tpu as pltpu
from jax.sharding import Mesh
from jax.sharding import PartitionSpec as P


MERIDIANS = 1440
ORDERS = 720
PADDED = 184
LAT_LEV = ("lat", "lev_0", "lev_1", "lev_2")
INNER = ("lev_1", "lev_2")
OUTER = "lev_0"
EPSILON = 1e-06
GROUPS = ((0,), (1, 2), (3, 4))
F32 = jnp.float32
BF16 = jnp.bfloat16
MIB = 1024 * 1024
CONTRACT = (((1,), (1,)), ((), ()))
SMEM = pl.BlockSpec(memory_space=pltpu.SMEM)
VMEM = pl.BlockSpec(memory_space=pltpu.VMEM)
HBM = pl.BlockSpec(memory_space=pltpu.HBM)
ANY = pl.BlockSpec(memory_space=pl.ANY)


def half_table(lon):
    order = np.arange(1, ORDERS + 1, dtype=np.int64)
    turns = (order[:, None] * np.arange(lon, dtype=np.int64)[None, :]) % MERIDIANS
    angle = turns.astype(np.float32) * np.float32(2.0 * math.pi / MERIDIANS)
    both = np.stack([np.cos(angle), np.sin(angle)]).reshape(2, 2, ORDERS // 4, 2, lon)
    rows = np.zeros((2, 2, 2, PADDED, lon), np.float32)
    rows[:, :, :, : ORDERS // 4] = both.transpose(1, 3, 0, 2, 4)
    return rows.reshape(2, 2, 2 * PADDED, lon)


def params(mib):
    return pltpu.CompilerParams(vmem_limit_bytes=mib * MIB)


def main_lanes(lon):
    return lon // 128 * 128


def packed_shape(cols, lon):
    main = main_lanes(lon)
    return cols + cols // (main // (lon - main)), main


def fold_tails(tail_ref, lon):
    main = main_lanes(lon)
    width = lon - main
    parts = main // width
    rows = tail_ref.shape[0] // parts
    low = lax.broadcasted_iota(jnp.int32, (rows, 128), 1) < width
    total = None
    for j in range(parts):
        piece = jnp.where(low, tail_ref[j * rows : (j + 1) * rows, :], 0.0)
        wide = jnp.concatenate([piece, jnp.zeros((rows, main - 128), F32)], axis=1)
        wide = pltpu.roll(wide, j * width, 1) if j else wide
        total = wide if total is None else total + wide
    return total


def unfold_tails(folded, tail_ref, lon):
    main = main_lanes(lon)
    width = lon - main
    rows = folded.shape[0]
    for j in range(main // width):
        wide = pltpu.roll(folded, main - j * width, 1) if j else folded
        tail_ref[j * rows : (j + 1) * rows, :] = wide[:, :128]


def put_packed(box, field, at, tail_ref, lon):
    main = main_lanes(lon)
    size = field.shape[0]
    box[at : at + size, :] = field[:, :main]
    tail_ref[at : at + size, 0 : lon - main] = field[:, main:].astype(F32)


def keep_of(mask):
    return mask.astype(F32).astype(BF16)


def pack_kernel(half_ref, u_ref, v_ref, t_ref, m_ref, o_ref, fields, mask, tails, sems):
    part = fields.shape[1]
    at = pl.ds((1 - half_ref[0]) * part, part)
    copies = [pltpu.make_async_copy(m_ref.at[0], mask, sems.at[3])]
    for f, ref in enumerate((t_ref, u_ref, v_ref)):
        copies.append(pltpu.make_async_copy(ref.at[0, at], fields.at[f], sems.at[f]))
    for c in copies:
        c.start()
    for c in copies:
        c.wait()
    size = part * fields.shape[2]
    keep = keep_of(mask[...])[None]
    lon = mask.shape[1]
    for f in range(3):
        put_packed(o_ref.at[0], (fields[f] * keep).reshape(size, lon), f * size, tails, lon)
    o_ref[0, 3 * size :, :] = fold_tails(tails, lon).astype(BF16)


def pack(half, u, v, t, mask):
    _, samples, levels, lon = u.shape
    part = samples // 2
    return pl.pallas_call(
        pack_kernel,
        out_shape=jax.ShapeDtypeStruct((1, *packed_shape(3 * part * levels, lon)), BF16),
        in_specs=[SMEM, HBM, HBM, HBM, HBM],
        out_specs=VMEM,
        scratch_shapes=[
            pltpu.VMEM((3, part, levels, lon), BF16),
            pltpu.VMEM((levels, lon), jnp.int32),
            pltpu.VMEM((3 * part * levels, 128), F32),
            pltpu.SemaphoreType.DMA((4,)),
        ],
        compiler_params=params(60),
        name="pack",
    )(half, u, v, t, mask)


def sums_kernel(v_ref, m_ref, _, sums_ref, vs, masks, sems):
    rows, samples, levels, lon = vs.shape
    copies = [
        (
            pltpu.make_async_copy(m_ref.at[j], masks.at[j], sems.at[j, 0]),
            pltpu.make_async_copy(v_ref.at[j], vs.at[j], sems.at[j, 1]),
        )
        for j in range(rows)
    ]
    for group in copies:
        for c in group:
            c.start()
    ones = jnp.ones((8, lon), BF16)
    for j in range(rows):
        for c in copies[j]:
            c.wait()
        keep = keep_of(masks[j])
        v = (vs[j] * keep[None]).reshape(samples * levels, lon)
        sums_ref[j : j + 1, :] = lax.dot_general(ones, v, CONTRACT, preferred_element_type=F32)[0:1]
        kept = lax.dot_general(ones, keep, CONTRACT, preferred_element_type=F32)[0:1]
        sums_ref[rows + j : rows + j + 1, :] = jnp.concatenate([kept] * samples, axis=1)


def zonal(v, mask, after):
    rows, samples, levels, lon = v.shape
    return pl.pallas_call(
        sums_kernel,
        out_shape=jax.ShapeDtypeStruct((2 * rows, samples * levels), F32),
        in_specs=[HBM, HBM, ANY],
        out_specs=VMEM,
        scratch_shapes=[
            pltpu.VMEM((rows, samples, levels, lon), BF16),
            pltpu.VMEM((rows, levels, lon), jnp.int32),
            pltpu.SemaphoreType.DMA((rows, 2)),
        ],
        compiler_params=params(60),
        name="sums",
    )(v, mask, after)


def send_kernel(groups, half_ref, u_ref, v_ref, t_ref, m_ref, _, *rest):
    n = len(groups)
    far_refs, near_refs = rest[: n - 1], rest[n - 1 : 2 * n - 1]
    us, vs, ts, masks, fars, nears, tails, sems, out_sems = rest[2 * n - 1 :]
    rows, samples, levels, lon = vs.shape
    part = samples // 2
    size = part * levels
    near = half_ref[0]
    far = 1 - near
    copies = []
    for j in range(rows):
        group = [
            pltpu.make_async_copy(m_ref.at[j], masks.at[j], sems.at[j, 0]),
            pltpu.make_async_copy(v_ref.at[j], vs.at[j], sems.at[j, 1]),
            pltpu.make_async_copy(u_ref.at[j], us.at[j], sems.at[j, 2]),
            pltpu.make_async_copy(t_ref.at[j], ts.at[j], sems.at[j, 3]),
        ]
        for c in group:
            c.start()
        copies.append(group)
    done = []
    for g, group in enumerate(groups):
        for i, j in enumerate(group):
            for c in copies[j]:
                c.wait()
            keep = keep_of(masks[j])
            for k, (where, box) in enumerate(((far, fars), (near, nears))):
                if k == 0 and g == 0:
                    continue
                ref = far_refs[g - 1] if k == 0 else near_refs[g]
                for f, field in enumerate((ts, us, vs)):
                    mine = (field[j, pl.ds(where * part, part)] * keep[None]).reshape(size, lon)
                    if k:
                        box[j, f * size : (f + 1) * size, :] = mine
                    else:
                        put_packed(box.at[j], mine, f * size, tails.at[j], lon)
                if not k:
                    box[j, 3 * size :, :] = fold_tails(tails.at[j], lon).astype(BF16)
                c = pltpu.make_async_copy(box.at[j], ref.at[i], out_sems.at[j, k])
                c.start()
                done.append(c)
    for c in done:
        c.wait()


def send(half, u, v, t, mask, after, groups):
    rows, samples, levels, lon = v.shape
    part = samples // 2
    unit = 3 * part * levels
    n = len(groups)
    wire = packed_shape(unit, lon)
    packed = [jax.ShapeDtypeStruct((len(g), unit, lon), BF16) for g in groups]
    sent = [jax.ShapeDtypeStruct((len(g), *wire), BF16) for g in groups[1:]]
    return pl.pallas_call(
        lambda *refs: send_kernel(groups, *refs),
        out_shape=(
            *sent,
            *packed,
        ),
        in_specs=[SMEM, HBM, HBM, HBM, HBM, ANY],
        out_specs=(HBM,) * (2 * n - 1),
        scratch_shapes=[
            pltpu.VMEM((rows, samples, levels, lon), BF16),
            pltpu.VMEM((rows, samples, levels, lon), BF16),
            pltpu.VMEM((rows, samples, levels, lon), BF16),
            pltpu.VMEM((rows, levels, lon), jnp.int32),
            pltpu.VMEM((rows, *wire), BF16),
            pltpu.VMEM((rows, unit, lon), BF16),
            pltpu.VMEM((rows, unit, 128), F32),
            pltpu.SemaphoreType.DMA((rows, 4)),
            pltpu.SemaphoreType.DMA((rows, 2)),
        ],
        compiler_params=params(60),
        name="send",
    )(half, u, v, t, mask, after)


def wave_kernel(half_ref, table_ref, own_ref, got_ref, _, *refs, flips):
    o_refs, (mix, tails) = refs[:-2], refs[-2:]
    n = table_ref.shape[2] // 2
    cols, lon = own_ref.shape[1:]
    main = main_lanes(lon)
    scale = 2.0 / (MERIDIANS * MERIDIANS)
    for i in range(got_ref.shape[0]):
        unfold_tails(got_ref[i, cols:].astype(F32), tails.at[i], lon)
        for at, end in ((0, main), (main, lon)):
            own = own_ref[i, :, at:end].astype(F32)
            got = tails[i, :, 0 : lon - main] if at else got_ref[i, 0:cols].astype(F32)
            for p, mixed in enumerate(((own - got).astype(BF16), (own + got).astype(BF16))):
                mix[i, p, 0:cols, at:end] = mixed
                mix[i, p, cols:, at:end] = mixed[2 * cols // 3 :]
        for p in range(2):
            x = mix[i, p]
            w = x.shape[0] // 2
            for flip, o_ref in zip(flips, o_refs):
                table = table_ref[1 - half_ref[0] if flip else half_ref[0], p]
                c = lax.dot_general(table, x, CONTRACT, preferred_element_type=F32)
                both = c[:n, :w] * c[:n, w:] + c[n:, :w] * c[n:, w:]
                o_ref[i, p] = (scale * both).astype(o_ref.dtype)


def waves(half, table, own, got, after, *flips):
    rows, cols, lon = own.shape
    shape = (rows, 2, PADDED, 2 * cols // 3)
    return pl.pallas_call(
        functools.partial(wave_kernel, flips=flips),
        out_shape=tuple(jax.ShapeDtypeStruct(shape, BF16 if f else F32) for f in flips),
        in_specs=[SMEM, VMEM, VMEM, VMEM, ANY],
        out_specs=(VMEM,) * len(flips),
        scratch_shapes=[
            pltpu.VMEM((rows, 2, 4 * cols // 3, lon), BF16),
            pltpu.VMEM((rows, cols, 128), F32),
        ],
        compiler_params=params(16),
        name="waves",
    )(half, table, own, got, after)


def join_kernel(first, parts, half_ref, *refs):
    own_refs, got_refs = refs[:parts], refs[parts : 2 * parts]
    heat_ref, mom_ref, heat, mom, sems = refs[-5:]
    copies = []
    at = 0
    for own_ref, got_ref in zip(own_refs, got_refs):
        for i in range(own_ref.shape[0]):
            zero = half_ref[0] == 0
            for p in range(2):
                own = own_ref[i, p]
                got = got_ref[i, p].astype(F32)
                a = jnp.where(zero, own, got)
                b = jnp.where(zero, got, own)
                w = own.shape[1] // 2
                low = lax.broadcasted_iota(jnp.int32, own.shape, 1) < w
                n = heat.shape[1] // 2
                every = pl.ds(p, n, stride=2)
                heat[at, every, :] = jnp.where(low, a, pltpu.roll(b, w, 1))[:n]
                mom[at, every, :] = jnp.where(low, pltpu.roll(a, w, 1), b)[:n]
            for k, (x, ref) in enumerate(((heat, heat_ref), (mom, mom_ref))):
                c = pltpu.make_async_copy(x.at[at], ref.at[first + at], sems.at[at, k])
                c.start()
                copies.append(c)
            at += 1
    for c in copies:
        c.wait()


def join(half, own, got, outs, rows, total):
    n, width = ORDERS // 2, own[0].shape[3]
    shape = jax.ShapeDtypeStruct((total, n, width), F32)
    parts = len(own)
    args = (half, *own, *got)
    specs = [SMEM] + [VMEM] * (2 * parts)
    extra = {}
    if outs is not None:
        extra = {"input_output_aliases": {len(args): 0, len(args) + 1: 1}}
        args += outs
        specs += [HBM, HBM]
    return pl.pallas_call(
        lambda *refs: join_kernel(rows[0], parts, *refs),
        out_shape=(shape, shape),
        in_specs=specs,
        out_specs=(HBM, HBM),
        scratch_shapes=[
            pltpu.VMEM((len(rows), n, width), F32),
            pltpu.VMEM((len(rows), n, width), F32),
            pltpu.SemaphoreType.DMA((len(rows), 2)),
        ],
        compiler_params=params(8),
        name="join",
        **extra,
    )(*args)


def cosines(first, rows, total):
    index = lax.broadcasted_iota(jnp.int32, (rows, 1), 0) + first
    return jnp.cos(((index.astype(F32) + 0.5) / total - 0.5) * math.pi)


def weight_of(first, rows, total):
    latitude = ((np.arange(first, first + rows) + 0.5) / total - 0.5) * math.pi
    return float(np.sum(np.cos(latitude)))


def weigh_kernel(total, place_ref, own_ref, lon_ref, depth_ref, d_ref, o_ref):
    rows, samples, levels = d_ref.shape
    band = place_ref[0] // 128 * 64 + place_ref[0] % 64
    depth = depth_ref[...]
    spread = jnp.concatenate([depth] * samples, axis=1)
    kept = own_ref[rows : 2 * rows] + lon_ref[rows : 2 * rows]
    mean = (own_ref[0:rows] + lon_ref[0:rows]) / jnp.maximum(kept, 1.0)
    weighted = mean * cosines(band * rows, rows, total) * spread
    for p in range(o_ref.shape[0]):
        o_ref[p, 0:rows, :] = weighted
        for b in range(samples):
            o_ref[p, 8 : 8 + rows, b * levels : (b + 1) * levels] = d_ref[:, b, :]


def band_kernel(total, rows, levels, place_ref, g_ref, mine_ref, s_ref, w_ref):
    peers, _, width = g_ref.shape
    span = peers * rows
    lane = lax.broadcasted_iota(jnp.int32, (1, width), 1) % levels
    so_far = jnp.zeros((1, width), F32)
    for p in range(peers):
        for r in range(rows):
            so_far = so_far + g_ref[p, r : r + 1, :]
            w_ref[p * rows + r : p * rows + r + 1, :] = so_far
            w_ref[span + p * rows + r : span + p * rows + r + 1, :] = g_ref[p, 8 + r : 9 + r, :]
    run = w_ref[0:span, :]
    step = 1
    while step < levels:
        run = run + jnp.where(lane >= step, pltpu.roll(run, step, 1), 0.0)
        step *= 2
    want = w_ref[span:, :]
    block = place_ref[0] // 128 * 8 + place_ref[0] % 64 // 8
    cosine = cosines(block * span, span, total)
    stats = (
        run[span - 1 : span],
        jnp.max(run, axis=0, keepdims=True),
        jnp.min(run, axis=0, keepdims=True),
        jnp.sum(cosine * run, axis=0, keepdims=True),
        jnp.sum(cosine * run * run, axis=0, keepdims=True),
        jnp.sum(cosine * want, axis=0, keepdims=True),
        jnp.sum(cosine * run * want, axis=0, keepdims=True),
        jnp.sum(cosine * want * want, axis=0, keepdims=True),
    )
    for p in range(s_ref.shape[0]):
        for i, stat in enumerate(stats):
            s_ref[p, i : i + 1, :] = stat
    w_ref[0:span, :] = run
    for p in range(peers):

        @pl.when(place_ref[0] % 8 == p)
        def _():
            mine_ref[...] = w_ref[p * rows : (p + 1) * rows, :]


def add_block(so_far, block, weight):
    s, hi, lo, run1, run2, want1, cross, want2 = block
    if so_far is None:
        return block
    off = so_far[0]
    return (
        off + s,
        jnp.maximum(so_far[1], off + hi),
        jnp.minimum(so_far[2], off + lo),
        so_far[3] + (run1 + off * weight),
        so_far[4] + (run2 + 2.0 * off * run1 + off * off * weight),
        so_far[5] + want1,
        so_far[6] + (cross + off * want1),
        so_far[7] + want2,
    )


def half_kernel(total, span, place_ref, mine_ref, s_ref, own_ref, half_ref):
    blocks = s_ref.shape[0]
    here = place_ref[0] % 64 // 8
    north = place_ref[0] // 128 == 1
    stats = None
    offset = jnp.zeros((1, s_ref.shape[2]), F32)
    for z in range(blocks):
        if z:
            offset = jnp.where(here == z, stats[0], offset)
        weights = [weight_of((h * blocks + z) * span, span, total) for h in range(2)]
        weight = jnp.where(north, weights[1], weights[0])
        stats = add_block(stats, [s_ref[z, i : i + 1, :] for i in range(8)], weight)
    own_ref[...] = mine_ref[...] + offset
    for i, stat in enumerate(stats):
        half_ref[i : i + 1, :] = stat


def finish_kernel(total, place_ref, own_ref, near_ref, far_ref, psi_ref, loss_ref):
    _, samples, levels = psi_ref.shape
    north = place_ref[0] // 128 == 1
    near = near_ref[...]
    far = far_ref[...]
    south_half = jnp.where(north, far, near)
    north_half = jnp.where(north, near, far)
    weight = weight_of(total // 2, total // 2, total)
    stats = add_block(
        [south_half[i : i + 1] for i in range(8)], [north_half[i : i + 1] for i in range(8)], weight
    )
    peak = jnp.max(jnp.maximum(jnp.abs(stats[1]), jnp.abs(stats[2])), axis=1, keepdims=True)
    scale = peak + EPSILON
    psi = (own_ref[...] + jnp.where(north, far[0:1], 0.0)) / scale
    for b in range(samples):
        psi_ref[:, b, :] = psi[:, b * levels : (b + 1) * levels]
    a, b, c = (jnp.sum(stats[i], axis=1, keepdims=True) for i in (4, 6, 7))
    loss = (a / scale / scale - 2.0 * (b / scale) + c) / (samples * levels * total)
    loss_ref[...] = jnp.broadcast_to(loss, loss_ref.shape)


def small(body, out_shape, *args, scratch=(), after=None):
    many = isinstance(out_shape, tuple)
    specs = [SMEM] + [VMEM] * (len(args) - 1)
    if after is not None:
        plain, count = body, len(args)
        body = lambda *refs: plain(*refs[:count], *refs[count + 1 :])
        args += (after,)
        specs.append(ANY)
    return pl.pallas_call(
        body,
        out_shape=out_shape,
        in_specs=specs,
        out_specs=(VMEM,) * len(out_shape) if many else VMEM,
        scratch_shapes=scratch,
        compiler_params=params(2),
    )(*args)


def all_of(x, axes):
    return lax.all_to_all(x, axes, split_axis=0, concat_axis=0, tiled=True)


def floats(*shape):
    return jax.ShapeDtypeStruct(shape, F32)


def per_device(u, v, t, mask, depth, desired):
    bands, samples, levels, lon = v.shape
    width = samples * levels
    total = bands * lax.axis_size(LAT_LEV)
    half = lax.axis_index("lon")[None].astype(jnp.int32)
    place = lax.axis_index(("lat", "lon", "lev_0", "lev_1", "lev_2"))[None].astype(jnp.int32)
    across = [(0, 1), (1, 0)]
    table = jnp.asarray(half_table(lon), BF16)

    def swap(x):
        return lax.ppermute(x, "lon", across)

    first = pack(half, u, v, t, mask)
    sums = zonal(v, mask, first)
    packed = send(half, u, v, t, mask, sums, GROUPS)
    rest, own = packed[: len(GROUPS) - 1], packed[len(GROUPS) - 1 :]
    got = [swap(first)]
    by_lon = swap(sums)
    got += [swap(x) for x in rest]

    peers = lax.axis_size(INNER)
    outer = lax.axis_size(OUTER)
    rows = small(
        lambda *refs: weigh_kernel(total, *refs),
        floats(peers, 16, width),
        place,
        sums,
        by_lon,
        depth[None],
        desired,
    )
    near_bands = all_of(rows, INNER)
    far0, near0 = waves(half, table, own[0], got[0], rows, True, False)
    span = bands * peers
    mine, stats = small(
        lambda *refs: band_kernel(total, bands, levels, *refs),
        (floats(bands, width), floats(outer, 8, width)),
        place,
        near_bands,
        scratch=[pltpu.VMEM((2 * span, width), F32)],
    )
    all_stats = all_of(stats, OUTER)
    mine, near_half = small(
        lambda *refs: half_kernel(total, span, *refs),
        (floats(bands, width), floats(8, width)),
        place,
        mine,
        all_stats,
    )
    far_half = lax.ppermute(near_half, ("lat", "lon"), [(i, 3 - i) for i in range(4)])
    far1, near1 = waves(half, table, own[1], got[1], stats, True, False)
    (far2,) = waves(half, table, own[2], got[2], near_half, True)
    (near2,) = waves(half, table, own[2], got[2], near_half, False)
    psi, loss = small(
        lambda *refs: finish_kernel(total, *refs),
        (floats(bands, samples, levels), floats(1, width)),
        place,
        mine,
        near_half,
        far_half,
        after=near2,
    )

    back = [swap(x) for x in (far0, far1, far2)]
    kept = [near0, near1, near2]
    outs = join(half, kept[:2], back[:2], None, GROUPS[0] + GROUPS[1], bands)
    outs = join(half, kept[2:], back[2:], outs, GROUPS[2], bands)
    heat, momentum = (jnp.transpose(x, (1, 0, 2)) for x in outs)
    return psi, heat, momentum, loss[0, 0]


def solution(mesh):
    torus = Mesh(
        mesh.devices.reshape(mesh.shape["lat"], mesh.shape["lon"], 8, 4, 2),
        ("lat", "lon", "lev_0", "lev_1", "lev_2"),
    )
    in_specs = (
        P(LAT_LEV, None, None, "lon"),
        P(LAT_LEV, None, None, "lon"),
        P(LAT_LEV, None, None, "lon"),
        P(LAT_LEV, None, "lon"),
        P(),
        P(LAT_LEV, None, None),
    )
    out_specs = (P(LAT_LEV, None, None), P("lon", LAT_LEV, None), P("lon", LAT_LEV, None), P())

    return jax.shard_map(
        per_device, mesh=torus, in_specs=in_specs, out_specs=out_specs, check_vma=False
    )
```

```python
import functools
import math

import jax
import jax.numpy as jnp
import numpy as np
from jax import lax
from jax.experimental import pallas as pl
from jax.experimental.pallas import tpu as pltpu
from jax.sharding import Mesh
from jax.sharding import PartitionSpec as P


MERIDIANS = 1440
ORDERS = 720
PADDED = 184
LAT_LEV = ("lat", "lev_0", "lev_1", "lev_2")
INNER = ("lev_1", "lev_2")
OUTER = "lev_0"
EPSILON = 1e-06
GROUPS = ((0,), (1, 2), (3, 4))
F32 = jnp.float32
BF16 = jnp.bfloat16
MIB = 1024 * 1024
CONTRACT = (((1,), (1,)), ((), ()))
SMEM = pl.BlockSpec(memory_space=pltpu.SMEM)
VMEM = pl.BlockSpec(memory_space=pltpu.VMEM)
HBM = pl.BlockSpec(memory_space=pltpu.HBM)
ANY = pl.BlockSpec(memory_space=pl.ANY)


def half_table(lon):
    order = np.arange(1, ORDERS + 1, dtype=np.int64)
    turns = (order[:, None] * np.arange(lon, dtype=np.int64)[None, :]) % MERIDIANS
    angle = turns.astype(np.float32) * np.float32(2.0 * math.pi / MERIDIANS)
    both = np.stack([np.cos(angle), np.sin(angle)]).reshape(2, 2, ORDERS // 4, 2, lon)
    rows = np.zeros((2, 2, 2, PADDED, lon), np.float32)
    rows[:, :, :, : ORDERS // 4] = both.transpose(1, 3, 0, 2, 4)
    return rows.reshape(2, 2, 2 * PADDED, lon)


def params(mib):
    return pltpu.CompilerParams(vmem_limit_bytes=mib * MIB)


def main_lanes(lon):
    return lon // 128 * 128


def packed_shape(cols, lon):
    main = main_lanes(lon)
    return cols + cols // (main // (lon - main)), main


def fold_tails(tail_ref, lon):
    main = main_lanes(lon)
    width = lon - main
    parts = main // width
    rows = tail_ref.shape[0] // parts
    low = lax.broadcasted_iota(jnp.int32, (rows, 128), 1) < width
    total = None
    for j in range(parts):
        piece = jnp.where(low, tail_ref[j * rows : (j + 1) * rows, :], 0.0)
        wide = jnp.concatenate([piece, jnp.zeros((rows, main - 128), F32)], axis=1)
        wide = pltpu.roll(wide, j * width, 1) if j else wide
        total = wide if total is None else total + wide
    return total


def unfold_tails(folded, tail_ref, lon):
    main = main_lanes(lon)
    width = lon - main
    rows = folded.shape[0]
    for j in range(main // width):
        wide = pltpu.roll(folded, main - j * width, 1) if j else folded
        tail_ref[j * rows : (j + 1) * rows, :] = wide[:, :128]


def put_packed(box, field, at, tail_ref, lon):
    main = main_lanes(lon)
    size = field.shape[0]
    box[at : at + size, :] = field[:, :main]
    tail_ref[at : at + size, 0 : lon - main] = field[:, main:].astype(F32)


def keep_of(mask):
    return mask.astype(F32).astype(BF16)


def pack_kernel(half_ref, u_ref, v_ref, t_ref, m_ref, o_ref, fields, mask, tails, sems):
    part = fields.shape[1]
    at = pl.ds((1 - half_ref[0]) * part, part)
    copies = [pltpu.make_async_copy(m_ref.at[0], mask, sems.at[3])]
    for f, ref in enumerate((t_ref, u_ref, v_ref)):
        copies.append(pltpu.make_async_copy(ref.at[0, at], fields.at[f], sems.at[f]))
    for c in copies:
        c.start()
    for c in copies:
        c.wait()
    size = part * fields.shape[2]
    keep = keep_of(mask[...])[None]
    lon = mask.shape[1]
    for f in range(3):
        put_packed(o_ref.at[0], (fields[f] * keep).reshape(size, lon), f * size, tails, lon)
    o_ref[0, 3 * size :, :] = fold_tails(tails, lon).astype(BF16)


def pack(half, u, v, t, mask):
    _, samples, levels, lon = u.shape
    part = samples // 2
    return pl.pallas_call(
        pack_kernel,
        out_shape=jax.ShapeDtypeStruct((1, *packed_shape(3 * part * levels, lon)), BF16),
        in_specs=[SMEM, HBM, HBM, HBM, HBM],
        out_specs=VMEM,
        scratch_shapes=[
            pltpu.VMEM((3, part, levels, lon), BF16),
            pltpu.VMEM((levels, lon), jnp.int32),
            pltpu.VMEM((3 * part * levels, 128), F32),
            pltpu.SemaphoreType.DMA((4,)),
        ],
        compiler_params=params(60),
        name="pack",
    )(half, u, v, t, mask)


def send_kernel(groups, half_ref, u_ref, v_ref, t_ref, m_ref, _, *rest):
    n = len(groups)
    far_refs, near_refs, sums_ref = rest[: n - 1], rest[n - 1 : 2 * n - 1], rest[2 * n - 1]
    us, vs, ts, masks, fars, nears, tails, sems, out_sems = rest[2 * n :]
    rows, samples, levels, lon = vs.shape
    part = samples // 2
    size = part * levels
    near = half_ref[0]
    far = 1 - near
    copies = []
    for j in range(rows):
        group = [
            pltpu.make_async_copy(m_ref.at[j], masks.at[j], sems.at[j, 0]),
            pltpu.make_async_copy(v_ref.at[j], vs.at[j], sems.at[j, 1]),
            pltpu.make_async_copy(u_ref.at[j], us.at[j], sems.at[j, 2]),
            pltpu.make_async_copy(t_ref.at[j], ts.at[j], sems.at[j, 3]),
        ]
        for c in group:
            c.start()
        copies.append(group)
    ones = jnp.ones((8, lon), BF16)
    done = []
    for g, group in enumerate(groups):
        for i, j in enumerate(group):
            for c in copies[j]:
                c.wait()
            keep = keep_of(masks[j])
            v = (vs[j] * keep[None]).reshape(samples * levels, lon)
            sums_ref[j : j + 1, :] = lax.dot_general(
                ones, v, CONTRACT, preferred_element_type=F32
            )[0:1]
            kept = lax.dot_general(ones, keep, CONTRACT, preferred_element_type=F32)[0:1]
            sums_ref[rows + j : rows + j + 1, :] = jnp.concatenate([kept] * samples, axis=1)
            for k, (where, box) in enumerate(((far, fars), (near, nears))):
                if k == 0 and g == 0:
                    continue
                ref = far_refs[g - 1] if k == 0 else near_refs[g]
                for f, field in enumerate((ts, us, vs)):
                    mine = (field[j, pl.ds(where * part, part)] * keep[None]).reshape(size, lon)
                    if k:
                        box[j, f * size : (f + 1) * size, :] = mine
                    else:
                        put_packed(box.at[j], mine, f * size, tails.at[j], lon)
                if not k:
                    box[j, 3 * size :, :] = fold_tails(tails.at[j], lon).astype(BF16)
                c = pltpu.make_async_copy(box.at[j], ref.at[i], out_sems.at[j, k])
                c.start()
                done.append(c)
    for c in done:
        c.wait()


def send(half, u, v, t, mask, after, groups):
    rows, samples, levels, lon = v.shape
    part = samples // 2
    unit = 3 * part * levels
    n = len(groups)
    wire = packed_shape(unit, lon)
    packed = [jax.ShapeDtypeStruct((len(g), unit, lon), BF16) for g in groups]
    sent = [jax.ShapeDtypeStruct((len(g), *wire), BF16) for g in groups[1:]]
    return pl.pallas_call(
        lambda *refs: send_kernel(groups, *refs),
        out_shape=(
            *sent,
            *packed,
            jax.ShapeDtypeStruct((2 * rows, samples * levels), F32),
        ),
        in_specs=[SMEM, HBM, HBM, HBM, HBM, ANY],
        out_specs=(HBM,) * (2 * n - 1) + (VMEM,),
        scratch_shapes=[
            pltpu.VMEM((rows, samples, levels, lon), BF16),
            pltpu.VMEM((rows, samples, levels, lon), BF16),
            pltpu.VMEM((rows, samples, levels, lon), BF16),
            pltpu.VMEM((rows, levels, lon), jnp.int32),
            pltpu.VMEM((rows, *wire), BF16),
            pltpu.VMEM((rows, unit, lon), BF16),
            pltpu.VMEM((rows, unit, 128), F32),
            pltpu.SemaphoreType.DMA((rows, 4)),
            pltpu.SemaphoreType.DMA((rows, 2)),
        ],
        compiler_params=params(60),
        name="send",
    )(half, u, v, t, mask, after)


def wave_kernel(half_ref, table_ref, own_ref, got_ref, _, *refs, flips):
    o_refs, (mix, tails) = refs[:-2], refs[-2:]
    n = table_ref.shape[2] // 2
    cols, lon = own_ref.shape[1:]
    main = main_lanes(lon)
    scale = 2.0 / (MERIDIANS * MERIDIANS)
    for i in range(got_ref.shape[0]):
        unfold_tails(got_ref[i, cols:].astype(F32), tails.at[i], lon)
        for at, end in ((0, main), (main, lon)):
            own = own_ref[i, :, at:end].astype(F32)
            got = tails[i, :, 0 : lon - main] if at else got_ref[i, 0:cols].astype(F32)
            for p, mixed in enumerate(((own - got).astype(BF16), (own + got).astype(BF16))):
                mix[i, p, 0:cols, at:end] = mixed
                mix[i, p, cols:, at:end] = mixed[2 * cols // 3 :]
        for p in range(2):
            x = mix[i, p]
            w = x.shape[0] // 2
            for flip, o_ref in zip(flips, o_refs):
                table = table_ref[1 - half_ref[0] if flip else half_ref[0], p]
                c = lax.dot_general(table, x, CONTRACT, preferred_element_type=F32)
                both = c[:n, :w] * c[:n, w:] + c[n:, :w] * c[n:, w:]
                o_ref[i, p] = (scale * both).astype(o_ref.dtype)


def waves(half, table, own, got, after, *flips):
    rows, cols, lon = own.shape
    shape = (rows, 2, PADDED, 2 * cols // 3)
    return pl.pallas_call(
        functools.partial(wave_kernel, flips=flips),
        out_shape=tuple(jax.ShapeDtypeStruct(shape, BF16 if f else F32) for f in flips),
        in_specs=[SMEM, VMEM, VMEM, VMEM, ANY],
        out_specs=(VMEM,) * len(flips),
        scratch_shapes=[
            pltpu.VMEM((rows, 2, 4 * cols // 3, lon), BF16),
            pltpu.VMEM((rows, cols, 128), F32),
        ],
        compiler_params=params(16),
        name="waves",
    )(half, table, own, got, after)


def join_kernel(first, parts, half_ref, *refs):
    own_refs, got_refs = refs[:parts], refs[parts : 2 * parts]
    heat_ref, mom_ref, heat, mom, sems = refs[-5:]
    copies = []
    at = 0
    for own_ref, got_ref in zip(own_refs, got_refs):
        for i in range(own_ref.shape[0]):
            zero = half_ref[0] == 0
            for p in range(2):
                own = own_ref[i, p]
                got = got_ref[i, p].astype(F32)
                a = jnp.where(zero, own, got)
                b = jnp.where(zero, got, own)
                w = own.shape[1] // 2
                low = lax.broadcasted_iota(jnp.int32, own.shape, 1) < w
                n = heat.shape[1] // 2
                every = pl.ds(p, n, stride=2)
                heat[at, every, :] = jnp.where(low, a, pltpu.roll(b, w, 1))[:n]
                mom[at, every, :] = jnp.where(low, pltpu.roll(a, w, 1), b)[:n]
            for k, (x, ref) in enumerate(((heat, heat_ref), (mom, mom_ref))):
                c = pltpu.make_async_copy(x.at[at], ref.at[first + at], sems.at[at, k])
                c.start()
                copies.append(c)
            at += 1
    for c in copies:
        c.wait()


def join(half, own, got, outs, rows, total):
    n, width = ORDERS // 2, own[0].shape[3]
    shape = jax.ShapeDtypeStruct((total, n, width), F32)
    parts = len(own)
    args = (half, *own, *got)
    specs = [SMEM] + [VMEM] * (2 * parts)
    extra = {}
    if outs is not None:
        extra = {"input_output_aliases": {len(args): 0, len(args) + 1: 1}}
        args += outs
        specs += [HBM, HBM]
    return pl.pallas_call(
        lambda *refs: join_kernel(rows[0], parts, *refs),
        out_shape=(shape, shape),
        in_specs=specs,
        out_specs=(HBM, HBM),
        scratch_shapes=[
            pltpu.VMEM((len(rows), n, width), F32),
            pltpu.VMEM((len(rows), n, width), F32),
            pltpu.SemaphoreType.DMA((len(rows), 2)),
        ],
        compiler_params=params(8),
        name="join",
        **extra,
    )(*args)


def cosines(first, rows, total):
    index = lax.broadcasted_iota(jnp.int32, (rows, 1), 0) + first
    return jnp.cos(((index.astype(F32) + 0.5) / total - 0.5) * math.pi)


def weight_of(first, rows, total):
    latitude = ((np.arange(first, first + rows) + 0.5) / total - 0.5) * math.pi
    return float(np.sum(np.cos(latitude)))


def weigh_kernel(total, place_ref, own_ref, lon_ref, depth_ref, d_ref, o_ref):
    rows, samples, levels = d_ref.shape
    band = place_ref[0] // 128 * 64 + place_ref[0] % 64
    depth = depth_ref[...]
    spread = jnp.concatenate([depth] * samples, axis=1)
    kept = own_ref[rows : 2 * rows] + lon_ref[rows : 2 * rows]
    mean = (own_ref[0:rows] + lon_ref[0:rows]) / jnp.maximum(kept, 1.0)
    weighted = mean * cosines(band * rows, rows, total) * spread
    for p in range(o_ref.shape[0]):
        o_ref[p, 0:rows, :] = weighted
        for b in range(samples):
            o_ref[p, 8 : 8 + rows, b * levels : (b + 1) * levels] = d_ref[:, b, :]


def band_kernel(total, rows, levels, place_ref, g_ref, mine_ref, s_ref, w_ref):
    peers, _, width = g_ref.shape
    span = peers * rows
    lane = lax.broadcasted_iota(jnp.int32, (1, width), 1) % levels
    so_far = jnp.zeros((1, width), F32)
    for p in range(peers):
        for r in range(rows):
            so_far = so_far + g_ref[p, r : r + 1, :]
            w_ref[p * rows + r : p * rows + r + 1, :] = so_far
            w_ref[span + p * rows + r : span + p * rows + r + 1, :] = g_ref[p, 8 + r : 9 + r, :]
    run = w_ref[0:span, :]
    step = 1
    while step < levels:
        run = run + jnp.where(lane >= step, pltpu.roll(run, step, 1), 0.0)
        step *= 2
    want = w_ref[span:, :]
    block = place_ref[0] // 128 * 8 + place_ref[0] % 64 // 8
    cosine = cosines(block * span, span, total)
    stats = (
        run[span - 1 : span],
        jnp.max(run, axis=0, keepdims=True),
        jnp.min(run, axis=0, keepdims=True),
        jnp.sum(cosine * run, axis=0, keepdims=True),
        jnp.sum(cosine * run * run, axis=0, keepdims=True),
        jnp.sum(cosine * want, axis=0, keepdims=True),
        jnp.sum(cosine * run * want, axis=0, keepdims=True),
        jnp.sum(cosine * want * want, axis=0, keepdims=True),
    )
    for p in range(s_ref.shape[0]):
        for i, stat in enumerate(stats):
            s_ref[p, i : i + 1, :] = stat
    w_ref[0:span, :] = run
    for p in range(peers):

        @pl.when(place_ref[0] % 8 == p)
        def _():
            mine_ref[...] = w_ref[p * rows : (p + 1) * rows, :]


def add_block(so_far, block, weight):
    s, hi, lo, run1, run2, want1, cross, want2 = block
    if so_far is None:
        return block
    off = so_far[0]
    return (
        off + s,
        jnp.maximum(so_far[1], off + hi),
        jnp.minimum(so_far[2], off + lo),
        so_far[3] + (run1 + off * weight),
        so_far[4] + (run2 + 2.0 * off * run1 + off * off * weight),
        so_far[5] + want1,
        so_far[6] + (cross + off * want1),
        so_far[7] + want2,
    )


def half_kernel(total, span, place_ref, mine_ref, s_ref, own_ref, half_ref):
    blocks = s_ref.shape[0]
    here = place_ref[0] % 64 // 8
    north = place_ref[0] // 128 == 1
    stats = None
    offset = jnp.zeros((1, s_ref.shape[2]), F32)
    for z in range(blocks):
        if z:
            offset = jnp.where(here == z, stats[0], offset)
        weights = [weight_of((h * blocks + z) * span, span, total) for h in range(2)]
        weight = jnp.where(north, weights[1], weights[0])
        stats = add_block(stats, [s_ref[z, i : i + 1, :] for i in range(8)], weight)
    own_ref[...] = mine_ref[...] + offset
    for i, stat in enumerate(stats):
        half_ref[i : i + 1, :] = stat


def finish_kernel(total, place_ref, own_ref, near_ref, far_ref, psi_ref, loss_ref):
    _, samples, levels = psi_ref.shape
    north = place_ref[0] // 128 == 1
    near = near_ref[...]
    far = far_ref[...]
    south_half = jnp.where(north, far, near)
    north_half = jnp.where(north, near, far)
    weight = weight_of(total // 2, total // 2, total)
    stats = add_block(
        [south_half[i : i + 1] for i in range(8)], [north_half[i : i + 1] for i in range(8)], weight
    )
    peak = jnp.max(jnp.maximum(jnp.abs(stats[1]), jnp.abs(stats[2])), axis=1, keepdims=True)
    scale = peak + EPSILON
    psi = (own_ref[...] + jnp.where(north, far[0:1], 0.0)) / scale
    for b in range(samples):
        psi_ref[:, b, :] = psi[:, b * levels : (b + 1) * levels]
    a, b, c = (jnp.sum(stats[i], axis=1, keepdims=True) for i in (4, 6, 7))
    loss = (a / scale / scale - 2.0 * (b / scale) + c) / (samples * levels * total)
    loss_ref[...] = jnp.broadcast_to(loss, loss_ref.shape)


def small(body, out_shape, *args, scratch=(), after=None):
    many = isinstance(out_shape, tuple)
    specs = [SMEM] + [VMEM] * (len(args) - 1)
    if after is not None:
        plain, count = body, len(args)
        body = lambda *refs: plain(*refs[:count], *refs[count + 1 :])
        args += (after,)
        specs.append(ANY)
    return pl.pallas_call(
        body,
        out_shape=out_shape,
        in_specs=specs,
        out_specs=(VMEM,) * len(out_shape) if many else VMEM,
        scratch_shapes=scratch,
        compiler_params=params(2),
    )(*args)


def all_of(x, axes):
    return lax.all_to_all(x, axes, split_axis=0, concat_axis=0, tiled=True)


def floats(*shape):
    return jax.ShapeDtypeStruct(shape, F32)


def per_device(u, v, t, mask, depth, desired):
    bands, samples, levels, lon = v.shape
    width = samples * levels
    total = bands * lax.axis_size(LAT_LEV)
    half = lax.axis_index("lon")[None].astype(jnp.int32)
    place = lax.axis_index(("lat", "lon", "lev_0", "lev_1", "lev_2"))[None].astype(jnp.int32)
    across = [(0, 1), (1, 0)]
    table = jnp.asarray(half_table(lon), BF16)

    def swap(x):
        return lax.ppermute(x, "lon", across)

    first = pack(half, u, v, t, mask)
    *packed, sums = send(half, u, v, t, mask, first, GROUPS)
    rest, own = packed[: len(GROUPS) - 1], packed[len(GROUPS) - 1 :]
    got = [swap(first)]
    by_lon = swap(sums)
    got += [swap(x) for x in rest]

    peers = lax.axis_size(INNER)
    outer = lax.axis_size(OUTER)
    rows = small(
        lambda *refs: weigh_kernel(total, *refs),
        floats(peers, 16, width),
        place,
        sums,
        by_lon,
        depth[None],
        desired,
    )
    near_bands = all_of(rows, INNER)
    far0, near0 = waves(half, table, own[0], got[0], rows, True, False)
    span = bands * peers
    mine, stats = small(
        lambda *refs: band_kernel(total, bands, levels, *refs),
        (floats(bands, width), floats(outer, 8, width)),
        place,
        near_bands,
        scratch=[pltpu.VMEM((2 * span, width), F32)],
    )
    all_stats = all_of(stats, OUTER)
    mine, near_half = small(
        lambda *refs: half_kernel(total, span, *refs),
        (floats(bands, width), floats(8, width)),
        place,
        mine,
        all_stats,
    )
    far_half = lax.ppermute(near_half, ("lat", "lon"), [(i, 3 - i) for i in range(4)])
    far1, near1 = waves(half, table, own[1], got[1], stats, True, False)
    (far2,) = waves(half, table, own[2], got[2], near_half, True)
    (near2,) = waves(half, table, own[2], got[2], near_half, False)
    psi, loss = small(
        lambda *refs: finish_kernel(total, *refs),
        (floats(bands, samples, levels), floats(1, width)),
        place,
        mine,
        near_half,
        far_half,
        after=near2,
    )

    back = [swap(x) for x in (far0, far1, far2)]
    kept = [near0, near1, near2]
    outs = join(half, kept[:2], back[:2], None, GROUPS[0] + GROUPS[1], bands)
    outs = join(half, kept[2:], back[2:], outs, GROUPS[2], bands)
    heat, momentum = (jnp.transpose(x, (1, 0, 2)) for x in outs)
    return psi, heat, momentum, loss[0, 0]


def solution(mesh):
    torus = Mesh(
        mesh.devices.reshape(mesh.shape["lat"], mesh.shape["lon"], 8, 4, 2),
        ("lat", "lon", "lev_0", "lev_1", "lev_2"),
    )
    in_specs = (
        P(LAT_LEV, None, None, "lon"),
        P(LAT_LEV, None, None, "lon"),
        P(LAT_LEV, None, None, "lon"),
        P(LAT_LEV, None, "lon"),
        P(),
        P(LAT_LEV, None, None),
    )
    out_specs = (P(LAT_LEV, None, None), P("lon", LAT_LEV, None), P("lon", LAT_LEV, None), P())

    return jax.shard_map(
        per_device, mesh=torus, in_specs=in_specs, out_specs=out_specs, check_vma=False
    )
```

```python
import functools
import math

import jax
import jax.numpy as jnp
import numpy as np
from jax import lax
from jax.experimental import pallas as pl
from jax.experimental.pallas import tpu as pltpu
from jax.sharding import Mesh
from jax.sharding import PartitionSpec as P


MERIDIANS = 1440
ORDERS = 720
PADDED = 184
LAT_LEV = ("lat", "lev_0", "lev_1", "lev_2")
INNER = ("lev_1", "lev_2")
OUTER = "lev_0"
EPSILON = 1e-06
GROUPS = ((0,), (1, 2), (3, 4))
F32 = jnp.float32
BF16 = jnp.bfloat16
MIB = 1024 * 1024
CONTRACT = (((1,), (1,)), ((), ()))
SMEM = pl.BlockSpec(memory_space=pltpu.SMEM)
VMEM = pl.BlockSpec(memory_space=pltpu.VMEM)
HBM = pl.BlockSpec(memory_space=pltpu.HBM)
ANY = pl.BlockSpec(memory_space=pl.ANY)


def half_table(lon):
    order = np.arange(1, ORDERS + 1, dtype=np.int64)
    turns = (order[:, None] * np.arange(lon, dtype=np.int64)[None, :]) % MERIDIANS
    angle = turns.astype(np.float32) * np.float32(2.0 * math.pi / MERIDIANS)
    both = np.stack([np.cos(angle), np.sin(angle)]).reshape(2, 2, ORDERS // 4, 2, lon)
    rows = np.zeros((2, 2, 2, PADDED, lon), np.float32)
    rows[:, :, :, : ORDERS // 4] = both.transpose(1, 3, 0, 2, 4)
    return rows.reshape(2, 2, 2 * PADDED, lon)


def params(mib):
    return pltpu.CompilerParams(vmem_limit_bytes=mib * MIB)


def main_lanes(lon):
    return lon // 128 * 128


def packed_shape(cols, lon):
    main = main_lanes(lon)
    return cols + cols // (main // (lon - main)), main


def fold_tails(tail_ref, lon):
    main = main_lanes(lon)
    width = lon - main
    parts = main // width
    rows = tail_ref.shape[0] // parts
    low = lax.broadcasted_iota(jnp.int32, (rows, 128), 1) < width
    total = None
    for j in range(parts):
        piece = jnp.where(low, tail_ref[j * rows : (j + 1) * rows, :], 0.0)
        wide = jnp.concatenate([piece, jnp.zeros((rows, main - 128), F32)], axis=1)
        wide = pltpu.roll(wide, j * width, 1) if j else wide
        total = wide if total is None else total + wide
    return total


def unfold_tails(folded, tail_ref, lon):
    main = main_lanes(lon)
    width = lon - main
    rows = folded.shape[0]
    for j in range(main // width):
        wide = pltpu.roll(folded, main - j * width, 1) if j else folded
        tail_ref[j * rows : (j + 1) * rows, :] = wide[:, :128]


def put_packed(box, field, at, tail_ref, lon):
    main = main_lanes(lon)
    size = field.shape[0]
    box[at : at + size, :] = field[:, :main]
    tail_ref[at : at + size, 0 : lon - main] = field[:, main:].astype(F32)


def keep_of(mask):
    return mask.astype(F32).astype(BF16)


def first_kernel(half_ref, u_ref, v_ref, t_ref, m_ref, o_ref, sums_ref, us, vs, ts, masks, tails, sems):
    rows, samples, levels, lon = vs.shape
    part = samples // 2
    size = part * levels
    far = 1 - half_ref[0]
    at = pl.ds(far * part, part)
    copies = []
    for j in range(rows):
        copies.append(
            [
                pltpu.make_async_copy(m_ref.at[j], masks.at[j], sems.at[j, 0]),
                pltpu.make_async_copy(v_ref.at[j], vs.at[j], sems.at[j, 1]),
            ]
        )
    extra = [
        pltpu.make_async_copy(u_ref.at[0, at], us, sems.at[0, 2]),
        pltpu.make_async_copy(t_ref.at[0, at], ts, sems.at[0, 3]),
    ]
    for group in (copies[0], extra, *copies[1:]):
        for c in group:
            c.start()
    ones = jnp.ones((8, lon), BF16)
    for j in range(rows):
        for c in copies[j]:
            c.wait()
        keep = keep_of(masks[j])
        v = (vs[j] * keep[None]).reshape(samples * levels, lon)
        sums_ref[j : j + 1, :] = lax.dot_general(ones, v, CONTRACT, preferred_element_type=F32)[0:1]
        kept = lax.dot_general(ones, keep, CONTRACT, preferred_element_type=F32)[0:1]
        sums_ref[rows + j : rows + j + 1, :] = jnp.concatenate([kept] * samples, axis=1)
    for c in extra:
        c.wait()
    keep = keep_of(masks[0])[None]
    for f, field in enumerate((ts[...], us[...], vs[0, at])):
        put_packed(o_ref.at[0], (field * keep).reshape(size, lon), f * size, tails, lon)
    o_ref[0, 3 * size :, :] = fold_tails(tails, lon).astype(BF16)


def first_part(half, u, v, t, mask):
    rows, samples, levels, lon = v.shape
    part = samples // 2
    return pl.pallas_call(
        first_kernel,
        out_shape=(
            jax.ShapeDtypeStruct((1, *packed_shape(3 * part * levels, lon)), BF16),
            jax.ShapeDtypeStruct((2 * rows, samples * levels), F32),
        ),
        in_specs=[SMEM, HBM, HBM, HBM, HBM],
        out_specs=(VMEM, VMEM),
        scratch_shapes=[
            pltpu.VMEM((part, levels, lon), BF16),
            pltpu.VMEM((rows, samples, levels, lon), BF16),
            pltpu.VMEM((part, levels, lon), BF16),
            pltpu.VMEM((rows, levels, lon), jnp.int32),
            pltpu.VMEM((3 * part * levels, 128), F32),
            pltpu.SemaphoreType.DMA((rows, 4)),
        ],
        compiler_params=params(60),
        name="sums",
    )(half, u, v, t, mask)


def send_kernel(groups, half_ref, u_ref, v_ref, t_ref, m_ref, _, *rest):
    n = len(groups)
    far_refs, near_refs = rest[: n - 1], rest[n - 1 : 2 * n - 1]
    us, vs, ts, masks, fars, nears, tails, sems, out_sems = rest[2 * n - 1 :]
    rows, samples, levels, lon = vs.shape
    part = samples // 2
    size = part * levels
    near = half_ref[0]
    far = 1 - near
    copies = []
    for j in range(rows):
        group = [
            pltpu.make_async_copy(m_ref.at[j], masks.at[j], sems.at[j, 0]),
            pltpu.make_async_copy(v_ref.at[j], vs.at[j], sems.at[j, 1]),
            pltpu.make_async_copy(u_ref.at[j], us.at[j], sems.at[j, 2]),
            pltpu.make_async_copy(t_ref.at[j], ts.at[j], sems.at[j, 3]),
        ]
        for c in group:
            c.start()
        copies.append(group)
    done = []
    for g, group in enumerate(groups):
        for i, j in enumerate(group):
            for c in copies[j]:
                c.wait()
            keep = keep_of(masks[j])
            for k, (where, box) in enumerate(((far, fars), (near, nears))):
                if k == 0 and g == 0:
                    continue
                ref = far_refs[g - 1] if k == 0 else near_refs[g]
                for f, field in enumerate((ts, us, vs)):
                    mine = (field[j, pl.ds(where * part, part)] * keep[None]).reshape(size, lon)
                    if k:
                        box[j, f * size : (f + 1) * size, :] = mine
                    else:
                        put_packed(box.at[j], mine, f * size, tails.at[j], lon)
                if not k:
                    box[j, 3 * size :, :] = fold_tails(tails.at[j], lon).astype(BF16)
                c = pltpu.make_async_copy(box.at[j], ref.at[i], out_sems.at[j, k])
                c.start()
                done.append(c)
    for c in done:
        c.wait()


def send(half, u, v, t, mask, after, groups):
    rows, samples, levels, lon = v.shape
    part = samples // 2
    unit = 3 * part * levels
    n = len(groups)
    wire = packed_shape(unit, lon)
    packed = [jax.ShapeDtypeStruct((len(g), unit, lon), BF16) for g in groups]
    sent = [jax.ShapeDtypeStruct((len(g), *wire), BF16) for g in groups[1:]]
    return pl.pallas_call(
        lambda *refs: send_kernel(groups, *refs),
        out_shape=(
            *sent,
            *packed,
        ),
        in_specs=[SMEM, HBM, HBM, HBM, HBM, ANY],
        out_specs=(HBM,) * (2 * n - 1),
        scratch_shapes=[
            pltpu.VMEM((rows, samples, levels, lon), BF16),
            pltpu.VMEM((rows, samples, levels, lon), BF16),
            pltpu.VMEM((rows, samples, levels, lon), BF16),
            pltpu.VMEM((rows, levels, lon), jnp.int32),
            pltpu.VMEM((rows, *wire), BF16),
            pltpu.VMEM((rows, unit, lon), BF16),
            pltpu.VMEM((rows, unit, 128), F32),
            pltpu.SemaphoreType.DMA((rows, 4)),
            pltpu.SemaphoreType.DMA((rows, 2)),
        ],
        compiler_params=params(60),
        name="send",
    )(half, u, v, t, mask, after)


def wave_kernel(half_ref, table_ref, own_ref, got_ref, _, *refs, flips):
    o_refs, (mix, tails) = refs[:-2], refs[-2:]
    n = table_ref.shape[2] // 2
    cols, lon = own_ref.shape[1:]
    main = main_lanes(lon)
    scale = 2.0 / (MERIDIANS * MERIDIANS)
    for i in range(got_ref.shape[0]):
        unfold_tails(got_ref[i, cols:].astype(F32), tails.at[i], lon)
        for at, end in ((0, main), (main, lon)):
            own = own_ref[i, :, at:end].astype(F32)
            got = tails[i, :, 0 : lon - main] if at else got_ref[i, 0:cols].astype(F32)
            for p, mixed in enumerate(((own - got).astype(BF16), (own + got).astype(BF16))):
                mix[i, p, 0:cols, at:end] = mixed
                mix[i, p, cols:, at:end] = mixed[2 * cols // 3 :]
        for p in range(2):
            x = mix[i, p]
            w = x.shape[0] // 2
            for flip, o_ref in zip(flips, o_refs):
                table = table_ref[1 - half_ref[0] if flip else half_ref[0], p]
                c = lax.dot_general(table, x, CONTRACT, preferred_element_type=F32)
                both = c[:n, :w] * c[:n, w:] + c[n:, :w] * c[n:, w:]
                o_ref[i, p] = (scale * both).astype(o_ref.dtype)


def waves(half, table, own, got, after, *flips):
    rows, cols, lon = own.shape
    shape = (rows, 2, PADDED, 2 * cols // 3)
    return pl.pallas_call(
        functools.partial(wave_kernel, flips=flips),
        out_shape=tuple(jax.ShapeDtypeStruct(shape, BF16 if f else F32) for f in flips),
        in_specs=[SMEM, VMEM, VMEM, VMEM, ANY],
        out_specs=(VMEM,) * len(flips),
        scratch_shapes=[
            pltpu.VMEM((rows, 2, 4 * cols // 3, lon), BF16),
            pltpu.VMEM((rows, cols, 128), F32),
        ],
        compiler_params=params(16),
        name="waves",
    )(half, table, own, got, after)


def join_kernel(first, parts, half_ref, *refs):
    own_refs, got_refs = refs[:parts], refs[parts : 2 * parts]
    heat_ref, mom_ref, heat, mom, sems = refs[-5:]
    copies = []
    at = 0
    for own_ref, got_ref in zip(own_refs, got_refs):
        for i in range(own_ref.shape[0]):
            zero = half_ref[0] == 0
            for p in range(2):
                own = own_ref[i, p]
                got = got_ref[i, p].astype(F32)
                a = jnp.where(zero, own, got)
                b = jnp.where(zero, got, own)
                w = own.shape[1] // 2
                low = lax.broadcasted_iota(jnp.int32, own.shape, 1) < w
                n = heat.shape[1] // 2
                every = pl.ds(p, n, stride=2)
                heat[at, every, :] = jnp.where(low, a, pltpu.roll(b, w, 1))[:n]
                mom[at, every, :] = jnp.where(low, pltpu.roll(a, w, 1), b)[:n]
            for k, (x, ref) in enumerate(((heat, heat_ref), (mom, mom_ref))):
                c = pltpu.make_async_copy(x.at[at], ref.at[first + at], sems.at[at, k])
                c.start()
                copies.append(c)
            at += 1
    for c in copies:
        c.wait()


def join(half, own, got, outs, rows, total):
    n, width = ORDERS // 2, own[0].shape[3]
    shape = jax.ShapeDtypeStruct((total, n, width), F32)
    parts = len(own)
    args = (half, *own, *got)
    specs = [SMEM] + [VMEM] * (2 * parts)
    extra = {}
    if outs is not None:
        extra = {"input_output_aliases": {len(args): 0, len(args) + 1: 1}}
        args += outs
        specs += [HBM, HBM]
    return pl.pallas_call(
        lambda *refs: join_kernel(rows[0], parts, *refs),
        out_shape=(shape, shape),
        in_specs=specs,
        out_specs=(HBM, HBM),
        scratch_shapes=[
            pltpu.VMEM((len(rows), n, width), F32),
            pltpu.VMEM((len(rows), n, width), F32),
            pltpu.SemaphoreType.DMA((len(rows), 2)),
        ],
        compiler_params=params(8),
        name="join",
        **extra,
    )(*args)


def cosines(first, rows, total):
    index = lax.broadcasted_iota(jnp.int32, (rows, 1), 0) + first
    return jnp.cos(((index.astype(F32) + 0.5) / total - 0.5) * math.pi)


def weight_of(first, rows, total):
    latitude = ((np.arange(first, first + rows) + 0.5) / total - 0.5) * math.pi
    return float(np.sum(np.cos(latitude)))


def weigh_kernel(total, place_ref, own_ref, lon_ref, depth_ref, d_ref, o_ref):
    rows, samples, levels = d_ref.shape
    band = place_ref[0] // 128 * 64 + place_ref[0] % 64
    depth = depth_ref[...]
    spread = jnp.concatenate([depth] * samples, axis=1)
    kept = own_ref[rows : 2 * rows] + lon_ref[rows : 2 * rows]
    mean = (own_ref[0:rows] + lon_ref[0:rows]) / jnp.maximum(kept, 1.0)
    weighted = mean * cosines(band * rows, rows, total) * spread
    for p in range(o_ref.shape[0]):
        o_ref[p, 0:rows, :] = weighted
        for b in range(samples):
            o_ref[p, 8 : 8 + rows, b * levels : (b + 1) * levels] = d_ref[:, b, :]


def band_kernel(total, rows, levels, place_ref, g_ref, mine_ref, s_ref, w_ref):
    peers, _, width = g_ref.shape
    span = peers * rows
    lane = lax.broadcasted_iota(jnp.int32, (1, width), 1) % levels
    so_far = jnp.zeros((1, width), F32)
    for p in range(peers):
        for r in range(rows):
            so_far = so_far + g_ref[p, r : r + 1, :]
            w_ref[p * rows + r : p * rows + r + 1, :] = so_far
            w_ref[span + p * rows + r : span + p * rows + r + 1, :] = g_ref[p, 8 + r : 9 + r, :]
    run = w_ref[0:span, :]
    step = 1
    while step < levels:
        run = run + jnp.where(lane >= step, pltpu.roll(run, step, 1), 0.0)
        step *= 2
    want = w_ref[span:, :]
    block = place_ref[0] // 128 * 8 + place_ref[0] % 64 // 8
    cosine = cosines(block * span, span, total)
    stats = (
        run[span - 1 : span],
        jnp.max(run, axis=0, keepdims=True),
        jnp.min(run, axis=0, keepdims=True),
        jnp.sum(cosine * run, axis=0, keepdims=True),
        jnp.sum(cosine * run * run, axis=0, keepdims=True),
        jnp.sum(cosine * want, axis=0, keepdims=True),
        jnp.sum(cosine * run * want, axis=0, keepdims=True),
        jnp.sum(cosine * want * want, axis=0, keepdims=True),
    )
    for p in range(s_ref.shape[0]):
        for i, stat in enumerate(stats):
            s_ref[p, i : i + 1, :] = stat
    w_ref[0:span, :] = run
    for p in range(peers):

        @pl.when(place_ref[0] % 8 == p)
        def _():
            mine_ref[...] = w_ref[p * rows : (p + 1) * rows, :]


def add_block(so_far, block, weight):
    s, hi, lo, run1, run2, want1, cross, want2 = block
    if so_far is None:
        return block
    off = so_far[0]
    return (
        off + s,
        jnp.maximum(so_far[1], off + hi),
        jnp.minimum(so_far[2], off + lo),
        so_far[3] + (run1 + off * weight),
        so_far[4] + (run2 + 2.0 * off * run1 + off * off * weight),
        so_far[5] + want1,
        so_far[6] + (cross + off * want1),
        so_far[7] + want2,
    )


def half_kernel(total, span, place_ref, mine_ref, s_ref, own_ref, half_ref):
    blocks = s_ref.shape[0]
    here = place_ref[0] % 64 // 8
    north = place_ref[0] // 128 == 1
    stats = None
    offset = jnp.zeros((1, s_ref.shape[2]), F32)
    for z in range(blocks):
        if z:
            offset = jnp.where(here == z, stats[0], offset)
        weights = [weight_of((h * blocks + z) * span, span, total) for h in range(2)]
        weight = jnp.where(north, weights[1], weights[0])
        stats = add_block(stats, [s_ref[z, i : i + 1, :] for i in range(8)], weight)
    own_ref[...] = mine_ref[...] + offset
    for i, stat in enumerate(stats):
        half_ref[i : i + 1, :] = stat


def finish_kernel(total, place_ref, own_ref, near_ref, far_ref, psi_ref, loss_ref):
    _, samples, levels = psi_ref.shape
    north = place_ref[0] // 128 == 1
    near = near_ref[...]
    far = far_ref[...]
    south_half = jnp.where(north, far, near)
    north_half = jnp.where(north, near, far)
    weight = weight_of(total // 2, total // 2, total)
    stats = add_block(
        [south_half[i : i + 1] for i in range(8)], [north_half[i : i + 1] for i in range(8)], weight
    )
    peak = jnp.max(jnp.maximum(jnp.abs(stats[1]), jnp.abs(stats[2])), axis=1, keepdims=True)
    scale = peak + EPSILON
    psi = (own_ref[...] + jnp.where(north, far[0:1], 0.0)) / scale
    for b in range(samples):
        psi_ref[:, b, :] = psi[:, b * levels : (b + 1) * levels]
    a, b, c = (jnp.sum(stats[i], axis=1, keepdims=True) for i in (4, 6, 7))
    loss = (a / scale / scale - 2.0 * (b / scale) + c) / (samples * levels * total)
    loss_ref[...] = jnp.broadcast_to(loss, loss_ref.shape)


def small(body, out_shape, *args, scratch=(), after=None):
    many = isinstance(out_shape, tuple)
    specs = [SMEM] + [VMEM] * (len(args) - 1)
    if after is not None:
        plain, count = body, len(args)
        body = lambda *refs: plain(*refs[:count], *refs[count + 1 :])
        args += (after,)
        specs.append(ANY)
    return pl.pallas_call(
        body,
        out_shape=out_shape,
        in_specs=specs,
        out_specs=(VMEM,) * len(out_shape) if many else VMEM,
        scratch_shapes=scratch,
        compiler_params=params(2),
    )(*args)


def all_of(x, axes):
    return lax.all_to_all(x, axes, split_axis=0, concat_axis=0, tiled=True)


def floats(*shape):
    return jax.ShapeDtypeStruct(shape, F32)


def per_device(u, v, t, mask, depth, desired):
    bands, samples, levels, lon = v.shape
    width = samples * levels
    total = bands * lax.axis_size(LAT_LEV)
    half = lax.axis_index("lon")[None].astype(jnp.int32)
    place = lax.axis_index(("lat", "lon", "lev_0", "lev_1", "lev_2"))[None].astype(jnp.int32)
    across = [(0, 1), (1, 0)]
    table = jnp.asarray(half_table(lon), BF16)

    def swap(x):
        return lax.ppermute(x, "lon", across)

    first, sums = first_part(half, u, v, t, mask)
    packed = send(half, u, v, t, mask, sums, GROUPS)
    rest, own = packed[: len(GROUPS) - 1], packed[len(GROUPS) - 1 :]
    got = [swap(first)]
    by_lon = swap(sums)
    got += [swap(x) for x in rest]

    peers = lax.axis_size(INNER)
    outer = lax.axis_size(OUTER)
    rows = small(
        lambda *refs: weigh_kernel(total, *refs),
        floats(peers, 16, width),
        place,
        sums,
        by_lon,
        depth[None],
        desired,
    )
    near_bands = all_of(rows, INNER)
    far0, near0 = waves(half, table, own[0], got[0], rows, True, False)
    span = bands * peers
    mine, stats = small(
        lambda *refs: band_kernel(total, bands, levels, *refs),
        (floats(bands, width), floats(outer, 8, width)),
        place,
        near_bands,
        scratch=[pltpu.VMEM((2 * span, width), F32)],
    )
    all_stats = all_of(stats, OUTER)
    mine, near_half = small(
        lambda *refs: half_kernel(total, span, *refs),
        (floats(bands, width), floats(8, width)),
        place,
        mine,
        all_stats,
    )
    far_half = lax.ppermute(near_half, ("lat", "lon"), [(i, 3 - i) for i in range(4)])
    far1, near1 = waves(half, table, own[1], got[1], stats, True, False)
    (far2,) = waves(half, table, own[2], got[2], near_half, True)
    (near2,) = waves(half, table, own[2], got[2], near_half, False)
    psi, loss = small(
        lambda *refs: finish_kernel(total, *refs),
        (floats(bands, samples, levels), floats(1, width)),
        place,
        mine,
        near_half,
        far_half,
        after=near2,
    )

    back = [swap(x) for x in (far0, far1, far2)]
    kept = [near0, near1, near2]
    outs = join(half, kept[:2], back[:2], None, GROUPS[0] + GROUPS[1], bands)
    outs = join(half, kept[2:], back[2:], outs, GROUPS[2], bands)
    heat, momentum = (jnp.transpose(x, (1, 0, 2)) for x in outs)
    return psi, heat, momentum, loss[0, 0]


def solution(mesh):
    torus = Mesh(
        mesh.devices.reshape(mesh.shape["lat"], mesh.shape["lon"], 8, 4, 2),
        ("lat", "lon", "lev_0", "lev_1", "lev_2"),
    )
    in_specs = (
        P(LAT_LEV, None, None, "lon"),
        P(LAT_LEV, None, None, "lon"),
        P(LAT_LEV, None, None, "lon"),
        P(LAT_LEV, None, "lon"),
        P(),
        P(LAT_LEV, None, None),
    )
    out_specs = (P(LAT_LEV, None, None), P("lon", LAT_LEV, None), P("lon", LAT_LEV, None), P())

    return jax.shard_map(
        per_device, mesh=torus, in_specs=in_specs, out_specs=out_specs, check_vma=False
    )
```

```python
import functools
import math

import jax
import jax.numpy as jnp
import numpy as np
from jax import lax
from jax.experimental import pallas as pl
from jax.experimental.pallas import tpu as pltpu
from jax.sharding import Mesh
from jax.sharding import PartitionSpec as P


MERIDIANS = 1440
ORDERS = 720
PADDED = 184
LAT_LEV = ("lat", "lev_0", "lev_1", "lev_2")
INNER = ("lev_1", "lev_2")
OUTER = "lev_0"
EPSILON = 1e-06
GROUPS = ((0,), (1, 2), (3, 4))
F32 = jnp.float32
BF16 = jnp.bfloat16
MIB = 1024 * 1024
CONTRACT = (((1,), (1,)), ((), ()))
SMEM = pl.BlockSpec(memory_space=pltpu.SMEM)
VMEM = pl.BlockSpec(memory_space=pltpu.VMEM)
HBM = pl.BlockSpec(memory_space=pltpu.HBM)
ANY = pl.BlockSpec(memory_space=pl.ANY)


def half_table(lon):
    order = np.arange(1, ORDERS + 1, dtype=np.int64)
    turns = (order[:, None] * np.arange(lon, dtype=np.int64)[None, :]) % MERIDIANS
    angle = turns.astype(np.float32) * np.float32(2.0 * math.pi / MERIDIANS)
    both = np.stack([np.cos(angle), np.sin(angle)]).reshape(2, 2, ORDERS // 4, 2, lon)
    rows = np.zeros((2, 2, 2, PADDED, lon), np.float32)
    rows[:, :, :, : ORDERS // 4] = both.transpose(1, 3, 0, 2, 4)
    return rows.reshape(2, 2, 2 * PADDED, lon)


def params(mib):
    return pltpu.CompilerParams(vmem_limit_bytes=mib * MIB)


def main_lanes(lon):
    return lon // 128 * 128


def packed_shape(cols, lon):
    main = main_lanes(lon)
    return cols + cols // (main // (lon - main)), main


def fold_tails(tail_ref, lon):
    main = main_lanes(lon)
    width = lon - main
    parts = main // width
    rows = tail_ref.shape[0] // parts
    low = lax.broadcasted_iota(jnp.int32, (rows, 128), 1) < width
    total = None
    for j in range(parts):
        piece = jnp.where(low, tail_ref[j * rows : (j + 1) * rows, :], 0.0)
        wide = jnp.concatenate([piece, jnp.zeros((rows, main - 128), F32)], axis=1)
        wide = pltpu.roll(wide, j * width, 1) if j else wide
        total = wide if total is None else total + wide
    return total


def unfold_tails(folded, tail_ref, lon):
    main = main_lanes(lon)
    width = lon - main
    rows = folded.shape[0]
    for j in range(main // width):
        wide = pltpu.roll(folded, main - j * width, 1) if j else folded
        tail_ref[j * rows : (j + 1) * rows, :] = wide[:, :128]


def put_packed(box, field, at, tail_ref, lon):
    main = main_lanes(lon)
    size = field.shape[0]
    box[at : at + size, :] = field[:, :main]
    tail_ref[at : at + size, 0 : lon - main] = field[:, main:].astype(F32)


def keep_of(mask):
    return mask.astype(F32).astype(BF16)


def first_kernel(half_ref, u_ref, v_ref, t_ref, m_ref, o_ref, sums_ref, us, vs, ts, masks, tails, box, sems, out_sem):
    rows, samples, levels, lon = vs.shape
    part = samples // 2
    size = part * levels
    far = 1 - half_ref[0]
    at = pl.ds(far * part, part)
    copies = []
    for j in range(rows):
        copies.append(
            [
                pltpu.make_async_copy(m_ref.at[j], masks.at[j], sems.at[j, 0]),
                pltpu.make_async_copy(v_ref.at[j], vs.at[j], sems.at[j, 1]),
            ]
        )
    extra = [
        pltpu.make_async_copy(u_ref.at[0, at], us, sems.at[0, 2]),
        pltpu.make_async_copy(t_ref.at[0, at], ts, sems.at[0, 3]),
    ]
    for group in (copies[0], extra, *copies[1:]):
        for c in group:
            c.start()
    for c in (*copies[0], *extra):
        c.wait()
    keep = keep_of(masks[0])[None]
    for f, field in enumerate((ts[...], us[...], vs[0, at])):
        put_packed(box, (field * keep).reshape(size, lon), f * size, tails, lon)
    box[3 * size :, :] = fold_tails(tails, lon).astype(BF16)
    out = pltpu.make_async_copy(box, o_ref.at[0], out_sem)
    out.start()
    ones = jnp.ones((8, lon), BF16)
    for j in range(rows):
        if j:
            for c in copies[j]:
                c.wait()
        keep = keep_of(masks[j])
        v = (vs[j] * keep[None]).reshape(samples * levels, lon)
        sums_ref[j : j + 1, :] = lax.dot_general(ones, v, CONTRACT, preferred_element_type=F32)[0:1]
        kept = lax.dot_general(ones, keep, CONTRACT, preferred_element_type=F32)[0:1]
        sums_ref[rows + j : rows + j + 1, :] = jnp.concatenate([kept] * samples, axis=1)
    out.wait()


def first_part(half, u, v, t, mask):
    rows, samples, levels, lon = v.shape
    part = samples // 2
    return pl.pallas_call(
        first_kernel,
        out_shape=(
            jax.ShapeDtypeStruct((1, *packed_shape(3 * part * levels, lon)), BF16),
            jax.ShapeDtypeStruct((2 * rows, samples * levels), F32),
        ),
        in_specs=[SMEM, HBM, HBM, HBM, HBM],
        out_specs=(HBM, VMEM),
        scratch_shapes=[
            pltpu.VMEM((part, levels, lon), BF16),
            pltpu.VMEM((rows, samples, levels, lon), BF16),
            pltpu.VMEM((part, levels, lon), BF16),
            pltpu.VMEM((rows, levels, lon), jnp.int32),
            pltpu.VMEM((3 * part * levels, 128), F32),
            pltpu.VMEM(packed_shape(3 * part * levels, lon), BF16),
            pltpu.SemaphoreType.DMA((rows, 4)),
            pltpu.SemaphoreType.DMA,
        ],
        compiler_params=params(60),
        name="sums",
    )(half, u, v, t, mask)


def send_kernel(groups, half_ref, u_ref, v_ref, t_ref, m_ref, _, *rest):
    n = len(groups)
    far_refs, near_refs = rest[: n - 1], rest[n - 1 : 2 * n - 1]
    us, vs, ts, masks, fars, nears, tails, sems, out_sems = rest[2 * n - 1 :]
    rows, samples, levels, lon = vs.shape
    part = samples // 2
    size = part * levels
    near = half_ref[0]
    far = 1 - near
    copies = []
    for j in range(rows):
        group = [
            pltpu.make_async_copy(m_ref.at[j], masks.at[j], sems.at[j, 0]),
            pltpu.make_async_copy(v_ref.at[j], vs.at[j], sems.at[j, 1]),
            pltpu.make_async_copy(u_ref.at[j], us.at[j], sems.at[j, 2]),
            pltpu.make_async_copy(t_ref.at[j], ts.at[j], sems.at[j, 3]),
        ]
        for c in group:
            c.start()
        copies.append(group)
    done = []
    for g, group in enumerate(groups):
        for i, j in enumerate(group):
            for c in copies[j]:
                c.wait()
            keep = keep_of(masks[j])
            for k, (where, box) in enumerate(((far, fars), (near, nears))):
                if k == 0 and g == 0:
                    continue
                ref = far_refs[g - 1] if k == 0 else near_refs[g]
                for f, field in enumerate((ts, us, vs)):
                    mine = (field[j, pl.ds(where * part, part)] * keep[None]).reshape(size, lon)
                    if k:
                        box[j, f * size : (f + 1) * size, :] = mine
                    else:
                        put_packed(box.at[j], mine, f * size, tails.at[j], lon)
                if not k:
                    box[j, 3 * size :, :] = fold_tails(tails.at[j], lon).astype(BF16)
                c = pltpu.make_async_copy(box.at[j], ref.at[i], out_sems.at[j, k])
                c.start()
                done.append(c)
    for c in done:
        c.wait()


def send(half, u, v, t, mask, after, groups):
    rows, samples, levels, lon = v.shape
    part = samples // 2
    unit = 3 * part * levels
    n = len(groups)
    wire = packed_shape(unit, lon)
    packed = [jax.ShapeDtypeStruct((len(g), unit, lon), BF16) for g in groups]
    sent = [jax.ShapeDtypeStruct((len(g), *wire), BF16) for g in groups[1:]]
    return pl.pallas_call(
        lambda *refs: send_kernel(groups, *refs),
        out_shape=(
            *sent,
            *packed,
        ),
        in_specs=[SMEM, HBM, HBM, HBM, HBM, ANY],
        out_specs=(HBM,) * (2 * n - 1),
        scratch_shapes=[
            pltpu.VMEM((rows, samples, levels, lon), BF16),
            pltpu.VMEM((rows, samples, levels, lon), BF16),
            pltpu.VMEM((rows, samples, levels, lon), BF16),
            pltpu.VMEM((rows, levels, lon), jnp.int32),
            pltpu.VMEM((rows, *wire), BF16),
            pltpu.VMEM((rows, unit, lon), BF16),
            pltpu.VMEM((rows, unit, 128), F32),
            pltpu.SemaphoreType.DMA((rows, 4)),
            pltpu.SemaphoreType.DMA((rows, 2)),
        ],
        compiler_params=params(60),
        name="send",
    )(half, u, v, t, mask, after)


def wave_kernel(half_ref, table_ref, own_ref, got_ref, _, *refs, flips):
    o_refs, (mix, tails) = refs[:-2], refs[-2:]
    n = table_ref.shape[2] // 2
    cols, lon = own_ref.shape[1:]
    main = main_lanes(lon)
    scale = 2.0 / (MERIDIANS * MERIDIANS)
    for i in range(got_ref.shape[0]):
        unfold_tails(got_ref[i, cols:].astype(F32), tails.at[i], lon)
        for at, end in ((0, main), (main, lon)):
            own = own_ref[i, :, at:end].astype(F32)
            got = tails[i, :, 0 : lon - main] if at else got_ref[i, 0:cols].astype(F32)
            for p, mixed in enumerate(((own - got).astype(BF16), (own + got).astype(BF16))):
                mix[i, p, 0:cols, at:end] = mixed
                mix[i, p, cols:, at:end] = mixed[2 * cols // 3 :]
        for p in range(2):
            x = mix[i, p]
            w = x.shape[0] // 2
            for flip, o_ref in zip(flips, o_refs):
                table = table_ref[1 - half_ref[0] if flip else half_ref[0], p]
                c = lax.dot_general(table, x, CONTRACT, preferred_element_type=F32)
                both = c[:n, :w] * c[:n, w:] + c[n:, :w] * c[n:, w:]
                o_ref[i, p] = (scale * both).astype(o_ref.dtype)


def waves(half, table, own, got, after, *flips):
    rows, cols, lon = own.shape
    shape = (rows, 2, PADDED, 2 * cols // 3)
    return pl.pallas_call(
        functools.partial(wave_kernel, flips=flips),
        out_shape=tuple(jax.ShapeDtypeStruct(shape, BF16 if f else F32) for f in flips),
        in_specs=[SMEM, VMEM, VMEM, VMEM, ANY],
        out_specs=(VMEM,) * len(flips),
        scratch_shapes=[
            pltpu.VMEM((rows, 2, 4 * cols // 3, lon), BF16),
            pltpu.VMEM((rows, cols, 128), F32),
        ],
        compiler_params=params(16),
        name="waves",
    )(half, table, own, got, after)


def join_kernel(first, parts, half_ref, *refs):
    own_refs, got_refs = refs[:parts], refs[parts : 2 * parts]
    heat_ref, mom_ref, heat, mom, sems = refs[-5:]
    copies = []
    at = 0
    for own_ref, got_ref in zip(own_refs, got_refs):
        for i in range(own_ref.shape[0]):
            zero = half_ref[0] == 0
            for p in range(2):
                own = own_ref[i, p]
                got = got_ref[i, p].astype(F32)
                a = jnp.where(zero, own, got)
                b = jnp.where(zero, got, own)
                w = own.shape[1] // 2
                low = lax.broadcasted_iota(jnp.int32, own.shape, 1) < w
                n = heat.shape[1] // 2
                every = pl.ds(p, n, stride=2)
                heat[at, every, :] = jnp.where(low, a, pltpu.roll(b, w, 1))[:n]
                mom[at, every, :] = jnp.where(low, pltpu.roll(a, w, 1), b)[:n]
            for k, (x, ref) in enumerate(((heat, heat_ref), (mom, mom_ref))):
                c = pltpu.make_async_copy(x.at[at], ref.at[first + at], sems.at[at, k])
                c.start()
                copies.append(c)
            at += 1
    for c in copies:
        c.wait()


def join(half, own, got, outs, rows, total):
    n, width = ORDERS // 2, own[0].shape[3]
    shape = jax.ShapeDtypeStruct((total, n, width), F32)
    parts = len(own)
    args = (half, *own, *got)
    specs = [SMEM] + [VMEM] * (2 * parts)
    extra = {}
    if outs is not None:
        extra = {"input_output_aliases": {len(args): 0, len(args) + 1: 1}}
        args += outs
        specs += [HBM, HBM]
    return pl.pallas_call(
        lambda *refs: join_kernel(rows[0], parts, *refs),
        out_shape=(shape, shape),
        in_specs=specs,
        out_specs=(HBM, HBM),
        scratch_shapes=[
            pltpu.VMEM((len(rows), n, width), F32),
            pltpu.VMEM((len(rows), n, width), F32),
            pltpu.SemaphoreType.DMA((len(rows), 2)),
        ],
        compiler_params=params(8),
        name="join",
        **extra,
    )(*args)


def cosines(first, rows, total):
    index = lax.broadcasted_iota(jnp.int32, (rows, 1), 0) + first
    return jnp.cos(((index.astype(F32) + 0.5) / total - 0.5) * math.pi)


def weight_of(first, rows, total):
    latitude = ((np.arange(first, first + rows) + 0.5) / total - 0.5) * math.pi
    return float(np.sum(np.cos(latitude)))


def weigh_kernel(total, place_ref, own_ref, lon_ref, depth_ref, d_ref, o_ref):
    rows, samples, levels = d_ref.shape
    band = place_ref[0] // 128 * 64 + place_ref[0] % 64
    depth = depth_ref[...]
    spread = jnp.concatenate([depth] * samples, axis=1)
    kept = own_ref[rows : 2 * rows] + lon_ref[rows : 2 * rows]
    mean = (own_ref[0:rows] + lon_ref[0:rows]) / jnp.maximum(kept, 1.0)
    weighted = mean * cosines(band * rows, rows, total) * spread
    for p in range(o_ref.shape[0]):
        o_ref[p, 0:rows, :] = weighted
        for b in range(samples):
            o_ref[p, 8 : 8 + rows, b * levels : (b + 1) * levels] = d_ref[:, b, :]


def band_kernel(total, rows, levels, place_ref, g_ref, mine_ref, s_ref, w_ref):
    peers, _, width = g_ref.shape
    span = peers * rows
    lane = lax.broadcasted_iota(jnp.int32, (1, width), 1) % levels
    so_far = jnp.zeros((1, width), F32)
    for p in range(peers):
        for r in range(rows):
            so_far = so_far + g_ref[p, r : r + 1, :]
            w_ref[p * rows + r : p * rows + r + 1, :] = so_far
            w_ref[span + p * rows + r : span + p * rows + r + 1, :] = g_ref[p, 8 + r : 9 + r, :]
    run = w_ref[0:span, :]
    step = 1
    while step < levels:
        run = run + jnp.where(lane >= step, pltpu.roll(run, step, 1), 0.0)
        step *= 2
    want = w_ref[span:, :]
    block = place_ref[0] // 128 * 8 + place_ref[0] % 64 // 8
    cosine = cosines(block * span, span, total)
    stats = (
        run[span - 1 : span],
        jnp.max(run, axis=0, keepdims=True),
        jnp.min(run, axis=0, keepdims=True),
        jnp.sum(cosine * run, axis=0, keepdims=True),
        jnp.sum(cosine * run * run, axis=0, keepdims=True),
        jnp.sum(cosine * want, axis=0, keepdims=True),
        jnp.sum(cosine * run * want, axis=0, keepdims=True),
        jnp.sum(cosine * want * want, axis=0, keepdims=True),
    )
    for p in range(s_ref.shape[0]):
        for i, stat in enumerate(stats):
            s_ref[p, i : i + 1, :] = stat
    w_ref[0:span, :] = run
    for p in range(peers):

        @pl.when(place_ref[0] % 8 == p)
        def _():
            mine_ref[...] = w_ref[p * rows : (p + 1) * rows, :]


def add_block(so_far, block, weight):
    s, hi, lo, run1, run2, want1, cross, want2 = block
    if so_far is None:
        return block
    off = so_far[0]
    return (
        off + s,
        jnp.maximum(so_far[1], off + hi),
        jnp.minimum(so_far[2], off + lo),
        so_far[3] + (run1 + off * weight),
        so_far[4] + (run2 + 2.0 * off * run1 + off * off * weight),
        so_far[5] + want1,
        so_far[6] + (cross + off * want1),
        so_far[7] + want2,
    )


def half_kernel(total, span, place_ref, mine_ref, s_ref, own_ref, half_ref):
    blocks = s_ref.shape[0]
    here = place_ref[0] % 64 // 8
    north = place_ref[0] // 128 == 1
    stats = None
    offset = jnp.zeros((1, s_ref.shape[2]), F32)
    for z in range(blocks):
        if z:
            offset = jnp.where(here == z, stats[0], offset)
        weights = [weight_of((h * blocks + z) * span, span, total) for h in range(2)]
        weight = jnp.where(north, weights[1], weights[0])
        stats = add_block(stats, [s_ref[z, i : i + 1, :] for i in range(8)], weight)
    own_ref[...] = mine_ref[...] + offset
    for i, stat in enumerate(stats):
        half_ref[i : i + 1, :] = stat


def finish_kernel(total, place_ref, own_ref, near_ref, far_ref, psi_ref, loss_ref):
    _, samples, levels = psi_ref.shape
    north = place_ref[0] // 128 == 1
    near = near_ref[...]
    far = far_ref[...]
    south_half = jnp.where(north, far, near)
    north_half = jnp.where(north, near, far)
    weight = weight_of(total // 2, total // 2, total)
    stats = add_block(
        [south_half[i : i + 1] for i in range(8)], [north_half[i : i + 1] for i in range(8)], weight
    )
    peak = jnp.max(jnp.maximum(jnp.abs(stats[1]), jnp.abs(stats[2])), axis=1, keepdims=True)
    scale = peak + EPSILON
    psi = (own_ref[...] + jnp.where(north, far[0:1], 0.0)) / scale
    for b in range(samples):
        psi_ref[:, b, :] = psi[:, b * levels : (b + 1) * levels]
    a, b, c = (jnp.sum(stats[i], axis=1, keepdims=True) for i in (4, 6, 7))
    loss = (a / scale / scale - 2.0 * (b / scale) + c) / (samples * levels * total)
    loss_ref[...] = jnp.broadcast_to(loss, loss_ref.shape)


def small(body, out_shape, *args, scratch=(), after=None):
    many = isinstance(out_shape, tuple)
    specs = [SMEM] + [VMEM] * (len(args) - 1)
    if after is not None:
        plain, count = body, len(args)
        body = lambda *refs: plain(*refs[:count], *refs[count + 1 :])
        args += (after,)
        specs.append(ANY)
    return pl.pallas_call(
        body,
        out_shape=out_shape,
        in_specs=specs,
        out_specs=(VMEM,) * len(out_shape) if many else VMEM,
        scratch_shapes=scratch,
        compiler_params=params(2),
    )(*args)


def all_of(x, axes):
    return lax.all_to_all(x, axes, split_axis=0, concat_axis=0, tiled=True)


def floats(*shape):
    return jax.ShapeDtypeStruct(shape, F32)


def per_device(u, v, t, mask, depth, desired):
    bands, samples, levels, lon = v.shape
    width = samples * levels
    total = bands * lax.axis_size(LAT_LEV)
    half = lax.axis_index("lon")[None].astype(jnp.int32)
    place = lax.axis_index(("lat", "lon", "lev_0", "lev_1", "lev_2"))[None].astype(jnp.int32)
    across = [(0, 1), (1, 0)]
    table = jnp.asarray(half_table(lon), BF16)

    def swap(x):
        return lax.ppermute(x, "lon", across)

    first, sums = first_part(half, u, v, t, mask)
    packed = send(half, u, v, t, mask, sums, GROUPS)
    rest, own = packed[: len(GROUPS) - 1], packed[len(GROUPS) - 1 :]
    got = [swap(first)]
    by_lon = swap(sums)
    got += [swap(x) for x in rest]

    peers = lax.axis_size(INNER)
    outer = lax.axis_size(OUTER)
    rows = small(
        lambda *refs: weigh_kernel(total, *refs),
        floats(peers, 16, width),
        place,
        sums,
        by_lon,
        depth[None],
        desired,
    )
    near_bands = all_of(rows, INNER)
    far0, near0 = waves(half, table, own[0], got[0], rows, True, False)
    span = bands * peers
    mine, stats = small(
        lambda *refs: band_kernel(total, bands, levels, *refs),
        (floats(bands, width), floats(outer, 8, width)),
        place,
        near_bands,
        scratch=[pltpu.VMEM((2 * span, width), F32)],
    )
    all_stats = all_of(stats, OUTER)
    mine, near_half = small(
        lambda *refs: half_kernel(total, span, *refs),
        (floats(bands, width), floats(8, width)),
        place,
        mine,
        all_stats,
    )
    far_half = lax.ppermute(near_half, ("lat", "lon"), [(i, 3 - i) for i in range(4)])
    far1, near1 = waves(half, table, own[1], got[1], stats, True, False)
    (far2,) = waves(half, table, own[2], got[2], near_half, True)
    (near2,) = waves(half, table, own[2], got[2], near_half, False)
    psi, loss = small(
        lambda *refs: finish_kernel(total, *refs),
        (floats(bands, samples, levels), floats(1, width)),
        place,
        mine,
        near_half,
        far_half,
        after=near2,
    )

    back = [swap(x) for x in (far0, far1, far2)]
    kept = [near0, near1, near2]
    outs = join(half, kept[:2], back[:2], None, GROUPS[0] + GROUPS[1], bands)
    outs = join(half, kept[2:], back[2:], outs, GROUPS[2], bands)
    heat, momentum = (jnp.transpose(x, (1, 0, 2)) for x in outs)
    return psi, heat, momentum, loss[0, 0]


def solution(mesh):
    torus = Mesh(
        mesh.devices.reshape(mesh.shape["lat"], mesh.shape["lon"], 8, 4, 2),
        ("lat", "lon", "lev_0", "lev_1", "lev_2"),
    )
    in_specs = (
        P(LAT_LEV, None, None, "lon"),
        P(LAT_LEV, None, None, "lon"),
        P(LAT_LEV, None, None, "lon"),
        P(LAT_LEV, None, "lon"),
        P(),
        P(LAT_LEV, None, None),
    )
    out_specs = (P(LAT_LEV, None, None), P("lon", LAT_LEV, None), P("lon", LAT_LEV, None), P())

    return jax.shard_map(
        per_device, mesh=torus, in_specs=in_specs, out_specs=out_specs, check_vma=False
    )
```
